8 devices in a mesh: dp: 1 (over z), fsdp: 2 (over y), sp: 4 (over x, core).
Axes of the slice: x: 2, y: 2, z: 1, core: 2. Of those that a mesh axis runs over, the one named last changes fastest.
Arguments:
- x_in: bfloat16 [24, 384, 5120], P(('dp', 'fsdp'), 'sp')
- norm_attn: bfloat16 [5120], P('fsdp')
- w_query: bfloat16 [5120, 5120], P('fsdp')
- w_key: bfloat16 [5120, 5120], P('fsdp')
- w_value: bfloat16 [5120, 5120], P('fsdp')
- w_out: bfloat16 [5120, 5120], P('fsdp')
- norm_mlp: bfloat16 [5120], P('fsdp')
- w_gate: bfloat16 [5120, 13824], P('fsdp')
- w_up: bfloat16 [5120, 13824], P('fsdp')
- w_down: bfloat16 [13824, 5120], P('fsdp')
Outputs:
- output: bfloat16 [24, 384, 5120], P(('dp', 'fsdp'), 'sp')
All inputs are finite; a program needn't handle non-finite values.
Results may differ from the reference program's by a relative error of at most 0.0114603.
Values are sent between devices in bfloat16 or wider.
A program may use at most 1.5 GiB of HBM per device.

```python
import math
import jax
import jax.numpy as jnp
from jax import lax

MODEL_DIM = 5120
NUM_HEADS = 40
FFN_DIM = 13824
NUM_ROWS = 24
SEQ_SHARDS = 4
SHARD_LEN = 96
QUERY_BLOCK = 32

HEAD_DIM = MODEL_DIM // NUM_HEADS
SEQ_LEN = SEQ_SHARDS * SHARD_LEN
ANCHOR_GAP = 2 * SEQ_SHARDS
NORM_EPS = 1e-5
ROPE_THETA = 5e7
MASK_VALUE = -1e30


def dealt_order(natural):
    lead_rows = natural.shape[0]
    tail_shape = natural.shape[2:]
    token_grid = natural.reshape((lead_rows, SHARD_LEN, SEQ_SHARDS) + tail_shape)
    return jnp.swapaxes(token_grid, 1, 2).reshape((lead_rows, SEQ_LEN) + tail_shape)


def draw_tokens(rng_key):
    key_anchor, key_noise = jax.random.split(rng_key)
    anchors = jax.random.normal(key_anchor, (NUM_ROWS, SEQ_LEN // ANCHOR_GAP + 1, MODEL_DIM), jnp.float32)
    ramp_wts = (jnp.arange(ANCHOR_GAP, dtype=jnp.float32) / ANCHOR_GAP)[None, None, :, None]
    smooth = (1.0 - ramp_wts) * anchors[:, :-1, None, :] + ramp_wts * anchors[:, 1:, None, :]
    smooth = smooth.reshape(NUM_ROWS, SEQ_LEN, MODEL_DIM)
    noise_part = jax.random.normal(key_noise, (NUM_ROWS, SEQ_LEN, MODEL_DIM), jnp.float32)
    return dealt_order(smooth + 0.3 * noise_part).astype(jnp.bfloat16)


def draw_matrix(rng_key, fan_in, fan_out):
    return jax.random.normal(rng_key, (fan_in, fan_out), jnp.float32) * fan_in ** -0.5


def draw_gain(rng_key):
    return jax.random.uniform(rng_key, (MODEL_DIM,), jnp.float32, 0.5, 1.5).astype(jnp.bfloat16)


def setup_inputs(seed: int = 0, part: int = 0) -> dict:
    root_key = jax.random.key(seed)
    shared_keys = jax.random.split(jax.random.fold_in(root_key, 100003), 9)
    query_w = draw_matrix(shared_keys[1], MODEL_DIM, MODEL_DIM)
    key_w = 0.8 * query_w + 0.6 * draw_matrix(shared_keys[2], MODEL_DIM, MODEL_DIM)
    return {
        'x_in': draw_tokens(jax.random.fold_in(root_key, part)),
        'norm_attn': draw_gain(shared_keys[0]),
        'w_query': query_w.astype(jnp.bfloat16),
        'w_key': key_w.astype(jnp.bfloat16),
        'w_value': draw_matrix(shared_keys[3], MODEL_DIM, MODEL_DIM).astype(jnp.bfloat16),
        'w_out': draw_matrix(shared_keys[4], MODEL_DIM, MODEL_DIM).astype(jnp.bfloat16),
        'norm_mlp': draw_gain(shared_keys[5]),
        'w_gate': draw_matrix(shared_keys[6], MODEL_DIM, FFN_DIM).astype(jnp.bfloat16),
        'w_up': draw_matrix(shared_keys[7], MODEL_DIM, FFN_DIM).astype(jnp.bfloat16),
        'w_down': draw_matrix(shared_keys[8], FFN_DIM, MODEL_DIM).astype(jnp.bfloat16),
    }


def rms_norm(hidden, gain):
    hid_f32 = hidden.astype(jnp.float32)
    inv_rms = lax.rsqrt(jnp.mean(hid_f32 * hid_f32, axis=-1, keepdims=True) + NORM_EPS)
    return (hid_f32 * inv_rms * gain.astype(jnp.float32)).astype(jnp.bfloat16)


def apply_rope(proj, angles):
    half_dim = proj.shape[-1] // 2
    lower_half = proj[..., :half_dim]
    upper_half = proj[..., half_dim:]
    cos_tab = jnp.cos(angles)[..., None, :]
    sin_tab = jnp.sin(angles)[..., None, :]
    return jnp.concatenate([lower_half * cos_tab - upper_half * sin_tab, upper_half * cos_tab + lower_half * sin_tab], axis=-1)


def reference(x_in, norm_attn, w_query, w_key, w_value, w_out, norm_mlp, w_gate, w_up, w_down):
    score_scale = HEAD_DIM ** -0.5
    num_blocks = SEQ_LEN // QUERY_BLOCK
    head_shape = (SEQ_LEN, NUM_HEADS, HEAD_DIM)
    seq_idx = jnp.arange(SEQ_LEN, dtype=jnp.int32)
    row_pos = (seq_idx % SHARD_LEN) * SEQ_SHARDS + seq_idx // SHARD_LEN
    inv_freq = jnp.exp(jnp.arange(HEAD_DIM // 2, dtype=jnp.float32) * (-2.0 * math.log(ROPE_THETA) / HEAD_DIM))
    angles = row_pos.astype(jnp.float32)[:, None] * inv_freq[None, :]
    query_pos = row_pos.reshape(num_blocks, QUERY_BLOCK)

    def row_layer(hidden):
        normed = rms_norm(hidden, norm_attn)
        query_rot = apply_rope(jnp.dot(normed, w_query, preferred_element_type=jnp.float32).reshape(head_shape), angles).astype(jnp.bfloat16)
        key_f32 = apply_rope(jnp.dot(normed, w_key, preferred_element_type=jnp.float32).reshape(head_shape), angles).astype(jnp.bfloat16).astype(jnp.float32)
        value_f32 = jnp.dot(normed, w_value, preferred_element_type=jnp.float32).astype(jnp.bfloat16).astype(jnp.float32).reshape(head_shape)

        def block_layer(block_args):
            hid_blk, query_blk, qpos_blk = block_args
            scores = jnp.einsum('qhd,khd->hqk', query_blk.astype(jnp.float32), key_f32) * score_scale
            allowed = row_pos[None, None, :] <= qpos_blk[None, :, None]
            attn_prob = jax.nn.softmax(jnp.where(allowed, scores, MASK_VALUE), axis=-1)
            attn_mix = jnp.einsum('hqk,khd->qhd', attn_prob, value_f32).astype(jnp.bfloat16).reshape(QUERY_BLOCK, MODEL_DIM)
            resid_blk = (hid_blk.astype(jnp.float32) + jnp.dot(attn_mix, w_out, preferred_element_type=jnp.float32)).astype(jnp.bfloat16)
            normed_mlp = rms_norm(resid_blk, norm_mlp)
            gate_act = jax.nn.silu(jnp.dot(normed_mlp, w_gate, preferred_element_type=jnp.float32))
            up_proj = jnp.dot(normed_mlp, w_up, preferred_element_type=jnp.float32)
            hidden_mlp = (gate_act * up_proj).astype(jnp.bfloat16)
            return (resid_blk.astype(jnp.float32) + jnp.dot(hidden_mlp, w_down, preferred_element_type=jnp.float32)).astype(jnp.bfloat16)

        blocks = (hidden.reshape(num_blocks, QUERY_BLOCK, MODEL_DIM), query_rot.reshape(num_blocks, QUERY_BLOCK, NUM_HEADS, HEAD_DIM), query_pos)
        return lax.map(block_layer, blocks).reshape(SEQ_LEN, MODEL_DIM)

    return lax.map(row_layer, x_in)
```

```python
import functools
import math

import jax
import jax.numpy as jnp
from jax import lax
from jax.experimental import pallas as pl
from jax.experimental.pallas import tpu as pltpu
from jax.sharding import PartitionSpec as P

HEAD_DIM = 128
NORM_EPS = 1e-5
ROPE_THETA = 5e7
MASK_VALUE = -1e30

MESH = pl.DeviceIdType.MESH
ANY = pl.BlockSpec(memory_space=pl.ANY)
VM = pl.BlockSpec(memory_space=pltpu.VMEM)
BF16 = jnp.bfloat16
F32 = jnp.float32

SP = 4
NB = 256
GATE_COLS = 512
FULL_CHUNKS = 6
DOWN_COLS = 256
ROW_CHUNKS = 3


def dot(a, b):
    return jnp.dot(a, b, preferred_element_type=F32)


def layer_kernel(
    x, gain, wq, wk, wv, wo, wg, wu, wd, cos, sin, qpos, kpos,
    out, a_all, qkv_rem, wo_rem, gu_rem, wd_rem, qkv, o_own, o_got, hid, b_all, u_own, u_got,
    gain_rem, send_sem, recv_sem, load_sem,
):
    tokens, dim = x.shape
    num_rows, shard_len = o_own.shape[1], o_own.shape[2]
    half, quarter, eighth = dim // 2, dim // 4, dim // 8
    feat = u_own.shape[1]
    half_feat = wd.shape[0]
    tile = tokens // ROW_CHUNKS
    tile_rows = num_rows // ROW_CHUNKS
    last_cols = feat - FULL_CHUNKS * GATE_COLS
    down_chunks = quarter // DOWN_COLS

    y = lax.axis_index("fsdp")
    me = lax.axis_index("sp")
    core, chip = me % 2, me // 2
    peer = [me, me + 1 - 2 * core, (me + 2) % 4, 3 - me]
    to_y = {"fsdp": 1 - y}
    to = [None] + [{"sp": peer[k]} for k in (1, 2, 3)]

    def sp_of(k):
        return 2 * ((chip + k // 2) % 2) + (core + k) % 2

    def cols(start, size):
        return pl.ds(pl.multiple_of(start, 128), size)

    used = [0]

    def slots(n):
        used[0] += n
        return used[0] - n

    s_gain, s_qkv, s_wo, s_gu, s_wd = slots(1), slots(6), slots(4), slots(2 * (FULL_CHUNKS + 1)), slots(4 * down_chunks)
    s_a, s_b = slots(3 * ROW_CHUNKS), slots(3 * ROW_CHUNKS)
    s_o, s_u = slots(3 * ROW_CHUNKS), slots(3 * (FULL_CHUNKS + 1))

    def copy(slot, src, dst, dev):
        return pltpu.make_async_remote_copy(
            src_ref=src, dst_ref=dst, send_sem=send_sem.at[slot], recv_sem=recv_sem.at[slot], device_id=dev, device_id_type=MESH
        )

    def load(slot, src, dst):
        return pltpu.make_async_copy(src, dst, load_sem.at[slot])

    barrier = pltpu.get_barrier_semaphore()
    for dev in (to_y, to[1], to[2], to[3]):
        pl.semaphore_signal(barrier, inc=1, device_id=dev, device_id_type=MESH)
    pl.semaphore_wait(barrier, 4)

    c_gain = copy(s_gain, gain, gain_rem, to_y)
    c_gain.start()

    def qkv_copy(j, h):
        part = (1 - y) if h == 0 else y
        src = (wq, wk, wv)[j].at[:, cols(part * half + me * eighth, eighth)]
        return copy(s_qkv + 2 * j + h, src, qkv_rem.at[j, :, h * eighth : (h + 1) * eighth], to_y)

    def wo_copy(k):
        if k == 0:
            return copy(s_wo, wo.at[:, cols(me * quarter, quarter)], wo_rem.at[0], to_y)
        return copy(s_wo + k, wo_rem.at[k - k % 2 if k == 3 else 0], wo_rem.at[k], to[2] if k == 2 else to[1])

    def gu_copy(c, t, size=GATE_COLS):
        src = (wg, wu)[t].at[:, cols(me * feat + c * GATE_COLS, size)]
        return copy(s_gu + 2 * c + t, src, gu_rem.at[t, :, cols(c * GATE_COLS, size)], to_y)

    def wd_copy(c, k):
        here = cols(c * DOWN_COLS, DOWN_COLS)
        if k == 0:
            return copy(s_wd + 4 * c, wd.at[:, cols(me * quarter + c * DOWN_COLS, DOWN_COLS)], wd_rem.at[0, :, here], to_y)
        src = wd_rem.at[2 if k == 3 else 0, :, here]
        return copy(s_wd + 4 * c + k, src, wd_rem.at[k, :, here], to[2] if k == 2 else to[1])

    for j in range(3):
        for h in range(2):
            qkv_copy(j, h).start()
    wo_copy(0).start()
    for c in range(FULL_CHUNKS + 1):
        for t in range(2):
            gu_copy(c, t, GATE_COLS if c < FULL_CHUNKS else last_cols).start()
    for c in range(down_chunks):
        wd_copy(c, 0).start()
    c_gain.wait_recv()

    def act_copy(base, ref, r, k):
        rows_of = lambda p: pl.ds(p * tokens + r * tile, tile)
        return copy(base + 3 * r + k - 1, ref.at[rows_of(2 if k == 3 else 0)], ref.at[rows_of(k)], to[2] if k == 2 else to[1])

    def norm_chunk(src, dst, which, r):
        rows = tile // 3
        gm = gain[which : which + 1, :]
        go = gain_rem[which : which + 1, :]

        def body(in_ref, out_ref):
            def sub(s, carry):
                here = pl.ds(pl.multiple_of(s * 16, 16), 16)
                mine = in_ref[here, cols(y * half, half)].astype(F32)
                other = in_ref[here, cols((1 - y) * half, half)].astype(F32)
                total = jnp.sum(mine * mine, axis=-1, keepdims=True) + jnp.sum(other * other, axis=-1, keepdims=True)
                inv = lax.rsqrt(total / dim + NORM_EPS)
                out_ref[here, 0:half] = (mine * inv * gm).astype(BF16)
                out_ref[here, half:dim] = (other * inv * go).astype(BF16)
                return carry

            lax.fori_loop(0, rows // 16, sub, 0)

        pltpu.emit_pipeline(
            body,
            grid=(3,),
            in_specs=[pl.BlockSpec((rows, dim), lambda t: (r * 3 + t, 0))],
            out_specs=[pl.BlockSpec((rows, dim), lambda t: (r * 3 + t, 0))],
        )(src, dst)

    def norm_and_send(src, dst, which, base):
        def chunk(r, carry):
            norm_chunk(src, dst, which, r)
            act_copy(base, dst, r, 2).start()
            act_copy(base, dst, r, 1).start()
            return carry

        lax.fori_loop(0, ROW_CHUNKS, chunk, 0)

    def pass_on(base, ref, r):
        act_copy(base, ref, r, 2).wait_recv()
        act_copy(base, ref, r, 3).start()

    def gemm_phases(w_buf):
        def qkv_load(j, slot):
            w = (wq, wk, wv)[j]
            ds = [
                load(4 * slot + h, w.at[:, cols((y if h == 0 else 1 - y) * half + me * eighth, eighth)],
                     w_buf.at[slot, 0:half, h * eighth : (h + 1) * eighth])
                for h in range(2)
            ]
            ds.append(load(4 * slot + 2, qkv_rem.at[j], w_buf.at[slot, half:dim, 0:quarter]))
            return ds

        def qkv_fetch(j, slot):
            ds = qkv_load(j, slot)
            ds[0].start()
            ds[1].start()
            qkv_copy(j, 0).wait_recv()
            qkv_copy(j, 1).wait_recv()
            ds[2].start()
            for d in ds:
                d.wait()

        def qkv_step(s, carry):
            late = s // 4
            j = (1 - late) * (s % 2) + late * 2
            side = (1 - late) * (s // 2) + late * (s % 2)
            slot = j % 2

            @pl.when(s == 0)
            def _():
                pass_on(s_a, a_all, 0)
                qkv_fetch(0, 0)
                for r in range(ROW_CHUNKS):
                    act_copy(s_a, a_all, r, 1).wait_recv()

            @pl.when(s == 1)
            def _():
                pass_on(s_a, a_all, 1)
                pass_on(s_a, a_all, 2)
                qkv_fetch(1, 1)

            @pl.when(s == 2)
            def _():
                for r in range(ROW_CHUNKS):
                    act_copy(s_a, a_all, r, 3).wait_recv()

            @pl.when(s == 4)
            def _():
                qkv_fetch(2, 0)

            def body(a_ref, cos_ref, sin_ref, o_ref):
                c_tab, s_tab = cos_ref[0, 0], sin_ref[0, 0]
                for n in range(quarter // NB):
                    acc = dot(a_ref[...], w_buf[slot, :, n * NB : (n + 1) * NB])
                    for h in range(NB // HEAD_DIM):
                        t = acc[:, h * HEAD_DIM : (h + 1) * HEAD_DIM]
                        rot = t * c_tab + pltpu.roll(t, HEAD_DIM // 2, 1) * s_tab
                        lo = n * NB + h * HEAD_DIM
                        o_ref[0, :, :, lo : lo + HEAD_DIM] = rot.astype(BF16).reshape(tile_rows, shard_len, HEAD_DIM)

            n_t = 2 * ROW_CHUNKS
            t0 = side * n_t
            tab = pl.BlockSpec((1, 1, tile, HEAD_DIM), lambda t: (j // 2, (t0 + t) // ROW_CHUNKS, 0, 0))
            pltpu.emit_pipeline(
                body,
                grid=(n_t,),
                in_specs=[pl.BlockSpec((tile, dim), lambda t: (t0 + t, 0)), tab, tab],
                out_specs=[
                    pl.BlockSpec(
                        (1, tile_rows, shard_len, quarter),
                        lambda t: (j * SP + (t0 + t) // ROW_CHUNKS, (t0 + t) % ROW_CHUNKS, 0, 0),
                    )
                ],
            )(a_all, cos, sin, qkv)
            return carry

        lax.fori_loop(0, 6, qkv_step, 0)

    def attention():
        def o_copy(r, k):
            rows = pl.ds(r * tile_rows, tile_rows)
            return copy(s_o + 3 * r + k - 1, o_own.at[k, rows], o_got.at[k, rows], to[k])

        seq = SP * shard_len

        def body(q_ref, k_ref, v_ref, o_ref):
            keep = kpos[0:1, :] <= qpos[:, 0:1]

            def head(h, carry):
                here = cols(h * HEAD_DIM, HEAD_DIM)
                q = q_ref[:, 0, :, here].reshape(seq, HEAD_DIM)
                k = k_ref[:, 0, :, here].reshape(seq, HEAD_DIM)
                v = v_ref[:, 0, :, here].reshape(seq, HEAD_DIM)
                s = lax.dot_general(q, k, (((1,), (1,)), ((), ())), preferred_element_type=F32) * HEAD_DIM**-0.5
                s = jnp.where(keep, s, MASK_VALUE)
                p = jnp.exp(s - jnp.max(s, axis=-1, keepdims=True))
                total = jnp.sum(p, axis=-1, keepdims=True)
                o = dot(p.astype(BF16), v) / total
                o_ref[:, 0, :, here] = o.astype(BF16).reshape(SP, shard_len, HEAD_DIM)
                return carry

            lax.fori_loop(0, quarter // HEAD_DIM, head, 0)

        def chunk(r, carry):
            def spec(j):
                return pl.BlockSpec((SP, 1, shard_len, quarter), lambda t: (j, r * tile_rows + t, 0, 0))

            pltpu.emit_pipeline(
                body, grid=(tile_rows,), in_specs=[spec(0), spec(1), spec(2)], out_specs=[spec(0)]
            )(qkv, qkv, qkv, o_own)
            for k in (2, 3, 1):
                o_copy(r, k).start()
            return carry

        lax.fori_loop(0, ROW_CHUNKS, chunk, 0)
        return o_copy

    def out_phase(w_buf, o_buf, o_copy):
        def fetch(k, slot):
            return [
                load(4 * slot, wo.at[:, cols(sp_of(k) * quarter, quarter)], w_buf.at[slot, 0:half]),
                load(4 * slot + 1, wo_rem.at[k], w_buf.at[slot, half:dim]),
            ]

        def o_load(k):
            src = o_own if k == 0 else o_got
            return [
                load(8 + 2 * k + h, src.at[k, :, :, h * eighth : (h + 1) * eighth],
                     o_buf.at[:, :, cols(h * half + sp_of(k) * eighth, eighth)])
                for h in range(2)
            ]

        wo_copy(0).wait_recv()
        wo_copy(2).start()
        wo_copy(1).start()
        for d in fetch(0, 0):
            d.start()
        loads = o_load(0)
        for k in (1, 2, 3):
            for r in range(ROW_CHUNKS):
                o_copy(r, k).wait_recv()
            loads += o_load(k)
        for d in loads:
            d.start()
        for d in loads:
            d.wait()

        def step(k, carry):
            slot = k % 2

            @pl.when(k == 1)
            def _():
                wo_copy(2).wait_recv()
                wo_copy(3).start()

            for nxt in range(1, SP):

                @pl.when(k == nxt - 1)
                def _():
                    if nxt != 2:
                        wo_copy(nxt).wait_recv()
                    for d in fetch(nxt, nxt % 2):
                        d.start()

            for d in fetch(k, slot):
                d.wait()

            def body(x_ref, h_ref):
                t = pl.program_id(0)
                lhs = o_buf[pl.ds(t * tile_rows, tile_rows)].reshape(tile, dim)
                for n in range(quarter // NB):
                    here = slice(n * NB, (n + 1) * NB)
                    h_ref[:, here] = (x_ref[:, here].astype(F32) + dot(lhs, w_buf[slot, :, here])).astype(BF16)

            spec = pl.BlockSpec((tile, quarter), lambda t: (t, sp_of(k)))
            pltpu.emit_pipeline(body, grid=(ROW_CHUNKS,), in_specs=[spec], out_specs=[spec])(x, hid)
            return carry

        lax.fori_loop(0, SP, step, 0)

    def gate_phase(w_buf):
        def u_copy(c, k, size=GATE_COLS):
            here = cols(c * GATE_COLS, size)
            return copy(
                s_u + 3 * c + k - 1, u_own.at[pl.ds(k * tokens, tokens), here], u_got.at[pl.ds(k * tokens, tokens), here], to[k]
            )

        def w_load(c, slot, size=GATE_COLS):
            mine = [
                load(4 * slot + t, (wg, wu)[t].at[:, cols(me * feat + c * GATE_COLS, size)],
                     w_buf.at[slot, 0:half, t * size : (t + 1) * size])
                for t in range(2)
            ]
            other = [
                load(4 * slot + 2 + t, gu_rem.at[t, :, cols(c * GATE_COLS, size)],
                     w_buf.at[slot, half:dim, t * size : (t + 1) * size])
                for t in range(2)
            ]
            return mine, other

        def run(c, side, slot, size):
            def body(b_ref, o_ref):
                parts = [dot(b_ref[...], w_buf[slot, :, n * NB : (n + 1) * NB]) for n in range(2 * size // NB)]
                if size % NB:
                    g = [parts[0], parts[1][:, :128]]
                    u = [jnp.concatenate([parts[1][:, 128:], parts[2][:, :128]], axis=1), parts[2][:, 128:]]
                else:
                    g, u = parts[: size // NB], parts[size // NB :]
                lo = 0
                for gg, uu in zip(g, u):
                    o_ref[:, lo : lo + gg.shape[1]] = (jax.nn.silu(gg) * uu).astype(BF16)
                    lo += gg.shape[1]

            n_t = 2 * ROW_CHUNKS
            pltpu.emit_pipeline(
                body,
                grid=(n_t,),
                in_specs=[pl.BlockSpec((tile, dim), lambda t: (side * n_t + t, 0))],
                out_specs=[pl.BlockSpec((tile, size), lambda t: (side * n_t + t, 0))],
            )(b_all, u_own.at[:, cols(c * GATE_COLS, size)])

            @pl.when(side == 0)
            def _():
                u_copy(c, 1, size).start()

            @pl.when(side == 1)
            def _():
                u_copy(c, 2, size).start()
                u_copy(c, 3, size).start()

        early = FULL_CHUNKS // 2

        def which(s):
            q = s // FULL_CHUNKS
            c = (1 - q) * (s % early) + q * (early + (s - FULL_CHUNKS) // 2)
            side = (1 - q) * (s // early) + q * (s % 2)
            return c, side

        first_mine, _ = w_load(0, 0)
        for d in first_mine:
            d.start()
        total = 2 * FULL_CHUNKS

        def step(s, carry):
            c, side = which(s)
            slot = s % 2
            mine, other = w_load(c, slot)

            for r in range(ROW_CHUNKS):

                @pl.when(s == r + 1)
                def _():
                    pass_on(s_b, b_all, r)

            @pl.when(side == 0)
            def _():
                gu_copy(c, 0).wait_recv()
                gu_copy(c, 1).wait_recv()

            for d in other:
                d.start()

            @pl.when(s == 0)
            def _():
                for r in range(ROW_CHUNKS):
                    act_copy(s_b, b_all, r, 1).wait_recv()

            @pl.when(s == early)
            def _():
                for r in range(ROW_CHUNKS):
                    act_copy(s_b, b_all, r, 3).wait_recv()

            for d in mine + other:
                d.wait()

            @pl.when(s + 1 < total)
            def _():
                nc, _ = which(s + 1)
                for d in w_load(nc, (s + 1) % 2)[0]:
                    d.start()

            run(c, side, slot, GATE_COLS)
            return carry

        lax.fori_loop(0, total, step, 0)

        mine, other = w_load(FULL_CHUNKS, 0, last_cols)
        for d in mine:
            d.start()
        for t in range(2):
            gu_copy(FULL_CHUNKS, t, last_cols).wait_recv()
        for d in other:
            d.start()
        for d in mine + other:
            d.wait()

        def last(side, carry):
            run(FULL_CHUNKS, side, 0, last_cols)
            return carry

        lax.fori_loop(0, 2, last, 0)
        return u_copy

    def down_phase(u_copy, u_buf, w_mine, w_other, h_buf, o_buf):
        def u_load(k):
            sp = sp_of(k)
            at = ((sp // 2 + y) % 2) * half_feat + (sp % 2) * feat
            src = u_own if k == 0 else u_got
            return load(k, src.at[pl.ds(k * tokens, tokens)], u_buf.at[:, cols(at, feat)])

        u_load(0).start()
        for k in (1, 2, 3):
            for c in range(FULL_CHUNKS + 1):
                u_copy(c, k, GATE_COLS if c < FULL_CHUNKS else last_cols).wait_recv()
            u_load(k).start()

        def out_cols(c, k):
            return cols(sp_of(k) * quarter + c * DOWN_COLS, DOWN_COLS)

        def fetch(c, k, slot):
            here = out_cols(c, k)
            return [load(4 + 2 * slot, wd.at[:, here], w_mine.at[slot]), load(5 + 2 * slot, hid.at[:, here], h_buf.at[slot])]

        def store(c, k, slot):
            return load(8 + slot, o_buf.at[slot], out.at[:, out_cols(c, k)])

        for d in fetch(0, 0, 0):
            d.start()
        for k in range(SP):
            u_load(k).wait()
        total = SP * down_chunks

        def step(n, carry):
            c, k = unit_of(n)
            slot = n % 2

            @pl.when(k == 0)
            def _():
                wd_copy(c, 0).wait_recv()
                wd_copy(c, 2).start()
                wd_copy(c, 1).start()

            @pl.when(k == 1)
            def _():
                wd_copy(c, 1).wait_recv()

            @pl.when(k == 2)
            def _():
                wd_copy(c, 2).wait_recv()
                wd_copy(c, 3).start()

            @pl.when(k == 3)
            def _():
                wd_copy(c, 3).wait_recv()

            rem = load(10, wd_rem.at[k, :, cols(c * DOWN_COLS, DOWN_COLS)], w_other)
            rem.start()

            @pl.when(n + 1 < total)
            def _():
                nc, nk = unit_of(n + 1)
                for d in fetch(nc, nk, (n + 1) % 2):
                    d.start()

            for d in fetch(c, k, slot):
                d.wait()
            acc = h_buf[slot].astype(F32) + dot(u_buf[:, 0:half_feat], w_mine[slot])
            rem.wait()
            acc = acc + dot(u_buf[:, half_feat:], w_other[...])

            @pl.when(n >= 2)
            def _():
                pc, pk = unit_of(n - 2)
                store(pc, pk, slot).wait()

            o_buf[slot] = acc.astype(BF16)
            store(c, k, slot).start()
            return carry

        def unit_of(n):
            tail = (n + 2) // total
            head = (total + 1 - n) // total
            m = n - 2
            b, u = m // 4, m % 4
            c = head * 0 + tail * (down_chunks - 1) + (1 - head) * (1 - tail) * (b + 1 - u // 2)
            k = head * n + tail * (2 + n - (total - 2)) + (1 - head) * (1 - tail) * u
            return c, k

        lax.fori_loop(0, total, step, 0)
        for n in (total - 2, total - 1):
            store(down_chunks - 1, 2 + n - (total - 2), n % 2).wait()

    norm_and_send(x, a_all, 0, s_a)
    pl.run_scoped(gemm_phases, pltpu.VMEM((2, dim, quarter), BF16))
    o_copy = attention()
    pl.run_scoped(
        functools.partial(out_phase, o_copy=o_copy),
        pltpu.VMEM((2, dim, quarter), BF16),
        pltpu.VMEM((num_rows, shard_len, dim), BF16),
    )
    norm_and_send(hid, b_all, 1, s_b)
    saved = []

    def gates(w_buf):
        saved.append(gate_phase(w_buf))

    pl.run_scoped(gates, pltpu.VMEM((2, dim, 2 * GATE_COLS), BF16))
    pl.run_scoped(
        functools.partial(down_phase, saved[0]),
        pltpu.VMEM((tokens, 2 * half_feat), BF16),
        pltpu.VMEM((2, half_feat, DOWN_COLS), BF16),
        pltpu.VMEM((half_feat, DOWN_COLS), BF16),
        pltpu.VMEM((2, tokens, DOWN_COLS), BF16),
        pltpu.VMEM((2, tokens, DOWN_COLS), BF16),
    )

    c_gain.wait_send()
    for j in range(3):
        for h in range(2):
            qkv_copy(j, h).wait_send()
    for k in range(SP):
        wo_copy(k).wait_send()
    u_copy = saved[0]
    for c in range(FULL_CHUNKS + 1):
        size = GATE_COLS if c < FULL_CHUNKS else last_cols
        for t in range(2):
            gu_copy(c, t, size).wait_send()
        for k in (1, 2, 3):
            u_copy(c, k, size).wait_send()
    for c in range(down_chunks):
        for k in range(SP):
            wd_copy(c, k).wait_send()
    for r in range(ROW_CHUNKS):
        for k in (1, 2, 3):
            act_copy(s_a, a_all, r, k).wait_send()
            act_copy(s_b, b_all, r, k).wait_send()
            o_copy(r, k).wait_send()


def tables(shard_len, tile_rows):
    me = lax.axis_index("sp")
    peer = jnp.stack([me, me ^ 1, me ^ 2, me ^ 3])
    pos = jnp.arange(shard_len, dtype=jnp.int32)[None, :] * SP + peer[:, None]
    inv_freq = jnp.exp(jnp.arange(HEAD_DIM // 2, dtype=F32) * (-2.0 * math.log(ROPE_THETA) / HEAD_DIM))
    angles = pos.astype(F32)[..., None] * inv_freq
    cos_tab, sin_tab = jnp.cos(angles), jnp.sin(angles)
    cos = jnp.tile(jnp.concatenate([cos_tab, cos_tab], axis=-1), (1, tile_rows, 1))
    sin = jnp.tile(jnp.concatenate([-sin_tab, sin_tab], axis=-1), (1, tile_rows, 1))
    cos = jnp.stack([cos, jnp.ones_like(cos)])
    sin = jnp.stack([sin, jnp.zeros_like(sin)])
    flat = pos.reshape(-1)
    qpos = jnp.broadcast_to(flat[:, None], (flat.size, 128))
    kpos = jnp.broadcast_to(flat[None, :], (8, flat.size))
    return cos, sin, qpos, kpos


def local_layer(x_loc, norm_attn, w_query, w_key, w_value, w_out, norm_mlp, w_gate, w_up, w_down):
    num_rows, shard_len, dim = x_loc.shape
    tokens = num_rows * shard_len
    half, quarter = dim // 2, dim // 4
    half_feat = w_down.shape[0]
    feat = half_feat // 2
    gain = jnp.zeros((8, half), F32).at[0].set(norm_attn.astype(F32)).at[1].set(norm_mlp.astype(F32))
    cos, sin, qpos, kpos = tables(shard_len, num_rows // ROW_CHUNKS)

    def buf(*shape):
        return jax.ShapeDtypeStruct(shape, BF16)

    shapes = [
        buf(tokens, dim),
        buf(SP * tokens, dim),
        buf(3, half, quarter),
        buf(SP, half, quarter),
        buf(2, half, feat),
        buf(SP, half_feat, quarter),
        buf(3 * SP, num_rows, shard_len, quarter),
        buf(SP, num_rows, shard_len, quarter),
        buf(SP, num_rows, shard_len, quarter),
        buf(tokens, dim),
        buf(SP * tokens, dim),
        buf(SP * tokens, feat),
        buf(SP * tokens, feat),
    ]
    copies = 1 + 6 + 4 + 2 * (FULL_CHUNKS + 1) + 4 * (quarter // DOWN_COLS) + 9 * ROW_CHUNKS + 3 * (FULL_CHUNKS + 1)
    outs = pl.pallas_call(
        layer_kernel,
        out_shape=shapes,
        in_specs=[ANY, VM] + [ANY] * 9 + [VM, VM],
        out_specs=[ANY] * len(shapes),
        scratch_shapes=[
            pltpu.VMEM((8, half), F32),
            pltpu.SemaphoreType.DMA((copies,)),
            pltpu.SemaphoreType.DMA((copies,)),
            pltpu.SemaphoreType.DMA((16,)),
        ],
        compiler_params=pltpu.CompilerParams(collective_id=0, has_side_effects=True, vmem_limit_bytes=67043328),
        name="decoder_layer",
    )(x_loc.reshape(tokens, dim), gain, w_query, w_key, w_value, w_out, w_gate, w_up, w_down, cos, sin, qpos, kpos)
    return outs[0].reshape(x_loc.shape)


def solution(mesh):
    row_spec = P(("dp", "fsdp"), "sp", None)
    weight_spec = P("fsdp", None)
    gain_spec = P("fsdp")
    in_specs = (row_spec, gain_spec, weight_spec, weight_spec, weight_spec, weight_spec, gain_spec, weight_spec, weight_spec, weight_spec)
    fn = jax.shard_map(local_layer, mesh=mesh, in_specs=in_specs, out_specs=row_spec, check_vma=False)

    def run(*args):
        with jax.sharding.use_abstract_mesh(mesh.abstract_mesh):
            return fn(*args)

    return run
```

```python
import functools
import math

import jax
import jax.numpy as jnp
import numpy as np
from jax import lax
from jax.experimental import pallas as pl
from jax.experimental.pallas import tpu as pltpu
from jax.sharding import PartitionSpec as P

HEAD_DIM = 128
NORM_EPS = 1e-5
ROPE_THETA = 5e7
MASK_VALUE = -1e30

MESH = pl.DeviceIdType.MESH
ANY = pl.BlockSpec(memory_space=pl.ANY)
VM = pl.BlockSpec(memory_space=pltpu.VMEM)
BF16 = jnp.bfloat16
F32 = jnp.float32

SP = 4
NB = 256
GATE_COLS = 384
FULL_CHUNKS = 8
DOWN_COLS = 256
DOWN_PARTS = 4
ROW_CHUNKS = 3


def dot(a, b):
    return jnp.dot(a, b, preferred_element_type=F32)


def layer_kernel(
    x, gain, wq, wk, wv, wo, wg, wu, wd, cos, sin,
    out, x_got, a_all, qkv_rem, wo_rem, gu_rem, wd_rem, qkv, o_own, o_got, hid, b_all, u_own, u_got,
    gain_rem, cos_buf, sin_buf, send_sem, recv_sem, load_sem,
):
    tokens, dim = x.shape
    num_rows, shard_len = o_own.shape[1], o_own.shape[2]
    half, quarter, eighth = dim // 2, dim // 4, dim // 8
    feat = u_own.shape[1]
    half_feat = wd.shape[0]
    tile = tokens // ROW_CHUNKS
    tile_rows = num_rows // ROW_CHUNKS
    down_chunks = quarter // DOWN_COLS
    part_rows = half_feat // DOWN_PARTS
    heads = eighth // HEAD_DIM
    rest = feat - FULL_CHUNKS * GATE_COLS
    sizes = [GATE_COLS] * FULL_CHUNKS + [rest - 128, 128]
    starts = [GATE_COLS * c for c in range(FULL_CHUNKS)] + [feat - rest, feat - 128]
    chunks = len(sizes)

    y = lax.axis_index("fsdp")
    me = lax.axis_index("sp")
    core, chip = me % 2, me // 2
    peer = [me, me + 1 - 2 * core, (me + 2) % 4, 3 - me]
    to_y = {"fsdp": 1 - y}
    to = [None] + [{"sp": peer[k]} for k in (1, 2, 3)]

    def sp_of(k):
        return 2 * ((chip + k // 2) % 2) + (core + k) % 2

    def cols(start, size):
        return pl.ds(pl.multiple_of(start, 128), size)

    def rows(start, size):
        return pl.ds(pl.multiple_of(start, 16), size)

    used = [0]

    def slots(n):
        used[0] += n
        return used[0] - n

    s_gain, s_qkv, s_wo, s_gu = slots(1), slots(6), slots(4), slots(2 * chunks)
    s_wd = slots(4 * DOWN_PARTS * down_chunks)
    s_x, s_a, s_b = slots(ROW_CHUNKS), slots(2 * ROW_CHUNKS), slots(2 * ROW_CHUNKS)
    s_o, s_u = slots(12 * ROW_CHUNKS), slots(3 * chunks)

    def copy(slot, src, dst, dev):
        return pltpu.make_async_remote_copy(
            src_ref=src, dst_ref=dst, send_sem=send_sem.at[slot], recv_sem=recv_sem.at[slot], device_id=dev, device_id_type=MESH
        )

    def load(slot, src, dst):
        return pltpu.make_async_copy(src, dst, load_sem.at[slot])

    barrier = pltpu.get_barrier_semaphore()
    for dev in (to_y, to[1], to[2], to[3]):
        pl.semaphore_signal(barrier, inc=1, device_id=dev, device_id_type=MESH)
    pl.semaphore_wait(barrier, 4)

    def x_copy(r):
        here = rows(r * tile, tile)
        return copy(s_x + r, x.at[here], x_got.at[here], to[2])

    gain_copy = copy(s_gain, gain, gain_rem, to_y)

    def qkv_copy(j, h):
        part = (1 - y + h) % 2
        src = (wq, wk, wv)[j].at[:, cols(part * half + me * eighth, eighth)]
        return copy(s_qkv + 2 * j + h, src, qkv_rem.at[2 * j + h], to_y)

    def wo_copy(k):
        if k == 0:
            return copy(s_wo, wo.at[:, cols(me * quarter, quarter)], wo_rem.at[0], to_y)
        return copy(s_wo + k, wo_rem.at[2 if k == 3 else 0], wo_rem.at[k], to[2] if k == 2 else to[1])

    def gu_copy(c, t, start, size):
        src = (wg, wu)[t].at[:, cols(me * feat + start, size)]
        return copy(s_gu + 2 * c + t, src, gu_rem.at[t, :, cols(start, size)], to_y)

    def wd_copy(m, k):
        part, col = rows((m % DOWN_PARTS) * part_rows, part_rows), (m // DOWN_PARTS) * DOWN_COLS
        if k == 0:
            return copy(s_wd + 4 * m, wd.at[part, cols(me * quarter + col, DOWN_COLS)], wd_rem.at[0, part, cols(col, DOWN_COLS)], to_y)
        here = (part, cols(col, DOWN_COLS))
        return copy(s_wd + 4 * m + k, wd_rem.at[(2 if k == 3 else 0, *here)], wd_rem.at[(k, *here)], to[2] if k == 2 else to[1])

    def act_copy(base, ref, piece, r):
        return copy(
            base + (piece // 2) * ROW_CHUNKS + r,
            ref.at[rows(piece * tokens + r * tile, tile)],
            ref.at[rows((piece + 1) * tokens + r * tile, tile)],
            to[1],
        )

    def o_copy(h, r, k, s):
        here = pl.ds(r * tile_rows, tile_rows)
        piece = k ^ (2 * s)
        return copy(
            s_o + ((h * ROW_CHUNKS + r) * 3 + k - 1) * 2 + s,
            o_own.at[4 * h + piece, here],
            o_got.at[6 * h + 2 * (k - 1) + s, here],
            to[k],
        )

    def u_copy(c, k, start, size):
        here = (pl.ds(k * tokens, tokens), cols(start, size))
        return copy(s_u + 3 * c + k - 1, u_own.at[here], u_got.at[here], to[k])

    for r in range(ROW_CHUNKS):
        x_copy(r).start()
    gain_copy.start()
    for h in range(2):
        for j in range(3):
            qkv_copy(j, h).start()
    wo_copy(0).start()
    for c in range(chunks):
        for t in range(2):
            gu_copy(c, t, starts[c], sizes[c]).start()
    for m in range(DOWN_PARTS * down_chunks):
        wd_copy(m, 0).start()
    tabs = [load(0, cos, cos_buf), load(1, sin, sin_buf)]
    for d in tabs:
        d.start()
    for d in tabs:
        d.wait()
    gain_copy.wait_recv()

    def norm_chunk(src, dst, which, src_row, dst_row):
        n = tile // 3
        gm = gain[which : which + 1, :]
        go = gain_rem[which : which + 1, :]

        def body(in_ref, out_ref):
            def sub(s, carry):
                here = pl.ds(pl.multiple_of(s * 16, 16), 16)
                mine = in_ref[here, cols(y * half, half)].astype(F32)
                other = in_ref[here, cols((1 - y) * half, half)].astype(F32)
                total = jnp.sum(mine * mine, axis=-1, keepdims=True) + jnp.sum(other * other, axis=-1, keepdims=True)
                inv = lax.rsqrt(total / dim + NORM_EPS)
                out_ref[here, 0:half] = (mine * inv * gm).astype(BF16)
                out_ref[here, half:dim] = (other * inv * go).astype(BF16)
                return carry

            lax.fori_loop(0, n // 16, sub, 0)

        pltpu.emit_pipeline(
            body,
            grid=(3,),
            in_specs=[pl.BlockSpec((n, dim), lambda t: (src_row // n + t, 0))],
            out_specs=[pl.BlockSpec((n, dim), lambda t: (dst_row // n + t, 0))],
        )(src, dst)

    def own_a(r, carry):
        norm_chunk(x, a_all, 0, r * tile, r * tile)
        act_copy(s_a, a_all, 0, r).start()
        return carry

    def got_a(r, carry):
        x_copy(r).wait_recv()
        norm_chunk(x_got, a_all, 0, r * tile, 2 * tokens + r * tile)
        act_copy(s_a, a_all, 2, r).start()
        return carry

    def attention(w_qk, w_v):
        seq = SP * shard_len
        idx = lax.broadcasted_iota(jnp.int32, (1, seq), 1)
        idq = lax.broadcasted_iota(jnp.int32, (seq, 1), 0)

        def position(i):
            piece = (i >= shard_len).astype(jnp.int32) + (i >= 2 * shard_len).astype(jnp.int32) + (i >= 3 * shard_len).astype(jnp.int32)
            chip_of = (chip + (piece >> 1)) & 1
            core_of = (core + piece) & 1
            return SP * (i - shard_len * piece) + 2 * chip_of + core_of

        def attn_body(q_ref, k_ref, v_ref, o_ref):
            keep = position(idx) <= position(idq)

            def head(h, carry):
                here = cols(h * HEAD_DIM, HEAD_DIM)
                q = q_ref[:, 0, :, here].reshape(seq, HEAD_DIM)
                k = k_ref[:, 0, :, here].reshape(seq, HEAD_DIM)
                v = v_ref[:, 0, :, here].reshape(seq, HEAD_DIM)
                s = lax.dot_general(q, k, (((1,), (1,)), ((), ())), preferred_element_type=F32) * HEAD_DIM**-0.5
                s = jnp.where(keep, s, MASK_VALUE)
                p = jnp.exp(s - jnp.max(s, axis=-1, keepdims=True))
                total = jnp.sum(p, axis=-1, keepdims=True)
                o = dot(p.astype(BF16), v) / total
                o_ref[:, 0, :, here] = o.astype(BF16).reshape(SP, shard_len, HEAD_DIM)
                return carry

            lax.fori_loop(0, heads, head, 0)

        def w_loads(j, h, dst, at):
            part = (y + h) % 2
            return [
                load(2 * j, (wq, wk, wv)[j].at[:, cols(part * half + me * eighth, eighth)], dst.at[0:half, at : at + eighth]),
                load(2 * j + 1, qkv_rem.at[2 * j + h], dst.at[half:dim, at : at + eighth]),
            ]

        def heads_half(h, carry):
            @pl.when(h == 0)
            def _():
                got_a(0, 0)

            loads = w_loads(0, h, w_qk, 0) + w_loads(1, h, w_qk, eighth)
            loads[0].start()
            loads[2].start()
            qkv_copy(0, h).wait_recv()
            loads[1].start()
            qkv_copy(1, h).wait_recv()
            loads[3].start()
            for d in loads:
                d.wait()

            def qk_side(side, c2):
                @pl.when((h == 0) & (side == 0))
                def _():
                    for r in range(ROW_CHUNKS):
                        act_copy(s_a, a_all, 0, r).wait_recv()

                @pl.when((h == 0) & (side == 1))
                def _():
                    lax.fori_loop(1, ROW_CHUNKS, got_a, 0)
                    for r in range(ROW_CHUNKS):
                        act_copy(s_a, a_all, 2, r).wait_recv()

                t0 = side * 2 * ROW_CHUNKS

                def body(a_ref, q_ref, k_ref):
                    sp = sp_of((t0 + pl.program_id(0)) // ROW_CHUNKS)
                    c_tab, s_tab = cos_buf[sp], sin_buf[sp]
                    for n in range(2 * eighth // NB):
                        acc = dot(a_ref[...], w_qk[:, n * NB : (n + 1) * NB])
                        for i in range(NB // HEAD_DIM):
                            t = acc[:, i * HEAD_DIM : (i + 1) * HEAD_DIM]
                            turned = pltpu.roll(t, HEAD_DIM // 2, 1)
                            shape = (tile_rows, shard_len, HEAD_DIM)
                            rot = t.reshape(shape) * c_tab + turned.reshape(shape) * s_tab
                            lo = n * NB + i * HEAD_DIM
                            ref = q_ref if lo < eighth else k_ref
                            lo = lo % eighth
                            ref[0, :, :, lo : lo + HEAD_DIM] = rot.astype(BF16)

                def spec(j):
                    return pl.BlockSpec(
                        (1, tile_rows, shard_len, eighth),
                        lambda t: ((2 * j + h) * SP + (t0 + t) // ROW_CHUNKS, (t0 + t) % ROW_CHUNKS, 0, 0),
                    )

                pltpu.emit_pipeline(
                    body,
                    grid=(2 * ROW_CHUNKS,),
                    in_specs=[pl.BlockSpec((tile, dim), lambda t: (t0 + t, 0))],
                    out_specs=[spec(0), spec(1)],
                )(a_all, qkv, qkv)
                return c2

            v_loads = w_loads(2, h, w_v, 0)
            v_loads[0].start()
            lax.fori_loop(0, 2, qk_side, 0)
            qkv_copy(2, h).wait_recv()
            v_loads[1].start()
            for d in v_loads:
                d.wait()

            def rows_chunk(r, c2):
                def v_body(a_ref, v_ref):
                    for lo in range(0, eighth, NB):
                        size = min(NB, eighth - lo)
                        acc = dot(a_ref[...], w_v[:, lo : lo + size])
                        v_ref[0, :, :, lo : lo + size] = acc.astype(BF16).reshape(tile_rows, shard_len, size)

                pltpu.emit_pipeline(
                    v_body,
                    grid=(SP,),
                    in_specs=[pl.BlockSpec((tile, dim), lambda t: (t * ROW_CHUNKS + r, 0))],
                    out_specs=[pl.BlockSpec((1, tile_rows, shard_len, eighth), lambda t: ((4 + h) * SP + t, r, 0, 0))],
                )(a_all, qkv)

                def spec(block):
                    return pl.BlockSpec((SP, 1, shard_len, eighth), lambda t: (block, r * tile_rows + t, 0, 0))

                pltpu.emit_pipeline(
                    attn_body,
                    grid=(tile_rows,),
                    in_specs=[spec(h), spec(2 + h), spec(4 + h)],
                    out_specs=[spec(h)],
                )(qkv, qkv, qkv, o_own)
                for k in (2, 3, 1):
                    for s in range(2):
                        o_copy(h, r, k, s).start()
                return c2

            lax.fori_loop(0, ROW_CHUNKS, rows_chunk, 0)
            return carry

        lax.fori_loop(0, 2, heads_half, 0)

    def out_phase(w_buf, o_buf):
        def fetch(k, slot):
            return [
                load(2 * slot, wo.at[:, cols(sp_of(k) * quarter, quarter)], w_buf.at[slot, 0:half]),
                load(2 * slot + 1, wo_rem.at[k], w_buf.at[slot, half:dim]),
            ]

        def o_load(h, k, s):
            src = o_own.at[4 * h + 2 * s] if k == 0 else o_got.at[6 * h + 2 * (k - 1) + s]
            dst = o_buf.at[s * num_rows : (s + 1) * num_rows, :, cols(h * half + sp_of(k) * eighth, eighth)]
            return load(4 + 8 * h + 2 * k + s, src, dst)

        loads = []

        def o_fetch(h):
            for k in (0, 1, 2, 3):
                for s in range(2):
                    if k:
                        for r in range(ROW_CHUNKS):
                            o_copy(h, r, k, s).wait_recv()
                    d = o_load(h, k, s)
                    d.start()
                    loads.append(d)

        o_fetch(0)
        wo_copy(0).wait_recv()
        wo_copy(2).start()
        wo_copy(1).start()
        for d in fetch(0, 0):
            d.start()
        o_fetch(1)
        for d in loads:
            d.wait()

        def step(k, carry):
            slot = k % 2

            @pl.when(k == 0)
            def _():
                wo_copy(1).wait_recv()
                for d in fetch(1, 1):
                    d.start()

            @pl.when(k == 2)
            def _():
                wo_copy(2).wait_recv()
                wo_copy(3).start()
                for d in fetch(2, 0):
                    d.start()

            for d in fetch(k, slot):
                d.wait()

            def run(x_ref_all, s):
                def body(x_ref, h_ref):
                    mine = pl.ds(s * num_rows + pl.program_id(0) * tile_rows, tile_rows)
                    for n in range(quarter // NB):
                        here = slice(n * NB, (n + 1) * NB)
                        lhs = o_buf[mine].reshape(tile, dim)
                        h_ref[:, here] = (x_ref[:, here].astype(F32) + dot(lhs, w_buf[slot, :, here])).astype(BF16)

                pltpu.emit_pipeline(
                    body,
                    grid=(ROW_CHUNKS,),
                    in_specs=[pl.BlockSpec((tile, quarter), lambda t: (t, sp_of(k)))],
                    out_specs=[pl.BlockSpec((tile, quarter), lambda t: (s * ROW_CHUNKS + t, sp_of(k)))],
                )(x_ref_all, hid)

            run(x, 0)

            @pl.when(k == 2)
            def _():
                wo_copy(3).wait_recv()
                for d in fetch(3, 1):
                    d.start()

            run(x_got, 1)
            return carry

        lax.fori_loop(0, SP, step, 0)

    def b_chunk(n, carry):
        s, r = n // ROW_CHUNKS, n % ROW_CHUNKS
        norm_chunk(hid, b_all, 1, n * tile, 2 * s * tokens + r * tile)
        copy(
            s_b + n,
            b_all.at[rows(2 * s * tokens + r * tile, tile)],
            b_all.at[rows((2 * s + 1) * tokens + r * tile, tile)],
            to[1],
        ).start()
        return carry

    def gate_phase(w_buf):
        def w_load(slot, start, size):
            mine = [
                load(4 * slot + t, (wg, wu)[t].at[:, cols(me * feat + start, size)], w_buf.at[slot, 0:half, t * size : (t + 1) * size])
                for t in range(2)
            ]
            other = [
                load(4 * slot + 2 + t, gu_rem.at[t, :, cols(start, size)], w_buf.at[slot, half:dim, t * size : (t + 1) * size])
                for t in range(2)
            ]
            return mine, other

        def run(c, side, slot, start, size):
            def body(b_ref, o_ref):
                parts = [dot(b_ref[...], w_buf[slot, :, n * NB : (n + 1) * NB]) for n in range(2 * size // NB)]
                both = [p[:, lo : lo + 128] for p in parts for lo in (0, 128)]
                n = size // 128
                for i in range(n):
                    o_ref[:, i * 128 : (i + 1) * 128] = (jax.nn.silu(both[i]) * both[n + i]).astype(BF16)

            n_t = 2 * ROW_CHUNKS
            pltpu.emit_pipeline(
                body,
                grid=(n_t,),
                in_specs=[pl.BlockSpec((tile, dim), lambda t: (side * n_t + t, 0))],
                out_specs=[pl.BlockSpec((tile, size), lambda t: (side * n_t + t, 0))],
            )(b_all, u_own.at[:, cols(start, size)])

            @pl.when(side == 0)
            def _():
                u_copy(c, 1, start, size).start()

            @pl.when(side == 1)
            def _():
                u_copy(c, 2, start, size).start()
                u_copy(c, 3, start, size).start()

        def chunk(c, slot, start, size, prefetch):
            mine, other = w_load(slot, start, size)
            for t in range(2):
                gu_copy(c, t, start, size).wait_recv()
            for d in other:
                d.start()
            for d in mine + other:
                d.wait()
            prefetch()

            def sides(t, carry):
                side = 1 - t

                @pl.when(c == 0)
                def _():
                    for r in range(ROW_CHUNKS):
                        n = side * ROW_CHUNKS + r
                        copy(
                            s_b + n,
                            b_all.at[rows(2 * side * tokens + r * tile, tile)],
                            b_all.at[rows((2 * side + 1) * tokens + r * tile, tile)],
                            to[1],
                        ).wait_recv()

                run(c, side, slot, start, size)
                return carry

            lax.fori_loop(0, 2, sides, 0)

        for d in w_load(0, 0, GATE_COLS)[0]:
            d.start()

        def full(c, carry):
            def prefetch():
                @pl.when(c + 1 < FULL_CHUNKS)
                def _():
                    for d in w_load((c + 1) % 2, (c + 1) * GATE_COLS, GATE_COLS)[0]:
                        d.start()

                @pl.when(c + 1 == FULL_CHUNKS)
                def _():
                    for d in w_load((c + 1) % 2, starts[FULL_CHUNKS], sizes[FULL_CHUNKS])[0]:
                        d.start()

            chunk(c, c % 2, c * GATE_COLS, GATE_COLS, prefetch)
            return carry

        lax.fori_loop(0, FULL_CHUNKS, full, 0)
        for c in range(FULL_CHUNKS, chunks):

            def prefetch(c=c):
                if c + 1 < chunks:
                    for d in w_load((c + 1) % 2, starts[c + 1], sizes[c + 1])[0]:
                        d.start()

            chunk(c, c % 2, starts[c], sizes[c], prefetch)

    def down_phase(u_buf, w_mine, w_other, h_buf, acc_buf, o_buf):
        total = SP * down_chunks
        pieces = DOWN_PARTS * down_chunks
        band = tokens // 2

        def pass_y(m):
            @pl.when(m < pieces)
            def _():
                wd_copy(m, 0).wait_recv()
                wd_copy(m, 2).start()
                wd_copy(m, 1).start()

        def pass_x(m):
            wd_copy(m, 2).wait_recv()
            wd_copy(m, 3).start()

        def u_load(k):
            sp = sp_of(k)
            at = ((sp // 2 + y) % 2) * half_feat + (sp % 2) * feat
            return load(k, (u_got if k else u_own).at[pl.ds(k * tokens, tokens)], u_buf.at[:, cols(at, feat)])

        def out_cols(n):
            return cols(sp_of(n % 4) * quarter + (n // 4) * DOWN_COLS, DOWN_COLS)

        def fetch(n):
            slot = n % 2
            here = out_cols(n)
            return [load(4 + 2 * slot, wd.at[:, here], w_mine.at[slot]), load(5 + 2 * slot, hid.at[0:tokens, here], h_buf.at[slot])]

        def store(n):
            return load(8 + n % 2, o_buf.at[n % 2], out.at[:, out_cols(n)])

        for d in fetch(0):
            d.start()
        u_load(0).start()
        for k in (1, 2, 3):
            for c in range(chunks):
                u_copy(c, k, starts[c], sizes[c]).wait_recv()
            u_load(k).start()
        pass_y(0)
        pass_y(1)
        for k in range(SP):
            u_load(k).wait()

        def step(i, carry):
            n = i - 2
            c, k = n // 4, n % 4

            @pl.when((n >= 0) & (k == 0))
            def _():
                pass_x(4 * c)
                pass_y(4 * c + 2)
                pass_y(4 * c + 3)

            @pl.when((n >= 0) & (k == 1))
            def _():
                pass_x(4 * c + 1)
                pass_x(4 * c + 2)

            @pl.when((n >= 0) & (k == 2))
            def _():
                pass_y(4 * c + 4)
                pass_x(4 * c + 3)

            @pl.when((n >= 0) & (k == 3))
            def _():
                pass_y(4 * c + 5)

            for side in (1, 3):

                @pl.when((n >= 0) & (k == side))
                def _():
                    for p in range(DOWN_PARTS):
                        wd_copy(DOWN_PARTS * c + p, side).wait_recv()

            def other_load():
                return load(10, wd_rem.at[k, :, cols(c * DOWN_COLS, DOWN_COLS)], w_other)

            @pl.when(n >= 0)
            def _():
                other_load().start()

            @pl.when(i + 1 < total)
            def _():
                for d in fetch(i + 1):
                    d.start()

            @pl.when(i < total)
            def _():
                for d in fetch(i):
                    d.wait()

                def mine(t, c2):
                    m = rows(t * band, band)
                    acc_buf[i % 3, m] = h_buf[i % 2, m].astype(F32) + dot(u_buf[m, 0:half_feat], w_mine[i % 2])
                    return c2

                lax.fori_loop(0, 2, mine, 0)

            @pl.when(n >= 0)
            def _():
                other_load().wait()

                @pl.when(n >= 2)
                def _():
                    store(n - 2).wait()

                def other(t, c2):
                    m = rows(t * band, band)
                    o_buf[n % 2, m] = (acc_buf[n % 3, m] + dot(u_buf[m, half_feat:], w_other[...])).astype(BF16)
                    return c2

                lax.fori_loop(0, 2, other, 0)
                store(n).start()

            return carry

        lax.fori_loop(0, total + 2, step, 0)
        for n in (total - 2, total - 1):
            store(n).wait()

    lax.fori_loop(0, ROW_CHUNKS, own_a, 0)
    pl.run_scoped(attention, pltpu.VMEM((dim, 2 * eighth), BF16), pltpu.VMEM((dim, eighth), BF16))
    pl.run_scoped(out_phase, pltpu.VMEM((2, dim, quarter), BF16), pltpu.VMEM((2 * num_rows, shard_len, dim), BF16))
    lax.fori_loop(0, 2 * ROW_CHUNKS, b_chunk, 0)
    pl.run_scoped(gate_phase, pltpu.VMEM((2, dim, 2 * GATE_COLS), BF16))
    pl.run_scoped(
        down_phase,
        pltpu.VMEM((tokens, 2 * half_feat), BF16),
        pltpu.VMEM((2, half_feat, DOWN_COLS), BF16),
        pltpu.VMEM((half_feat, DOWN_COLS), BF16),
        pltpu.VMEM((2, tokens, DOWN_COLS), BF16),
        pltpu.VMEM((3, tokens, DOWN_COLS), F32),
        pltpu.VMEM((2, tokens, DOWN_COLS), BF16),
    )

    gain_copy.wait_send()
    for h in range(2):
        for j in range(3):
            qkv_copy(j, h).wait_send()
    for k in range(SP):
        wo_copy(k).wait_send()
    for c in range(chunks):
        for t in range(2):
            gu_copy(c, t, starts[c], sizes[c]).wait_send()
        for k in (1, 2, 3):
            u_copy(c, k, starts[c], sizes[c]).wait_send()
    for r in range(ROW_CHUNKS):
        x_copy(r).wait_send()
        for piece in (0, 2):
            act_copy(s_a, a_all, piece, r).wait_send()
            act_copy(s_b, b_all, piece, r).wait_send()

        def o_sent(h, carry):
            for k in (1, 2, 3):
                for s in range(2):
                    o_copy(h, r, k, s).wait_send()
            return carry

        lax.fori_loop(0, 2, o_sent, 0)

    def wd_sent(m, carry):
        for k in range(SP):
            wd_copy(m, k).wait_send()
        return carry

    lax.fori_loop(0, DOWN_PARTS * down_chunks, wd_sent, 0)


def tables(shard_len):
    inv_freq = np.exp(np.arange(HEAD_DIM // 2, dtype=np.float32) * np.float32(-2.0 * math.log(ROPE_THETA) / HEAD_DIM))
    pos = np.arange(shard_len)[None, :] * SP + np.arange(SP)[:, None]
    angles = (pos.astype(np.float32)[..., None] * inv_freq.astype(np.float32)).astype(np.float64)
    cos, sin = np.cos(angles), np.sin(angles)
    return (
        np.concatenate([cos, cos], axis=-1).astype(np.float32),
        np.concatenate([-sin, sin], axis=-1).astype(np.float32),
    )


def local_layer(x_loc, norm_attn, w_query, w_key, w_value, w_out, norm_mlp, w_gate, w_up, w_down):
    num_rows, shard_len, dim = x_loc.shape
    tokens = num_rows * shard_len
    half, quarter, eighth = dim // 2, dim // 4, dim // 8
    half_feat = w_down.shape[0]
    feat = half_feat // 2
    gain = jnp.zeros((8, half), F32).at[0].set(norm_attn.astype(F32)).at[1].set(norm_mlp.astype(F32))
    cos, sin = tables(shard_len)

    def buf(*shape):
        return jax.ShapeDtypeStruct(shape, BF16)

    shapes = [
        buf(tokens, dim),
        buf(tokens, dim),
        buf(SP * tokens, dim),
        buf(6, half, eighth),
        buf(SP, half, quarter),
        buf(2, half, feat),
        buf(SP, half_feat, quarter),
        buf(6 * SP, num_rows, shard_len, eighth),
        buf(2 * SP, num_rows, shard_len, eighth),
        buf(12, num_rows, shard_len, eighth),
        buf(2 * tokens, dim),
        buf(SP * tokens, dim),
        buf(SP * tokens, feat),
        buf(SP * tokens, feat),
    ]
    chunks = FULL_CHUNKS + 2
    copies = 1 + 6 + 4 + 2 * chunks + 4 * DOWN_PARTS * (quarter // DOWN_COLS) + 17 * ROW_CHUNKS + 3 * chunks
    outs = pl.pallas_call(
        layer_kernel,
        out_shape=shapes,
        in_specs=[ANY, VM] + [ANY] * 9,
        out_specs=[ANY] * len(shapes),
        scratch_shapes=[
            pltpu.VMEM((8, half), F32),
            pltpu.VMEM((SP, shard_len, HEAD_DIM), F32),
            pltpu.VMEM((SP, shard_len, HEAD_DIM), F32),
            pltpu.SemaphoreType.DMA((copies,)),
            pltpu.SemaphoreType.DMA((copies,)),
            pltpu.SemaphoreType.DMA((20,)),
        ],
        compiler_params=pltpu.CompilerParams(collective_id=0, has_side_effects=True, vmem_limit_bytes=67043328),
        name="decoder_layer",
    )(x_loc.reshape(tokens, dim), gain, w_query, w_key, w_value, w_out, w_gate, w_up, w_down, jnp.asarray(cos), jnp.asarray(sin))
    return outs[0].reshape(x_loc.shape)


def solution(mesh):
    row_spec = P(("dp", "fsdp"), "sp", None)
    weight_spec = P("fsdp", None)
    gain_spec = P("fsdp")
    in_specs = (row_spec, gain_spec, weight_spec, weight_spec, weight_spec, weight_spec, gain_spec, weight_spec, weight_spec, weight_spec)
    fn = jax.shard_map(local_layer, mesh=mesh, in_specs=in_specs, out_specs=row_spec, check_vma=False)

    def run(*args):
        with jax.sharding.use_abstract_mesh(mesh.abstract_mesh):
            return fn(*args)

    return run
```

```python
import functools
import math

import jax
import jax.numpy as jnp
import numpy as np
from jax import lax
from jax.experimental import pallas as pl
from jax.experimental.pallas import tpu as pltpu
from jax.sharding import PartitionSpec as P

HEAD_DIM = 128
NORM_EPS = 1e-5
ROPE_THETA = 5e7
MASK_VALUE = -1e30

MESH = pl.DeviceIdType.MESH
ANY = pl.BlockSpec(memory_space=pl.ANY)
VM = pl.BlockSpec(memory_space=pltpu.VMEM)
BF16 = jnp.bfloat16
F32 = jnp.float32

SP = 4
NB = 256
GATE_COLS = 384
FULL_CHUNKS = 8
DOWN_COLS = 256
DOWN_PARTS = 4
LAST_PARTS = 9
ROW_CHUNKS = 3


def dot(a, b):
    return jnp.dot(a, b, preferred_element_type=F32)


def layer_kernel(
    x, gain_attn, gain_mlp, wq, wk, wv, wo, wg, wu, wd, cos, sin,
    out, rem_attn, rem_mlp, x_got, a_all, qkv_rem, wo_rem, gu_rem, wd_rem, qkv, o_own, o_got, hid, b_all, u_own, u_got,
    gain_a, rem_a, gain_m, rem_m, cos_buf, sin_buf, send_sem, recv_sem, load_sem,
):
    tokens, dim = x.shape
    num_rows, shard_len = o_own.shape[1], o_own.shape[2]
    half, quarter, eighth = dim // 2, dim // 4, dim // 8
    feat = u_own.shape[1]
    half_feat = wd.shape[0]
    tile = tokens // ROW_CHUNKS
    tile_rows = num_rows // ROW_CHUNKS
    down_chunks = quarter // DOWN_COLS
    part_rows, last_rows = half_feat // DOWN_PARTS, half_feat // LAST_PARTS
    heads = eighth // HEAD_DIM
    rest = feat - FULL_CHUNKS * GATE_COLS
    sizes = [GATE_COLS] * FULL_CHUNKS + [rest - 128, 128]
    starts = [GATE_COLS * c for c in range(FULL_CHUNKS)] + [feat - rest, feat - 128]
    chunks = len(sizes)

    y = lax.axis_index("fsdp")
    me = lax.axis_index("sp")
    core, chip = me % 2, me // 2
    peer = [me, me + 1 - 2 * core, (me + 2) % 4, 3 - me]
    to_y = {"fsdp": 1 - y}
    to = [None] + [{"sp": peer[k]} for k in (1, 2, 3)]

    def sp_of(k):
        return 2 * ((chip + k // 2) % 2) + (core + k) % 2

    def cols(start, size):
        return pl.ds(pl.multiple_of(start, 128), size)

    def rows(start, size):
        return pl.ds(pl.multiple_of(start, 16), size)

    used = [0]

    def slots(n):
        used[0] += n
        return used[0] - n

    s_gain, s_qkv, s_wo, s_gu = slots(2), slots(6), slots(4), slots(2 * chunks)
    s_wd, s_wl = slots(4 * DOWN_PARTS * (down_chunks - 1)), slots(4 * LAST_PARTS)
    s_x, s_a, s_b = slots(ROW_CHUNKS), slots(2 * ROW_CHUNKS), slots(2 * ROW_CHUNKS)
    s_o, s_u = slots(12 * ROW_CHUNKS), slots(3 * chunks)

    def copy(slot, src, dst, dev):
        return pltpu.make_async_remote_copy(
            src_ref=src, dst_ref=dst, send_sem=send_sem.at[slot], recv_sem=recv_sem.at[slot], device_id=dev, device_id_type=MESH
        )

    def load(slot, src, dst):
        return pltpu.make_async_copy(src, dst, load_sem.at[slot])

    barrier = pltpu.get_barrier_semaphore()
    for dev in (to_y, to[1], to[2], to[3]):
        pl.semaphore_signal(barrier, inc=1, device_id=dev, device_id_type=MESH)
    pl.semaphore_wait(barrier, 4)

    def x_copy(r):
        here = rows(r * tile, tile)
        return copy(s_x + r, x.at[here], x_got.at[here], to[2])

    gain_copies = [copy(s_gain, gain_attn, rem_attn, to_y), copy(s_gain + 1, gain_mlp, rem_mlp, to_y)]

    def qkv_copy(j, h):
        part = (1 - y + h) % 2
        src = (wq, wk, wv)[j].at[:, cols(part * half + me * eighth, eighth)]
        return copy(s_qkv + 2 * j + h, src, qkv_rem.at[2 * j + h], to_y)

    def wo_copy(k):
        if k == 0:
            return copy(s_wo, wo.at[:, cols(me * quarter, quarter)], wo_rem.at[0], to_y)
        return copy(s_wo + k, wo_rem.at[2 if k == 3 else 0], wo_rem.at[k], to[2] if k == 2 else to[1])

    def gu_copy(c, t, start, size):
        src = (wg, wu)[t].at[:, cols(me * feat + start, size)]
        return copy(s_gu + 2 * c + t, src, gu_rem.at[t, :, cols(start, size)], to_y)

    def wd_copy(m, k):
        part, col = rows((m % DOWN_PARTS) * part_rows, part_rows), (m // DOWN_PARTS) * DOWN_COLS
        if k == 0:
            return copy(s_wd + 4 * m, wd.at[part, cols(me * quarter + col, DOWN_COLS)], wd_rem.at[0, part, cols(col, DOWN_COLS)], to_y)
        here = (part, cols(col, DOWN_COLS))
        return copy(s_wd + 4 * m + k, wd_rem.at[(2 if k == 3 else 0, *here)], wd_rem.at[(k, *here)], to[2] if k == 2 else to[1])

    def wl_copy(p, k):
        last = quarter - DOWN_COLS
        part = rows(p * last_rows, last_rows)
        if k == 0:
            src = wd.at[part, cols(me * quarter + last, DOWN_COLS)]
            return copy(s_wl + 4 * p, src, wd_rem.at[0, part, cols(last, DOWN_COLS)], to_y)
        here = (part, cols(last, DOWN_COLS))
        return copy(s_wl + 4 * p + k, wd_rem.at[(2 if k == 3 else 0, *here)], wd_rem.at[(k, *here)], to[2] if k == 2 else to[1])

    def act_copy(base, ref, piece, r):
        return copy(
            base + (piece // 2) * ROW_CHUNKS + r,
            ref.at[rows(piece * tokens + r * tile, tile)],
            ref.at[rows((piece + 1) * tokens + r * tile, tile)],
            to[1],
        )

    def o_copy(h, r, k, s):
        here = pl.ds(r * tile_rows, tile_rows)
        piece = k ^ (2 * s)
        return copy(
            s_o + ((h * ROW_CHUNKS + r) * 3 + k - 1) * 2 + s,
            o_own.at[4 * h + piece, here],
            o_got.at[6 * h + 2 * (k - 1) + s, here],
            to[k],
        )

    def u_copy(c, k, start, size):
        here = (pl.ds(k * tokens, tokens), cols(start, size))
        return copy(s_u + 3 * c + k - 1, u_own.at[here], u_got.at[here], to[k])

    for r in range(ROW_CHUNKS):
        x_copy(r).start()
    for d in gain_copies:
        d.start()
    for h in range(2):
        for j in range(3):
            qkv_copy(j, h).start()
    wo_copy(0).start()
    for c in range(chunks):
        for t in range(2):
            gu_copy(c, t, starts[c], sizes[c]).start()
    for m in range(DOWN_PARTS * (down_chunks - 1)):
        wd_copy(m, 0).start()
    for p in range(LAST_PARTS):
        wl_copy(p, 0).start()
    tabs = [load(0, cos, cos_buf), load(1, sin, sin_buf), load(2, gain_attn, gain_a), load(3, gain_mlp, gain_m)]
    for d in tabs:
        d.start()
    for d in gain_copies:
        d.wait_recv()
    tabs += [load(4, rem_attn, rem_a), load(5, rem_mlp, rem_m)]
    for d in tabs[4:]:
        d.start()
    for d in tabs:
        d.wait()

    def norm_chunk(src, dst, which, src_row, dst_row):
        n = tile // 3
        gm = (gain_a, gain_m)[which][...].astype(F32).reshape(1, half)
        go = (rem_a, rem_m)[which][...].astype(F32).reshape(1, half)

        def body(in_ref, out_ref):
            def sub(s, carry):
                here = pl.ds(pl.multiple_of(s * 16, 16), 16)
                mine = in_ref[here, cols(y * half, half)].astype(F32)
                other = in_ref[here, cols((1 - y) * half, half)].astype(F32)
                total = jnp.sum(mine * mine, axis=-1, keepdims=True) + jnp.sum(other * other, axis=-1, keepdims=True)
                inv = lax.rsqrt(total / dim + NORM_EPS)
                out_ref[here, 0:half] = (mine * inv * gm).astype(BF16)
                out_ref[here, half:dim] = (other * inv * go).astype(BF16)
                return carry

            lax.fori_loop(0, n // 16, sub, 0)

        pltpu.emit_pipeline(
            body,
            grid=(3,),
            in_specs=[pl.BlockSpec((n, dim), lambda t: (src_row // n + t, 0))],
            out_specs=[pl.BlockSpec((n, dim), lambda t: (dst_row // n + t, 0))],
        )(src, dst)

    def own_a(r, carry):
        norm_chunk(x, a_all, 0, r * tile, r * tile)
        act_copy(s_a, a_all, 0, r).start()
        return carry

    def got_a(r, carry):
        x_copy(r).wait_recv()
        norm_chunk(x_got, a_all, 0, r * tile, 2 * tokens + r * tile)
        act_copy(s_a, a_all, 2, r).start()
        return carry

    def attention(w_qk, w_v):
        seq = SP * shard_len
        idx = lax.broadcasted_iota(jnp.int32, (1, seq), 1)
        idq = lax.broadcasted_iota(jnp.int32, (seq, 1), 0)

        def position(i):
            piece = (i >= shard_len).astype(jnp.int32) + (i >= 2 * shard_len).astype(jnp.int32) + (i >= 3 * shard_len).astype(jnp.int32)
            chip_of = (chip + (piece >> 1)) & 1
            core_of = (core + piece) & 1
            return SP * (i - shard_len * piece) + 2 * chip_of + core_of

        def attn_body(q_ref, k_ref, v_ref, o_ref):
            keep = position(idx) <= position(idq)

            def head(h, carry):
                here = cols(h * HEAD_DIM, HEAD_DIM)
                q = q_ref[:, 0, :, here].reshape(seq, HEAD_DIM)
                k = k_ref[:, 0, :, here].reshape(seq, HEAD_DIM)
                v = v_ref[:, 0, :, here].reshape(seq, HEAD_DIM)
                s = lax.dot_general(q, k, (((1,), (1,)), ((), ())), preferred_element_type=F32) * HEAD_DIM**-0.5
                s = jnp.where(keep, s, MASK_VALUE)
                p = jnp.exp(s - jnp.max(s, axis=-1, keepdims=True))
                total = jnp.sum(p, axis=-1, keepdims=True)
                o = dot(p.astype(BF16), v) / total
                o_ref[:, 0, :, here] = o.astype(BF16).reshape(SP, shard_len, HEAD_DIM)
                return carry

            lax.fori_loop(0, heads, head, 0)

        def w_loads(j, h, dst, at):
            part = (y + h) % 2
            return [
                load(2 * j, (wq, wk, wv)[j].at[:, cols(part * half + me * eighth, eighth)], dst.at[0:half, at : at + eighth]),
                load(2 * j + 1, qkv_rem.at[2 * j + h], dst.at[half:dim, at : at + eighth]),
            ]

        def heads_half(h, carry):
            @pl.when(h == 0)
            def _():
                got_a(0, 0)

            loads = w_loads(0, h, w_qk, 0) + w_loads(1, h, w_qk, eighth)
            loads[0].start()
            loads[2].start()
            qkv_copy(0, h).wait_recv()
            loads[1].start()
            qkv_copy(1, h).wait_recv()
            loads[3].start()
            for d in loads:
                d.wait()

            def qk_side(side, c2):
                @pl.when((h == 0) & (side == 0))
                def _():
                    for r in range(ROW_CHUNKS):
                        act_copy(s_a, a_all, 0, r).wait_recv()

                @pl.when((h == 0) & (side == 1))
                def _():
                    lax.fori_loop(1, ROW_CHUNKS, got_a, 0)
                    for r in range(ROW_CHUNKS):
                        act_copy(s_a, a_all, 2, r).wait_recv()

                t0 = side * 2 * ROW_CHUNKS

                def body(a_ref, q_ref, k_ref):
                    sp = sp_of((t0 + pl.program_id(0)) // ROW_CHUNKS)
                    c_tab, s_tab = cos_buf[sp], sin_buf[sp]
                    for n in range(2 * eighth // NB):
                        acc = dot(a_ref[...], w_qk[:, n * NB : (n + 1) * NB])
                        for i in range(NB // HEAD_DIM):
                            t = acc[:, i * HEAD_DIM : (i + 1) * HEAD_DIM]
                            turned = pltpu.roll(t, HEAD_DIM // 2, 1)
                            shape = (tile_rows, shard_len, HEAD_DIM)
                            rot = t.reshape(shape) * c_tab + turned.reshape(shape) * s_tab
                            lo = n * NB + i * HEAD_DIM
                            ref = q_ref if lo < eighth else k_ref
                            lo = lo % eighth
                            ref[0, :, :, lo : lo + HEAD_DIM] = rot.astype(BF16)

                def spec(j):
                    return pl.BlockSpec(
                        (1, tile_rows, shard_len, eighth),
                        lambda t: ((2 * j + h) * SP + (t0 + t) // ROW_CHUNKS, (t0 + t) % ROW_CHUNKS, 0, 0),
                    )

                pltpu.emit_pipeline(
                    body,
                    grid=(2 * ROW_CHUNKS,),
                    in_specs=[pl.BlockSpec((tile, dim), lambda t: (t0 + t, 0))],
                    out_specs=[spec(0), spec(1)],
                )(a_all, qkv, qkv)
                return c2

            v_loads = w_loads(2, h, w_v, 0)
            v_loads[0].start()
            lax.fori_loop(0, 2, qk_side, 0)
            qkv_copy(2, h).wait_recv()
            v_loads[1].start()
            for d in v_loads:
                d.wait()

            def rows_chunk(r, c2):
                def v_body(a_ref, v_ref):
                    for lo in range(0, eighth, NB):
                        size = min(NB, eighth - lo)
                        acc = dot(a_ref[...], w_v[:, lo : lo + size])
                        v_ref[0, :, :, lo : lo + size] = acc.astype(BF16).reshape(tile_rows, shard_len, size)

                pltpu.emit_pipeline(
                    v_body,
                    grid=(SP,),
                    in_specs=[pl.BlockSpec((tile, dim), lambda t: (t * ROW_CHUNKS + r, 0))],
                    out_specs=[pl.BlockSpec((1, tile_rows, shard_len, eighth), lambda t: ((4 + h) * SP + t, r, 0, 0))],
                )(a_all, qkv)

                def spec(block):
                    return pl.BlockSpec((SP, 1, shard_len, eighth), lambda t: (block, r * tile_rows + t, 0, 0))

                pltpu.emit_pipeline(
                    attn_body,
                    grid=(tile_rows,),
                    in_specs=[spec(h), spec(2 + h), spec(4 + h)],
                    out_specs=[spec(h)],
                )(qkv, qkv, qkv, o_own)
                for k in (2, 3, 1):
                    for s in range(2):
                        o_copy(h, r, k, s).start()
                return c2

            lax.fori_loop(0, ROW_CHUNKS, rows_chunk, 0)
            return carry

        lax.fori_loop(0, 2, heads_half, 0)

    def out_phase(w_buf, o_buf):
        def fetch(k, slot):
            return [
                load(2 * slot, wo.at[:, cols(sp_of(k) * quarter, quarter)], w_buf.at[slot, 0:half]),
                load(2 * slot + 1, wo_rem.at[k], w_buf.at[slot, half:dim]),
            ]

        def o_load(h, k, s):
            src = o_own.at[4 * h + 2 * s] if k == 0 else o_got.at[6 * h + 2 * (k - 1) + s]
            dst = o_buf.at[s * num_rows : (s + 1) * num_rows, :, cols(h * half + sp_of(k) * eighth, eighth)]
            return load(4 + 8 * h + 2 * k + s, src, dst)

        loads = []

        def o_fetch(h):
            for k in (0, 1, 2, 3):
                for s in range(2):
                    if k:
                        for r in range(ROW_CHUNKS):
                            o_copy(h, r, k, s).wait_recv()
                    d = o_load(h, k, s)
                    d.start()
                    loads.append(d)

        o_fetch(0)
        wo_copy(0).wait_recv()
        wo_copy(2).start()
        wo_copy(1).start()
        for d in fetch(0, 0):
            d.start()
        o_fetch(1)
        for d in loads:
            d.wait()

        def step(k, carry):
            slot = k % 2

            @pl.when(k == 0)
            def _():
                wo_copy(1).wait_recv()
                for d in fetch(1, 1):
                    d.start()

            @pl.when(k == 2)
            def _():
                wo_copy(2).wait_recv()
                wo_copy(3).start()
                for d in fetch(2, 0):
                    d.start()

            for d in fetch(k, slot):
                d.wait()

            def run(x_ref_all, s):
                def body(x_ref, h_ref):
                    mine = pl.ds(s * num_rows + pl.program_id(0) * tile_rows, tile_rows)
                    for n in range(quarter // NB):
                        here = slice(n * NB, (n + 1) * NB)
                        lhs = o_buf[mine].reshape(tile, dim)
                        h_ref[:, here] = (x_ref[:, here].astype(F32) + dot(lhs, w_buf[slot, :, here])).astype(BF16)

                pltpu.emit_pipeline(
                    body,
                    grid=(ROW_CHUNKS,),
                    in_specs=[pl.BlockSpec((tile, quarter), lambda t: (t, sp_of(k)))],
                    out_specs=[pl.BlockSpec((tile, quarter), lambda t: (s * ROW_CHUNKS + t, sp_of(k)))],
                )(x_ref_all, hid)

            run(x, 0)

            @pl.when(k == 2)
            def _():
                wo_copy(3).wait_recv()
                for d in fetch(3, 1):
                    d.start()

            run(x_got, 1)
            return carry

        lax.fori_loop(0, SP, step, 0)

    def b_chunk(n, carry):
        s, r = n // ROW_CHUNKS, n % ROW_CHUNKS
        norm_chunk(hid, b_all, 1, n * tile, 2 * s * tokens + r * tile)
        copy(
            s_b + n,
            b_all.at[rows(2 * s * tokens + r * tile, tile)],
            b_all.at[rows((2 * s + 1) * tokens + r * tile, tile)],
            to[1],
        ).start()
        return carry

    def gate_phase(w_buf):
        def w_load(slot, start, size):
            mine = [
                load(4 * slot + t, (wg, wu)[t].at[:, cols(me * feat + start, size)], w_buf.at[slot, 0:half, t * size : (t + 1) * size])
                for t in range(2)
            ]
            other = [
                load(4 * slot + 2 + t, gu_rem.at[t, :, cols(start, size)], w_buf.at[slot, half:dim, t * size : (t + 1) * size])
                for t in range(2)
            ]
            return mine, other

        def run(c, side, slot, start, size):
            def body(b_ref, o_ref):
                parts = [dot(b_ref[...], w_buf[slot, :, n * NB : (n + 1) * NB]) for n in range(2 * size // NB)]
                both = [p[:, lo : lo + 128] for p in parts for lo in (0, 128)]
                n = size // 128
                for i in range(n):
                    o_ref[:, i * 128 : (i + 1) * 128] = (jax.nn.silu(both[i]) * both[n + i]).astype(BF16)

            n_t = 2 * ROW_CHUNKS
            pltpu.emit_pipeline(
                body,
                grid=(n_t,),
                in_specs=[pl.BlockSpec((tile, dim), lambda t: (side * n_t + t, 0))],
                out_specs=[pl.BlockSpec((tile, size), lambda t: (side * n_t + t, 0))],
            )(b_all, u_own.at[:, cols(start, size)])

            @pl.when(side == 0)
            def _():
                u_copy(c, 1, start, size).start()

            @pl.when(side == 1)
            def _():
                u_copy(c, 2, start, size).start()
                u_copy(c, 3, start, size).start()

        def chunk(c, slot, start, size, prefetch):
            mine, other = w_load(slot, start, size)
            for t in range(2):
                gu_copy(c, t, start, size).wait_recv()
            for d in other:
                d.start()
            for d in mine + other:
                d.wait()
            prefetch()

            def sides(t, carry):
                side = 1 - t

                @pl.when(c == 0)
                def _():
                    for r in range(ROW_CHUNKS):
                        n = side * ROW_CHUNKS + r
                        copy(
                            s_b + n,
                            b_all.at[rows(2 * side * tokens + r * tile, tile)],
                            b_all.at[rows((2 * side + 1) * tokens + r * tile, tile)],
                            to[1],
                        ).wait_recv()

                run(c, side, slot, start, size)
                return carry

            lax.fori_loop(0, 2, sides, 0)

        for d in w_load(0, 0, GATE_COLS)[0]:
            d.start()

        def full(c, carry):
            def prefetch():
                @pl.when(c + 1 < FULL_CHUNKS)
                def _():
                    for d in w_load((c + 1) % 2, (c + 1) * GATE_COLS, GATE_COLS)[0]:
                        d.start()

                @pl.when(c + 1 == FULL_CHUNKS)
                def _():
                    for d in w_load((c + 1) % 2, starts[FULL_CHUNKS], sizes[FULL_CHUNKS])[0]:
                        d.start()

            chunk(c, c % 2, c * GATE_COLS, GATE_COLS, prefetch)
            return carry

        lax.fori_loop(0, FULL_CHUNKS, full, 0)
        for c in range(FULL_CHUNKS, chunks):

            def prefetch(c=c):
                if c + 1 < chunks:
                    for d in w_load((c + 1) % 2, starts[c + 1], sizes[c + 1])[0]:
                        d.start()

            chunk(c, c % 2, starts[c], sizes[c], prefetch)

    def down_phase(u_buf, w_mine, w_other, h_buf, acc_buf, o_buf):
        total = SP * down_chunks
        main = total - SP
        pieces = DOWN_PARTS * (down_chunks - 1)
        band = tokens // 2

        def pass_y(m):
            @pl.when(m < pieces)
            def _():
                wd_copy(m, 0).wait_recv()
                wd_copy(m, 2).start()
                wd_copy(m, 1).start()

        def pass_x(m):
            wd_copy(m, 2).wait_recv()
            wd_copy(m, 3).start()

        def last_y(p):
            wl_copy(p, 0).wait_recv()
            wl_copy(p, 2).start()
            wl_copy(p, 1).start()

        def u_load(k):
            sp = sp_of(k)
            at = ((sp // 2 + y) % 2) * half_feat + (sp % 2) * feat
            return load(k, (u_got if k else u_own).at[pl.ds(k * tokens, tokens)], u_buf.at[:, cols(at, feat)])

        def out_cols(n):
            return cols(sp_of(n % SP) * quarter + (n // SP) * DOWN_COLS, DOWN_COLS)

        def fetch(n):
            slot = n % 2
            here = out_cols(n)
            return [load(4 + 2 * slot, wd.at[:, here], w_mine.at[slot]), load(5 + 2 * slot, hid.at[0:tokens, here], h_buf.at[slot])]

        def store(n):
            return load(8 + n % SP, o_buf.at[n % SP], out.at[:, out_cols(n)])

        def mine(n):
            @pl.when(n + 1 < total)
            def _():
                for d in fetch(n + 1):
                    d.start()

            for d in fetch(n):
                d.wait()

            def part(t, carry):
                m = rows(t * band, band)
                acc_buf[n % SP, m] = h_buf[n % 2, m].astype(F32) + dot(u_buf[m, 0:half_feat], w_mine[n % 2])
                return carry

            lax.fori_loop(0, 2, part, 0)

        for d in fetch(0):
            d.start()
        u_load(0).start()
        for k in (1, 2, 3):
            for c in range(chunks):
                u_copy(c, k, starts[c], sizes[c]).wait_recv()
            u_load(k).start()
        pass_y(0)
        pass_y(1)
        for k in range(SP):
            u_load(k).wait()

        def step(i, carry):
            n = i - 2
            c, k = n // SP, n % SP

            @pl.when((n >= 0) & (k == 0))
            def _():
                pass_x(4 * c)
                pass_y(4 * c + 2)
                pass_y(4 * c + 3)

            @pl.when((n >= 0) & (k == 1))
            def _():
                pass_x(4 * c + 1)
                pass_x(4 * c + 2)

            @pl.when((n >= 0) & (k == 2))
            def _():
                pass_y(4 * c + 4)
                pass_x(4 * c + 3)

            @pl.when((n >= 0) & (k == 3))
            def _():
                pass_y(4 * c + 5)

            @pl.when(n == main - 2)
            def _():
                last_y(0)
                last_y(1)

            @pl.when(n == main - 1)
            def _():
                last_y(2)
                last_y(3)

            for side in (1, 3):

                @pl.when((n >= 0) & (k == side))
                def _():
                    for p in range(DOWN_PARTS):
                        wd_copy(DOWN_PARTS * c + p, side).wait_recv()

            def other_load():
                return load(12, wd_rem.at[k, :, cols(c * DOWN_COLS, DOWN_COLS)], w_other)

            @pl.when(n >= 0)
            def _():
                other_load().start()

            mine(i)

            @pl.when(n >= 0)
            def _():
                other_load().wait()

                @pl.when(n >= SP)
                def _():
                    store(n - SP).wait()

                def part(t, c2):
                    m = rows(t * band, band)
                    o_buf[n % SP, m] = (acc_buf[n % SP, m] + dot(u_buf[m, half_feat:], w_other[...])).astype(BF16)
                    return c2

                lax.fori_loop(0, 2, part, 0)
                store(n).start()

            return carry

        lax.fori_loop(0, main + 2, step, 0)
        last_y(4)

        def rest_mine(n, carry):
            mine(n)

            @pl.when(n == main + 2)
            def _():
                last_y(5)

            return carry

        lax.fori_loop(main + 2, total, rest_mine, 0)
        for k in range(SP):
            store(main - SP + k).wait()

        def piece_load(k, p):
            at = rows((2 * k + p % 2) * last_rows, last_rows)
            return load(2 * k + p % 2, wd_rem.at[k, rows(p * last_rows, last_rows), cols(quarter - DOWN_COLS, DOWN_COLS)], w_other.at[at])

        def piece_dot(k, p):
            piece_load(k, p).wait()
            at = rows((2 * k + p % 2) * last_rows, last_rows)
            acc_buf[k] = acc_buf[k] + dot(u_buf[:, cols(half_feat + p * last_rows, last_rows)], w_other[at])

        def finish(k):
            o_buf[k] = acc_buf[k].astype(BF16)
            store(main + k).start()

        def first_two(p):
            wl_copy(p, 1).wait_recv()
            for k in (0, 1):
                piece_load(k, p).start()

        first_two(0)

        def last_step(p, carry):
            @pl.when(p + 6 < LAST_PARTS)
            def _():
                last_y(p + 6)

            piece_dot(0, p)
            piece_dot(1, p)

            @pl.when(p == LAST_PARTS - 1)
            def _():
                finish(0)
                finish(1)

            wl_copy(p, 2).wait_recv()
            wl_copy(p, 3).start()
            piece_load(2, p).start()

            @pl.when(p + 1 < LAST_PARTS)
            def _():
                first_two(p + 1)

            @pl.when(p > 0)
            def _():
                piece_dot(3, p - 1)

            piece_dot(2, p)

            @pl.when(p == LAST_PARTS - 1)
            def _():
                finish(2)

            wl_copy(p, 3).wait_recv()
            piece_load(3, p).start()
            return carry

        lax.fori_loop(0, LAST_PARTS, last_step, 0)
        piece_dot(3, LAST_PARTS - 1)
        finish(3)
        for k in range(SP):
            store(main + k).wait()

    lax.fori_loop(0, ROW_CHUNKS, own_a, 0)
    pl.run_scoped(attention, pltpu.VMEM((dim, 2 * eighth), BF16), pltpu.VMEM((dim, eighth), BF16))
    pl.run_scoped(out_phase, pltpu.VMEM((2, dim, quarter), BF16), pltpu.VMEM((2 * num_rows, shard_len, dim), BF16))
    lax.fori_loop(0, 2 * ROW_CHUNKS, b_chunk, 0)
    pl.run_scoped(gate_phase, pltpu.VMEM((2, dim, 2 * GATE_COLS), BF16))
    pl.run_scoped(
        down_phase,
        pltpu.VMEM((tokens, 2 * half_feat), BF16),
        pltpu.VMEM((2, half_feat, DOWN_COLS), BF16),
        pltpu.VMEM((half_feat, DOWN_COLS), BF16),
        pltpu.VMEM((2, tokens, DOWN_COLS), BF16),
        pltpu.VMEM((SP, tokens, DOWN_COLS), F32),
        pltpu.VMEM((SP, tokens, DOWN_COLS), BF16),
    )

    for d in gain_copies:
        d.wait_send()
    for h in range(2):
        for j in range(3):
            qkv_copy(j, h).wait_send()
    for k in range(SP):
        wo_copy(k).wait_send()
    for c in range(chunks):
        for t in range(2):
            gu_copy(c, t, starts[c], sizes[c]).wait_send()
        for k in (1, 2, 3):
            u_copy(c, k, starts[c], sizes[c]).wait_send()
    for r in range(ROW_CHUNKS):
        x_copy(r).wait_send()
        for piece in (0, 2):
            act_copy(s_a, a_all, piece, r).wait_send()
            act_copy(s_b, b_all, piece, r).wait_send()

        def o_sent(h, carry):
            for k in (1, 2, 3):
                for s in range(2):
                    o_copy(h, r, k, s).wait_send()
            return carry

        lax.fori_loop(0, 2, o_sent, 0)

    def wd_sent(m, carry):
        for k in range(SP):
            wd_copy(m, k).wait_send()
        return carry

    lax.fori_loop(0, DOWN_PARTS * (down_chunks - 1), wd_sent, 0)

    def wl_sent(p, carry):
        for k in range(SP):
            wl_copy(p, k).wait_send()
        return carry

    lax.fori_loop(0, LAST_PARTS, wl_sent, 0)


def tables(shard_len):
    inv_freq = np.exp(np.arange(HEAD_DIM // 2, dtype=np.float32) * np.float32(-2.0 * math.log(ROPE_THETA) / HEAD_DIM))
    pos = np.arange(shard_len)[None, :] * SP + np.arange(SP)[:, None]
    angles = (pos.astype(np.float32)[..., None] * inv_freq.astype(np.float32)).astype(np.float64)
    cos, sin = np.cos(angles), np.sin(angles)
    return (
        np.concatenate([cos, cos], axis=-1).astype(np.float32),
        np.concatenate([-sin, sin], axis=-1).astype(np.float32),
    )


def local_layer(x_loc, norm_attn, w_query, w_key, w_value, w_out, norm_mlp, w_gate, w_up, w_down):
    num_rows, shard_len, dim = x_loc.shape
    tokens = num_rows * shard_len
    half, quarter, eighth = dim // 2, dim // 4, dim // 8
    half_feat = w_down.shape[0]
    feat = half_feat // 2
    cos, sin = tables(shard_len)

    def buf(*shape):
        return jax.ShapeDtypeStruct(shape, BF16)

    shapes = [
        buf(tokens, dim),
        buf(half),
        buf(half),
        buf(tokens, dim),
        buf(SP * tokens, dim),
        buf(6, half, eighth),
        buf(SP, half, quarter),
        buf(2, half, feat),
        buf(SP, half_feat, quarter),
        buf(6 * SP, num_rows, shard_len, eighth),
        buf(2 * SP, num_rows, shard_len, eighth),
        buf(12, num_rows, shard_len, eighth),
        buf(2 * tokens, dim),
        buf(SP * tokens, dim),
        buf(SP * tokens, feat),
        buf(SP * tokens, feat),
    ]
    chunks = FULL_CHUNKS + 2
    copies = 2 + 6 + 4 + 2 * chunks + 4 * DOWN_PARTS * (quarter // DOWN_COLS - 1) + 4 * LAST_PARTS + 17 * ROW_CHUNKS + 3 * chunks
    outs = pl.pallas_call(
        layer_kernel,
        out_shape=shapes,
        in_specs=[ANY] * 12,
        out_specs=[ANY] * len(shapes),
        scratch_shapes=[
            *[pltpu.VMEM((half,), BF16)] * 4,
            pltpu.VMEM((SP, shard_len, HEAD_DIM), F32),
            pltpu.VMEM((SP, shard_len, HEAD_DIM), F32),
            pltpu.SemaphoreType.DMA((copies,)),
            pltpu.SemaphoreType.DMA((copies,)),
            pltpu.SemaphoreType.DMA((20,)),
        ],
        compiler_params=pltpu.CompilerParams(collective_id=0, has_side_effects=True, vmem_limit_bytes=67043328),
        name="decoder_layer",
    )(x_loc.reshape(tokens, dim), norm_attn, norm_mlp, w_query, w_key, w_value, w_out, w_gate, w_up, w_down, jnp.asarray(cos), jnp.asarray(sin))
    return outs[0].reshape(x_loc.shape)


def solution(mesh):
    row_spec = P(("dp", "fsdp"), "sp", None)
    weight_spec = P("fsdp", None)
    gain_spec = P("fsdp")
    in_specs = (row_spec, gain_spec, weight_spec, weight_spec, weight_spec, weight_spec, gain_spec, weight_spec, weight_spec, weight_spec)
    fn = jax.shard_map(local_layer, mesh=mesh, in_specs=in_specs, out_specs=row_spec, check_vma=False)

    def run(*args):
        with jax.sharding.use_abstract_mesh(mesh.abstract_mesh):
            return fn(*args)

    return run
```

```python
import functools
import math

import jax
import jax.numpy as jnp
import numpy as np
from jax import lax
from jax.experimental import pallas as pl
from jax.experimental.pallas import tpu as pltpu
from jax.sharding import PartitionSpec as P

HEAD_DIM = 128
NORM_EPS = 1e-5
ROPE_THETA = 5e7
MASK_VALUE = -1e30

MESH = pl.DeviceIdType.MESH
ANY = pl.BlockSpec(memory_space=pl.ANY)
VM = pl.BlockSpec(memory_space=pltpu.VMEM)
BF16 = jnp.bfloat16
F32 = jnp.float32

SP = 4
NB = 256
GATE_COLS = 384
FULL_CHUNKS = 8
DOWN_COLS = 256
DOWN_PARTS = 9
ROW_CHUNKS = 3


def dot(a, b):
    return jnp.dot(a, b, preferred_element_type=F32)


def layer_kernel(
    x, gain_attn, gain_mlp, wq, wk, wv, wo, wg, wu, wd, cos, sin,
    out, rem_attn, rem_mlp, x_got, a_all, qkv_rem, wo_rem, gu_rem, wd_rem, qkv, o_own, o_got, hid, b_all, u_own, u_got,
    gain_a, rem_a, gain_m, rem_m, cos_buf, sin_buf, send_sem, recv_sem, load_sem,
):
    tokens, dim = x.shape
    num_rows, shard_len = o_own.shape[1], o_own.shape[2]
    half, quarter, eighth = dim // 2, dim // 4, dim // 8
    feat = u_own.shape[1]
    half_feat = wd.shape[0]
    tile = tokens // ROW_CHUNKS
    tile_rows = num_rows // ROW_CHUNKS
    down_chunks = quarter // DOWN_COLS
    part_rows = half_feat // DOWN_PARTS
    heads = eighth // HEAD_DIM
    rest = feat - FULL_CHUNKS * GATE_COLS
    sizes = [GATE_COLS] * FULL_CHUNKS + [rest - 128, 128]
    starts = [GATE_COLS * c for c in range(FULL_CHUNKS)] + [feat - rest, feat - 128]
    chunks = len(sizes)

    y = lax.axis_index("fsdp")
    me = lax.axis_index("sp")
    core, chip = me % 2, me // 2
    peer = [me, me + 1 - 2 * core, (me + 2) % 4, 3 - me]
    to_y = {"fsdp": 1 - y}
    to = [None] + [{"sp": peer[k]} for k in (1, 2, 3)]

    def sp_of(k):
        return 2 * ((chip + k // 2) % 2) + (core + k) % 2

    def cols(start, size):
        return pl.ds(pl.multiple_of(start, 128), size)

    def rows(start, size):
        return pl.ds(pl.multiple_of(start, 16), size)

    used = [0]

    def slots(n):
        used[0] += n
        return used[0] - n

    s_gain, s_qkv, s_wo, s_gu = slots(2), slots(6), slots(4), slots(2 * chunks)
    s_wd = slots(4 * DOWN_PARTS * down_chunks)
    s_x, s_a, s_b = slots(ROW_CHUNKS), slots(2 * ROW_CHUNKS), slots(2 * ROW_CHUNKS)
    s_o, s_u = slots(12 * ROW_CHUNKS), slots(3 * chunks)

    def copy(slot, src, dst, dev):
        return pltpu.make_async_remote_copy(
            src_ref=src, dst_ref=dst, send_sem=send_sem.at[slot], recv_sem=recv_sem.at[slot], device_id=dev, device_id_type=MESH
        )

    def load(slot, src, dst):
        return pltpu.make_async_copy(src, dst, load_sem.at[slot])

    barrier = pltpu.get_barrier_semaphore()
    for dev in (to_y, to[1], to[2], to[3]):
        pl.semaphore_signal(barrier, inc=1, device_id=dev, device_id_type=MESH)
    pl.semaphore_wait(barrier, 4)

    def x_copy(r):
        here = rows(r * tile, tile)
        return copy(s_x + r, x.at[here], x_got.at[here], to[2])

    gain_copies = [copy(s_gain, gain_attn, rem_attn, to_y), copy(s_gain + 1, gain_mlp, rem_mlp, to_y)]

    def qkv_copy(j, h):
        part = (1 - y + h) % 2
        src = (wq, wk, wv)[j].at[:, cols(part * half + me * eighth, eighth)]
        return copy(s_qkv + 2 * j + h, src, qkv_rem.at[2 * j + h], to_y)

    def wo_copy(k):
        if k == 0:
            return copy(s_wo, wo.at[:, cols(me * quarter, quarter)], wo_rem.at[0], to_y)
        return copy(s_wo + k, wo_rem.at[2 if k == 3 else 0], wo_rem.at[k], to[2] if k == 2 else to[1])

    def gu_copy(c, t, start, size):
        src = (wg, wu)[t].at[:, cols(me * feat + start, size)]
        return copy(s_gu + 2 * c + t, src, gu_rem.at[t, :, cols(start, size)], to_y)

    def wd_copy(m, k):
        part, col = rows((m % DOWN_PARTS) * part_rows, part_rows), (m // DOWN_PARTS) * DOWN_COLS
        if k == 0:
            return copy(s_wd + 4 * m, wd.at[part, cols(me * quarter + col, DOWN_COLS)], wd_rem.at[0, part, cols(col, DOWN_COLS)], to_y)
        here = (part, cols(col, DOWN_COLS))
        return copy(s_wd + 4 * m + k, wd_rem.at[(2 if k == 3 else 0, *here)], wd_rem.at[(k, *here)], to[2] if k == 2 else to[1])

    def act_copy(base, ref, piece, r):
        return copy(
            base + (piece // 2) * ROW_CHUNKS + r,
            ref.at[rows(piece * tokens + r * tile, tile)],
            ref.at[rows((piece + 1) * tokens + r * tile, tile)],
            to[1],
        )

    def o_copy(h, r, k, s):
        here = pl.ds(r * tile_rows, tile_rows)
        piece = k ^ (2 * s)
        return copy(
            s_o + ((h * ROW_CHUNKS + r) * 3 + k - 1) * 2 + s,
            o_own.at[4 * h + piece, here],
            o_got.at[6 * h + 2 * (k - 1) + s, here],
            to[k],
        )

    def u_copy(c, k, start, size):
        here = (pl.ds(k * tokens, tokens), cols(start, size))
        return copy(s_u + 3 * c + k - 1, u_own.at[here], u_got.at[here], to[k])

    for r in range(ROW_CHUNKS):
        x_copy(r).start()
    for d in gain_copies:
        d.start()
    for h in range(2):
        for j in range(3):
            qkv_copy(j, h).start()
    wo_copy(0).start()
    for c in range(chunks):
        for t in range(2):
            gu_copy(c, t, starts[c], sizes[c]).start()
    for m in range(DOWN_PARTS * down_chunks):
        wd_copy(m, 0).start()
    tabs = [load(0, cos, cos_buf), load(1, sin, sin_buf), load(2, gain_attn, gain_a), load(3, gain_mlp, gain_m)]
    for d in tabs:
        d.start()
    for d in gain_copies:
        d.wait_recv()
    tabs += [load(4, rem_attn, rem_a), load(5, rem_mlp, rem_m)]
    for d in tabs[4:]:
        d.start()
    for d in tabs:
        d.wait()

    def norm_chunk(src, dst, which, src_row, dst_row):
        n = tile // 3
        gm = (gain_a, gain_m)[which][...].astype(F32).reshape(1, half)
        go = (rem_a, rem_m)[which][...].astype(F32).reshape(1, half)

        def body(in_ref, out_ref):
            def sub(s, carry):
                here = pl.ds(pl.multiple_of(s * 16, 16), 16)
                mine = in_ref[here, cols(y * half, half)].astype(F32)
                other = in_ref[here, cols((1 - y) * half, half)].astype(F32)
                total = jnp.sum(mine * mine, axis=-1, keepdims=True) + jnp.sum(other * other, axis=-1, keepdims=True)
                inv = lax.rsqrt(total / dim + NORM_EPS)
                out_ref[here, 0:half] = (mine * inv * gm).astype(BF16)
                out_ref[here, half:dim] = (other * inv * go).astype(BF16)
                return carry

            lax.fori_loop(0, n // 16, sub, 0)

        pltpu.emit_pipeline(
            body,
            grid=(3,),
            in_specs=[pl.BlockSpec((n, dim), lambda t: (src_row // n + t, 0))],
            out_specs=[pl.BlockSpec((n, dim), lambda t: (dst_row // n + t, 0))],
        )(src, dst)

    def own_a(r, carry):
        norm_chunk(x, a_all, 0, r * tile, r * tile)
        act_copy(s_a, a_all, 0, r).start()
        return carry

    def got_a(r, carry):
        x_copy(r).wait_recv()
        norm_chunk(x_got, a_all, 0, r * tile, 2 * tokens + r * tile)
        act_copy(s_a, a_all, 2, r).start()
        return carry

    def attention(w_qk, w_v):
        seq = SP * shard_len
        idx = lax.broadcasted_iota(jnp.int32, (1, seq), 1)
        idq = lax.broadcasted_iota(jnp.int32, (seq, 1), 0)

        def position(i):
            piece = (i >= shard_len).astype(jnp.int32) + (i >= 2 * shard_len).astype(jnp.int32) + (i >= 3 * shard_len).astype(jnp.int32)
            chip_of = (chip + (piece >> 1)) & 1
            core_of = (core + piece) & 1
            return SP * (i - shard_len * piece) + 2 * chip_of + core_of

        def attn_body(q_ref, k_ref, v_ref, o_ref):
            keep = position(idx) <= position(idq)

            def head(h, carry):
                here = cols(h * HEAD_DIM, HEAD_DIM)
                q = q_ref[:, 0, :, here].reshape(seq, HEAD_DIM)
                k = k_ref[:, 0, :, here].reshape(seq, HEAD_DIM)
                v = v_ref[:, 0, :, here].reshape(seq, HEAD_DIM)
                s = lax.dot_general(q, k, (((1,), (1,)), ((), ())), preferred_element_type=F32) * HEAD_DIM**-0.5
                s = jnp.where(keep, s, MASK_VALUE)
                p = jnp.exp(s - jnp.max(s, axis=-1, keepdims=True))
                total = jnp.sum(p, axis=-1, keepdims=True)
                o = dot(p.astype(BF16), v) / total
                o_ref[:, 0, :, here] = o.astype(BF16).reshape(SP, shard_len, HEAD_DIM)
                return carry

            lax.fori_loop(0, heads, head, 0)

        def w_loads(j, h, dst, at):
            part = (y + h) % 2
            return [
                load(2 * j, (wq, wk, wv)[j].at[:, cols(part * half + me * eighth, eighth)], dst.at[0:half, at : at + eighth]),
                load(2 * j + 1, qkv_rem.at[2 * j + h], dst.at[half:dim, at : at + eighth]),
            ]

        def heads_half(h, carry):
            @pl.when(h == 0)
            def _():
                got_a(0, 0)

            loads = w_loads(0, h, w_qk, 0) + w_loads(1, h, w_qk, eighth)
            loads[0].start()
            loads[2].start()
            qkv_copy(0, h).wait_recv()
            loads[1].start()
            qkv_copy(1, h).wait_recv()
            loads[3].start()
            for d in loads:
                d.wait()

            def qk_side(side, c2):
                @pl.when((h == 0) & (side == 0))
                def _():
                    for r in range(ROW_CHUNKS):
                        act_copy(s_a, a_all, 0, r).wait_recv()

                @pl.when((h == 0) & (side == 1))
                def _():
                    lax.fori_loop(1, ROW_CHUNKS, got_a, 0)
                    for r in range(ROW_CHUNKS):
                        act_copy(s_a, a_all, 2, r).wait_recv()

                t0 = side * 2 * ROW_CHUNKS

                def body(a_ref, q_ref, k_ref):
                    sp = sp_of((t0 + pl.program_id(0)) // ROW_CHUNKS)
                    c_tab, s_tab = cos_buf[sp], sin_buf[sp]
                    for n in range(2 * eighth // NB):
                        acc = dot(a_ref[...], w_qk[:, n * NB : (n + 1) * NB])
                        for i in range(NB // HEAD_DIM):
                            t = acc[:, i * HEAD_DIM : (i + 1) * HEAD_DIM]
                            turned = pltpu.roll(t, HEAD_DIM // 2, 1)
                            shape = (tile_rows, shard_len, HEAD_DIM)
                            rot = t.reshape(shape) * c_tab + turned.reshape(shape) * s_tab
                            lo = n * NB + i * HEAD_DIM
                            ref = q_ref if lo < eighth else k_ref
                            lo = lo % eighth
                            ref[0, :, :, lo : lo + HEAD_DIM] = rot.astype(BF16)

                def spec(j):
                    return pl.BlockSpec(
                        (1, tile_rows, shard_len, eighth),
                        lambda t: ((2 * j + h) * SP + (t0 + t) // ROW_CHUNKS, (t0 + t) % ROW_CHUNKS, 0, 0),
                    )

                pltpu.emit_pipeline(
                    body,
                    grid=(2 * ROW_CHUNKS,),
                    in_specs=[pl.BlockSpec((tile, dim), lambda t: (t0 + t, 0))],
                    out_specs=[spec(0), spec(1)],
                )(a_all, qkv, qkv)
                return c2

            v_loads = w_loads(2, h, w_v, 0)
            v_loads[0].start()
            lax.fori_loop(0, 2, qk_side, 0)
            qkv_copy(2, h).wait_recv()
            v_loads[1].start()
            for d in v_loads:
                d.wait()

            def rows_chunk(r, c2):
                def v_body(a_ref, v_ref):
                    for lo in range(0, eighth, NB):
                        size = min(NB, eighth - lo)
                        acc = dot(a_ref[...], w_v[:, lo : lo + size])
                        v_ref[0, :, :, lo : lo + size] = acc.astype(BF16).reshape(tile_rows, shard_len, size)

                pltpu.emit_pipeline(
                    v_body,
                    grid=(SP,),
                    in_specs=[pl.BlockSpec((tile, dim), lambda t: (t * ROW_CHUNKS + r, 0))],
                    out_specs=[pl.BlockSpec((1, tile_rows, shard_len, eighth), lambda t: ((4 + h) * SP + t, r, 0, 0))],
                )(a_all, qkv)

                def spec(block):
                    return pl.BlockSpec((SP, 1, shard_len, eighth), lambda t: (block, r * tile_rows + t, 0, 0))

                pltpu.emit_pipeline(
                    attn_body,
                    grid=(tile_rows,),
                    in_specs=[spec(h), spec(2 + h), spec(4 + h)],
                    out_specs=[spec(h)],
                )(qkv, qkv, qkv, o_own)
                for k in (2, 3, 1):
                    for s in range(2):
                        o_copy(h, r, k, s).start()
                return c2

            lax.fori_loop(0, ROW_CHUNKS, rows_chunk, 0)
            return carry

        lax.fori_loop(0, 2, heads_half, 0)

    def out_phase(w_buf, o_buf):
        def fetch(k, slot):
            return [
                load(2 * slot, wo.at[:, cols(sp_of(k) * quarter, quarter)], w_buf.at[slot, 0:half]),
                load(2 * slot + 1, wo_rem.at[k], w_buf.at[slot, half:dim]),
            ]

        def o_load(h, k, s):
            src = o_own.at[4 * h + 2 * s] if k == 0 else o_got.at[6 * h + 2 * (k - 1) + s]
            dst = o_buf.at[s * num_rows : (s + 1) * num_rows, :, cols(h * half + sp_of(k) * eighth, eighth)]
            return load(4 + 8 * h + 2 * k + s, src, dst)

        loads = []

        def o_fetch(h):
            for k in (0, 1, 2, 3):
                for s in range(2):
                    if k:
                        for r in range(ROW_CHUNKS):
                            o_copy(h, r, k, s).wait_recv()
                    d = o_load(h, k, s)
                    d.start()
                    loads.append(d)

        o_fetch(0)
        wo_copy(0).wait_recv()
        wo_copy(2).start()
        wo_copy(1).start()
        for d in fetch(0, 0):
            d.start()
        o_fetch(1)
        for d in loads:
            d.wait()

        def step(k, carry):
            slot = k % 2

            @pl.when(k == 0)
            def _():
                wo_copy(1).wait_recv()
                for d in fetch(1, 1):
                    d.start()

            @pl.when(k == 2)
            def _():
                wo_copy(2).wait_recv()
                wo_copy(3).start()
                for d in fetch(2, 0):
                    d.start()

            for d in fetch(k, slot):
                d.wait()

            def run(x_ref_all, s):
                def body(x_ref, h_ref):
                    mine = pl.ds(s * num_rows + pl.program_id(0) * tile_rows, tile_rows)
                    for n in range(quarter // NB):
                        here = slice(n * NB, (n + 1) * NB)
                        lhs = o_buf[mine].reshape(tile, dim)
                        h_ref[:, here] = (x_ref[:, here].astype(F32) + dot(lhs, w_buf[slot, :, here])).astype(BF16)

                pltpu.emit_pipeline(
                    body,
                    grid=(ROW_CHUNKS,),
                    in_specs=[pl.BlockSpec((tile, quarter), lambda t: (t, sp_of(k)))],
                    out_specs=[pl.BlockSpec((tile, quarter), lambda t: (s * ROW_CHUNKS + t, sp_of(k)))],
                )(x_ref_all, hid)

            run(x, 0)

            @pl.when(k == 2)
            def _():
                wo_copy(3).wait_recv()
                for d in fetch(3, 1):
                    d.start()

            run(x_got, 1)
            return carry

        lax.fori_loop(0, SP, step, 0)

    def b_chunk(n, carry):
        s, r = n // ROW_CHUNKS, n % ROW_CHUNKS
        norm_chunk(hid, b_all, 1, n * tile, 2 * s * tokens + r * tile)
        copy(
            s_b + n,
            b_all.at[rows(2 * s * tokens + r * tile, tile)],
            b_all.at[rows((2 * s + 1) * tokens + r * tile, tile)],
            to[1],
        ).start()
        return carry

    def gate_phase(w_buf):
        def w_load(slot, start, size):
            mine = [
                load(4 * slot + t, (wg, wu)[t].at[:, cols(me * feat + start, size)], w_buf.at[slot, 0:half, t * size : (t + 1) * size])
                for t in range(2)
            ]
            other = [
                load(4 * slot + 2 + t, gu_rem.at[t, :, cols(start, size)], w_buf.at[slot, half:dim, t * size : (t + 1) * size])
                for t in range(2)
            ]
            return mine, other

        def run(c, side, slot, start, size):
            def body(b_ref, o_ref):
                parts = [dot(b_ref[...], w_buf[slot, :, n * NB : (n + 1) * NB]) for n in range(2 * size // NB)]
                both = [p[:, lo : lo + 128] for p in parts for lo in (0, 128)]
                n = size // 128
                for i in range(n):
                    o_ref[:, i * 128 : (i + 1) * 128] = (jax.nn.silu(both[i]) * both[n + i]).astype(BF16)

            n_t = 2 * ROW_CHUNKS
            pltpu.emit_pipeline(
                body,
                grid=(n_t,),
                in_specs=[pl.BlockSpec((tile, dim), lambda t: (side * n_t + t, 0))],
                out_specs=[pl.BlockSpec((tile, size), lambda t: (side * n_t + t, 0))],
            )(b_all, u_own.at[:, cols(start, size)])

            @pl.when(side == 0)
            def _():
                u_copy(c, 1, start, size).start()

            @pl.when(side == 1)
            def _():
                u_copy(c, 2, start, size).start()
                u_copy(c, 3, start, size).start()

        def chunk(c, slot, start, size, prefetch):
            mine, other = w_load(slot, start, size)
            for t in range(2):
                gu_copy(c, t, start, size).wait_recv()
            for d in other:
                d.start()
            for d in mine + other:
                d.wait()
            prefetch()

            def sides(t, carry):
                side = 1 - t

                @pl.when(c == 0)
                def _():
                    for r in range(ROW_CHUNKS):
                        n = side * ROW_CHUNKS + r
                        copy(
                            s_b + n,
                            b_all.at[rows(2 * side * tokens + r * tile, tile)],
                            b_all.at[rows((2 * side + 1) * tokens + r * tile, tile)],
                            to[1],
                        ).wait_recv()

                run(c, side, slot, start, size)
                return carry

            lax.fori_loop(0, 2, sides, 0)

        for d in w_load(0, 0, GATE_COLS)[0]:
            d.start()

        def full(c, carry):
            def prefetch():
                @pl.when(c + 1 < FULL_CHUNKS)
                def _():
                    for d in w_load((c + 1) % 2, (c + 1) * GATE_COLS, GATE_COLS)[0]:
                        d.start()

                @pl.when(c + 1 == FULL_CHUNKS)
                def _():
                    for d in w_load((c + 1) % 2, starts[FULL_CHUNKS], sizes[FULL_CHUNKS])[0]:
                        d.start()

            chunk(c, c % 2, c * GATE_COLS, GATE_COLS, prefetch)
            return carry

        lax.fori_loop(0, FULL_CHUNKS, full, 0)
        for c in range(FULL_CHUNKS, chunks):

            def prefetch(c=c):
                if c + 1 < chunks:
                    for d in w_load((c + 1) % 2, starts[c + 1], sizes[c + 1])[0]:
                        d.start()

            chunk(c, c % 2, starts[c], sizes[c], prefetch)

    def down_phase(u_buf, w_mine, w_other, h_buf, acc_buf, o_buf):
        total = SP * down_chunks
        main = total - SP
        pieces = DOWN_PARTS * down_chunks
        last = pieces - DOWN_PARTS
        band = tokens // 2

        def pass_y(*ms):
            for m in ms:
                wd_copy(m, 0).wait_recv()
                wd_copy(m, 2).start()
                wd_copy(m, 1).start()

        def pass_x(*ms):
            for m in ms:
                wd_copy(m, 2).wait_recv()
                wd_copy(m, 3).start()

        def u_load(k):
            sp = sp_of(k)
            at = ((sp // 2 + y) % 2) * half_feat + (sp % 2) * feat
            return load(k, (u_got if k else u_own).at[pl.ds(k * tokens, tokens)], u_buf.at[:, cols(at, feat)])

        def out_cols(n):
            return cols(sp_of(n % SP) * quarter + (n // SP) * DOWN_COLS, DOWN_COLS)

        def fetch(n):
            slot = n % 2
            here = out_cols(n)
            return [load(4 + 2 * slot, wd.at[:, here], w_mine.at[slot]), load(5 + 2 * slot, hid.at[0:tokens, here], h_buf.at[slot])]

        def store(n):
            return load(8 + n % SP, o_buf.at[n % SP], out.at[:, out_cols(n)])

        def mine(n):
            @pl.when(n + 1 < total)
            def _():
                for d in fetch(n + 1):
                    d.start()

            for d in fetch(n):
                d.wait()

            def part(t, carry):
                m = rows(t * band, band)
                acc_buf[n % SP, m] = h_buf[n % 2, m].astype(F32) + dot(u_buf[m, 0:half_feat], w_mine[n % 2])
                return carry

            lax.fori_loop(0, 2, part, 0)

        for d in fetch(0):
            d.start()
        u_load(0).start()
        pass_y(0, 1, 2)
        for k in (1, 2, 3):
            for c in range(chunks):
                u_copy(c, k, starts[c], sizes[c]).wait_recv()
            u_load(k).start()
        pass_y(3)
        pass_x(0)
        for k in range(SP):
            u_load(k).wait()

        def step(i, carry):
            n = i - 2
            c, k = n // SP, n % SP
            j = DOWN_PARTS * c

            def other_load():
                return load(12, wd_rem.at[k, :, cols(c * DOWN_COLS, DOWN_COLS)], w_other)

            def arrived(side):
                for p in range(DOWN_PARTS):
                    wd_copy(j + p, side).wait_recv()

            @pl.when(i == 0)
            def _():
                pass_y(4)
                pass_x(1, 2)

            @pl.when(i == 1)
            def _():
                pass_y(5)
                pass_x(3)
                pass_y(6)
                pass_x(4)

            @pl.when((n >= 0) & (k == 0))
            def _():
                pass_y(j + 7)

                @pl.when(c == 0)
                def _():
                    pass_x(5)

            @pl.when((n >= 0) & (k == 1))
            def _():
                pass_x(j + 7)
                arrived(1)

            @pl.when((n >= 0) & (k == 2))
            def _():
                pass_x(j + 8)

            @pl.when((n >= 0) & (k == 3))
            def _():
                pass_x(j + 9)
                arrived(3)

            @pl.when((n >= 0) & (k > 0))
            def _():
                other_load().start()

            mine(i)

            @pl.when((n >= 0) & (k == 0))
            def _():
                pass_y(j + 8)
                other_load().start()
                pass_x(j + 6)

            @pl.when((n >= 0) & (k > 0))
            def _():
                pass_y(j + 8 + k)

            @pl.when(n >= 0)
            def _():
                other_load().wait()

                @pl.when(n >= SP)
                def _():
                    store(n - SP).wait()

                def part(t, c2):
                    m = rows(t * band, band)
                    o_buf[n % SP, m] = (acc_buf[n % SP, m] + dot(u_buf[m, half_feat:], w_other[...])).astype(BF16)
                    return c2

                lax.fori_loop(0, 2, part, 0)
                store(n).start()

            @pl.when((n >= 0) & (k == 3))
            def _():
                pass_x(j + 10)

                @pl.when(n < main - 1)
                def _():
                    for p in range(4):
                        pass_y(j + 12 + p)
                        pass_x(j + 11 + p)

            return carry

        lax.fori_loop(0, main + 2, step, 0)

        def rest_mine(n, carry):
            mine(n)
            pass_y(last + 3 + n - (main + 2))
            pass_x(last + 2 + n - (main + 2))
            return carry

        lax.fori_loop(main + 2, total, rest_mine, 0)
        for k in range(SP):
            store(main - SP + k).wait()

        def piece_load(k, p):
            at = rows((2 * k + p % 2) * part_rows, part_rows)
            return load(2 * k + p % 2, wd_rem.at[k, rows(p * part_rows, part_rows), cols(quarter - DOWN_COLS, DOWN_COLS)], w_other.at[at])

        def piece_dot(k, p):
            piece_load(k, p).wait()
            at = rows((2 * k + p % 2) * part_rows, part_rows)
            acc_buf[k] = acc_buf[k] + dot(u_buf[:, cols(half_feat + p * part_rows, part_rows)], w_other[at])

        def finish(k):
            o_buf[k] = acc_buf[k].astype(BF16)
            store(main + k).start()

        def first_two(p):
            wd_copy(last + p, 1).wait_recv()
            for k in (0, 1):
                piece_load(k, p).start()

        first_two(0)

        def last_step(p, carry):
            for at, m in ((2, 5), (4, 6), (5, 7), (6, 8)):

                @pl.when(p == at)
                def _():
                    pass_y(last + m)

            piece_dot(0, p)
            piece_dot(1, p)

            @pl.when(p == DOWN_PARTS - 1)
            def _():
                finish(0)
                finish(1)

            @pl.when(p >= 4)
            def _():
                pass_x(last + p)

            piece_load(2, p).start()

            @pl.when(p + 1 < DOWN_PARTS)
            def _():
                first_two(p + 1)

            @pl.when(p > 0)
            def _():
                piece_dot(3, p - 1)

            piece_dot(2, p)

            @pl.when(p == DOWN_PARTS - 1)
            def _():
                finish(2)

            wd_copy(last + p, 3).wait_recv()
            piece_load(3, p).start()
            return carry

        lax.fori_loop(0, DOWN_PARTS, last_step, 0)
        piece_dot(3, DOWN_PARTS - 1)
        finish(3)
        for k in range(SP):
            store(main + k).wait()

    lax.fori_loop(0, ROW_CHUNKS, own_a, 0)
    pl.run_scoped(attention, pltpu.VMEM((dim, 2 * eighth), BF16), pltpu.VMEM((dim, eighth), BF16))
    pl.run_scoped(out_phase, pltpu.VMEM((2, dim, quarter), BF16), pltpu.VMEM((2 * num_rows, shard_len, dim), BF16))
    lax.fori_loop(0, 2 * ROW_CHUNKS, b_chunk, 0)
    pl.run_scoped(gate_phase, pltpu.VMEM((2, dim, 2 * GATE_COLS), BF16))
    pl.run_scoped(
        down_phase,
        pltpu.VMEM((tokens, 2 * half_feat), BF16),
        pltpu.VMEM((2, half_feat, DOWN_COLS), BF16),
        pltpu.VMEM((half_feat, DOWN_COLS), BF16),
        pltpu.VMEM((2, tokens, DOWN_COLS), BF16),
        pltpu.VMEM((SP, tokens, DOWN_COLS), F32),
        pltpu.VMEM((SP, tokens, DOWN_COLS), BF16),
    )

    for d in gain_copies:
        d.wait_send()
    for h in range(2):
        for j in range(3):
            qkv_copy(j, h).wait_send()
    for k in range(SP):
        wo_copy(k).wait_send()
    for c in range(chunks):
        for t in range(2):
            gu_copy(c, t, starts[c], sizes[c]).wait_send()
        for k in (1, 2, 3):
            u_copy(c, k, starts[c], sizes[c]).wait_send()
    for r in range(ROW_CHUNKS):
        x_copy(r).wait_send()
        for piece in (0, 2):
            act_copy(s_a, a_all, piece, r).wait_send()
            act_copy(s_b, b_all, piece, r).wait_send()

        def o_sent(h, carry):
            for k in (1, 2, 3):
                for s in range(2):
                    o_copy(h, r, k, s).wait_send()
            return carry

        lax.fori_loop(0, 2, o_sent, 0)

    def wd_sent(m, carry):
        for k in range(SP):
            wd_copy(m, k).wait_send()
        return carry

    lax.fori_loop(0, DOWN_PARTS * down_chunks, wd_sent, 0)


def hand_over(src, dst, buf, in_sem, out_sem):
    n = src.shape[0]
    reads = [pltpu.make_async_copy(src.at[r], buf.at[r], in_sem.at[r]) for r in range(n)]
    writes = [pltpu.make_async_copy(buf.at[r], dst.at[r], out_sem.at[r]) for r in range(n)]
    for d in reads:
        d.start()
    for r in range(n):
        reads[r].wait()
        writes[r].start()
    for d in writes:
        d.wait()


def tables(shard_len):
    inv_freq = np.exp(np.arange(HEAD_DIM // 2, dtype=np.float32) * np.float32(-2.0 * math.log(ROPE_THETA) / HEAD_DIM))
    pos = np.arange(shard_len)[None, :] * SP + np.arange(SP)[:, None]
    angles = (pos.astype(np.float32)[..., None] * inv_freq.astype(np.float32)).astype(np.float64)
    cos, sin = np.cos(angles), np.sin(angles)
    return (
        np.concatenate([cos, cos], axis=-1).astype(np.float32),
        np.concatenate([-sin, sin], axis=-1).astype(np.float32),
    )


def local_layer(x_loc, norm_attn, w_query, w_key, w_value, w_out, norm_mlp, w_gate, w_up, w_down):
    num_rows, shard_len, dim = x_loc.shape
    tokens = num_rows * shard_len
    half, quarter, eighth = dim // 2, dim // 4, dim // 8
    half_feat = w_down.shape[0]
    feat = half_feat // 2
    cos, sin = tables(shard_len)

    def buf(*shape):
        return jax.ShapeDtypeStruct(shape, BF16)

    shapes = [
        buf(tokens, dim),
        buf(half),
        buf(half),
        buf(tokens, dim),
        buf(SP * tokens, dim),
        buf(6, half, eighth),
        buf(SP, half, quarter),
        buf(2, half, feat),
        buf(SP, half_feat, quarter),
        buf(6 * SP, num_rows, shard_len, eighth),
        buf(2 * SP, num_rows, shard_len, eighth),
        buf(12, num_rows, shard_len, eighth),
        buf(2 * tokens, dim),
        buf(SP * tokens, dim),
        buf(SP * tokens, feat),
        buf(SP * tokens, feat),
    ]
    chunks = FULL_CHUNKS + 2
    copies = 2 + 6 + 4 + 2 * chunks + 4 * DOWN_PARTS * (quarter // DOWN_COLS) + 17 * ROW_CHUNKS + 3 * chunks
    outs = pl.pallas_call(
        layer_kernel,
        out_shape=shapes,
        in_specs=[ANY] * 12,
        out_specs=[ANY] * len(shapes),
        scratch_shapes=[
            *[pltpu.VMEM((half,), BF16)] * 4,
            pltpu.VMEM((SP, shard_len, HEAD_DIM), F32),
            pltpu.VMEM((SP, shard_len, HEAD_DIM), F32),
            pltpu.SemaphoreType.DMA((copies,)),
            pltpu.SemaphoreType.DMA((copies,)),
            pltpu.SemaphoreType.DMA((20,)),
        ],
        compiler_params=pltpu.CompilerParams(collective_id=0, has_side_effects=True, vmem_limit_bytes=67043328),
        name="decoder_layer",
    )(x_loc.reshape(tokens, dim), norm_attn, norm_mlp, w_query, w_key, w_value, w_out, w_gate, w_up, w_down, jnp.asarray(cos), jnp.asarray(sin))
    return pl.pallas_call(
        hand_over,
        out_shape=buf(*x_loc.shape),
        in_specs=[ANY],
        out_specs=ANY,
        scratch_shapes=[
            pltpu.VMEM(x_loc.shape, BF16),
            pltpu.SemaphoreType.DMA((num_rows,)),
            pltpu.SemaphoreType.DMA((num_rows,)),
        ],
        compiler_params=pltpu.CompilerParams(vmem_limit_bytes=67043328),
        name="hand_over",
    )(outs[0].reshape(x_loc.shape))


def solution(mesh):
    row_spec = P(("dp", "fsdp"), "sp", None)
    weight_spec = P("fsdp", None)
    gain_spec = P("fsdp")
    in_specs = (row_spec, gain_spec, weight_spec, weight_spec, weight_spec, weight_spec, gain_spec, weight_spec, weight_spec, weight_spec)
    fn = jax.shard_map(local_layer, mesh=mesh, in_specs=in_specs, out_specs=row_spec, check_vma=False)

    def run(*args):
        with jax.sharding.use_abstract_mesh(mesh.abstract_mesh):
            return fn(*args)

    return run
```

```python
import functools
import math

import jax
import jax.numpy as jnp
import numpy as np
from jax import lax
from jax.experimental import pallas as pl
from jax.experimental.pallas import tpu as pltpu
from jax.sharding import PartitionSpec as P

HEAD_DIM = 128
NORM_EPS = 1e-5
ROPE_THETA = 5e7
MASK_VALUE = -1e30

MESH = pl.DeviceIdType.MESH
ANY = pl.BlockSpec(memory_space=pl.ANY)
VM = pl.BlockSpec(memory_space=pltpu.VMEM)
BF16 = jnp.bfloat16
F32 = jnp.float32

SP = 4
NB = 256
GATE_COLS = 384
FULL_CHUNKS = 8
DOWN_COLS = 256
DOWN_PARTS = 9
ROW_CHUNKS = 3


def dot(a, b):
    return jnp.dot(a, b, preferred_element_type=F32)


def layer_kernel(
    x, gain_attn, gain_mlp, wq, wk, wv, wo, wg, wu, wd, cos, sin,
    out, rem_attn, rem_mlp, x_got, a_all, qkv_rem, wo_rem, gu_rem, wd_rem, qkv, o_own, o_got, hid, b_all, u_own, u_got,
    gain_a, rem_a, gain_m, rem_m, cos_buf, sin_buf, send_sem, recv_sem, load_sem,
):
    tokens, dim = x.shape
    num_rows, shard_len = o_own.shape[1], o_own.shape[2]
    half, quarter, eighth = dim // 2, dim // 4, dim // 8
    feat = u_own.shape[1]
    half_feat = wd.shape[0]
    tile = tokens // ROW_CHUNKS
    tile_rows = num_rows // ROW_CHUNKS
    down_chunks = quarter // DOWN_COLS
    part_rows = half_feat // DOWN_PARTS
    heads = eighth // HEAD_DIM
    short = (feat - FULL_CHUNKS * GATE_COLS) // 128
    sizes = [GATE_COLS] * FULL_CHUNKS + [128] * short
    starts = [sum(sizes[:c]) for c in range(len(sizes))]
    chunks = len(sizes)

    y = lax.axis_index("fsdp")
    me = lax.axis_index("sp")
    core, chip = me % 2, me // 2
    peer = [me, me + 1 - 2 * core, (me + 2) % 4, 3 - me]
    to_y = {"fsdp": 1 - y}
    to = [None] + [{"sp": peer[k]} for k in (1, 2, 3)]

    def sp_of(k):
        return 2 * ((chip + k // 2) % 2) + (core + k) % 2

    def cols(start, size):
        return pl.ds(pl.multiple_of(start, 128), size)

    def rows(start, size):
        return pl.ds(pl.multiple_of(start, 16), size)

    used = [0]

    def slots(n):
        used[0] += n
        return used[0] - n

    s_gain, s_qkv, s_wo, s_gu = slots(2), slots(6), slots(4), slots(2 * chunks)
    s_wd = slots(4 * DOWN_PARTS * down_chunks)
    s_x, s_a, s_b = slots(ROW_CHUNKS), slots(2 * ROW_CHUNKS), slots(2 * ROW_CHUNKS)
    s_o, s_u = slots(12 * ROW_CHUNKS), slots(3 * chunks)

    def copy(slot, src, dst, dev):
        return pltpu.make_async_remote_copy(
            src_ref=src, dst_ref=dst, send_sem=send_sem.at[slot], recv_sem=recv_sem.at[slot], device_id=dev, device_id_type=MESH
        )

    def load(slot, src, dst):
        return pltpu.make_async_copy(src, dst, load_sem.at[slot])

    barrier = pltpu.get_barrier_semaphore()
    for dev in (to_y, to[1], to[2], to[3]):
        pl.semaphore_signal(barrier, inc=1, device_id=dev, device_id_type=MESH)
    pl.semaphore_wait(barrier, 4)

    def x_copy(r):
        here = rows(r * tile, tile)
        return copy(s_x + r, x.at[here], x_got.at[here], to[2])

    gain_copies = [copy(s_gain, gain_attn, rem_attn, to_y), copy(s_gain + 1, gain_mlp, rem_mlp, to_y)]

    def qkv_copy(j, h):
        part = (1 - y + h) % 2
        src = (wq, wk, wv)[j].at[:, cols(part * half + me * eighth, eighth)]
        return copy(s_qkv + 2 * j + h, src, qkv_rem.at[2 * j + h], to_y)

    def wo_copy(k):
        if k == 0:
            return copy(s_wo, wo.at[:, cols(me * quarter, quarter)], wo_rem.at[0], to_y)
        return copy(s_wo + k, wo_rem.at[2 if k == 3 else 0], wo_rem.at[k], to[2] if k == 2 else to[1])

    def gu_copy(c, t, start, size):
        src = (wg, wu)[t].at[:, cols(me * feat + start, size)]
        return copy(s_gu + 2 * c + t, src, gu_rem.at[t, :, cols(start, size)], to_y)

    def wd_copy(m, k):
        part, col = rows((m % DOWN_PARTS) * part_rows, part_rows), (m // DOWN_PARTS) * DOWN_COLS
        if k == 0:
            return copy(s_wd + 4 * m, wd.at[part, cols(me * quarter + col, DOWN_COLS)], wd_rem.at[0, part, cols(col, DOWN_COLS)], to_y)
        here = (part, cols(col, DOWN_COLS))
        return copy(s_wd + 4 * m + k, wd_rem.at[(2 if k == 3 else 0, *here)], wd_rem.at[(k, *here)], to[2] if k == 2 else to[1])

    def act_copy(base, ref, piece, r):
        return copy(
            base + (piece // 2) * ROW_CHUNKS + r,
            ref.at[rows(piece * tokens + r * tile, tile)],
            ref.at[rows((piece + 1) * tokens + r * tile, tile)],
            to[1],
        )

    def o_copy(h, r, k, s):
        here = pl.ds(r * tile_rows, tile_rows)
        piece = k ^ (2 * s)
        return copy(
            s_o + ((h * ROW_CHUNKS + r) * 3 + k - 1) * 2 + s,
            o_own.at[4 * h + piece, here],
            o_got.at[6 * h + 2 * (k - 1) + s, here],
            to[k],
        )

    def u_copy(c, k, start, size):
        here = (pl.ds(k * tokens, tokens), cols(start, size))
        return copy(s_u + 3 * c + k - 1, u_own.at[here], u_got.at[here], to[k])

    def pass_y(*ms):
        for m in ms:
            wd_copy(m, 0).wait_recv()
            wd_copy(m, 2).start()
            wd_copy(m, 1).start()

    def pass_x(*ms):
        for m in ms:
            wd_copy(m, 2).wait_recv()
            wd_copy(m, 3).start()

    for r in range(ROW_CHUNKS):
        x_copy(r).start()
    for d in gain_copies:
        d.start()
    for h in range(2):
        for j in range(3):
            qkv_copy(j, h).start()
    wo_copy(0).start()
    for c in range(chunks):
        if c == FULL_CHUNKS:
            for m in range(DOWN_PARTS):
                wd_copy(m, 0).start()
        for t in range(2):
            gu_copy(c, t, starts[c], sizes[c]).start()
    for m in range(DOWN_PARTS, DOWN_PARTS * down_chunks):
        wd_copy(m, 0).start()
    tabs = [load(0, cos, cos_buf), load(1, sin, sin_buf), load(2, gain_attn, gain_a), load(3, gain_mlp, gain_m)]
    for d in tabs:
        d.start()
    for d in gain_copies:
        d.wait_recv()
    tabs += [load(4, rem_attn, rem_a), load(5, rem_mlp, rem_m)]
    for d in tabs[4:]:
        d.start()
    for d in tabs:
        d.wait()

    def norm_chunk(src, dst, which, src_row, dst_row):
        n = tile // 3
        gm = (gain_a, gain_m)[which][...].astype(F32).reshape(1, half)
        go = (rem_a, rem_m)[which][...].astype(F32).reshape(1, half)

        def body(in_ref, out_ref):
            def sub(s, carry):
                here = pl.ds(pl.multiple_of(s * 16, 16), 16)
                mine = in_ref[here, cols(y * half, half)].astype(F32)
                other = in_ref[here, cols((1 - y) * half, half)].astype(F32)
                total = jnp.sum(mine * mine, axis=-1, keepdims=True) + jnp.sum(other * other, axis=-1, keepdims=True)
                inv = lax.rsqrt(total / dim + NORM_EPS)
                out_ref[here, 0:half] = (mine * inv * gm).astype(BF16)
                out_ref[here, half:dim] = (other * inv * go).astype(BF16)
                return carry

            lax.fori_loop(0, n // 16, sub, 0)

        pltpu.emit_pipeline(
            body,
            grid=(3,),
            in_specs=[pl.BlockSpec((n, dim), lambda t: (src_row // n + t, 0))],
            out_specs=[pl.BlockSpec((n, dim), lambda t: (dst_row // n + t, 0))],
        )(src, dst)

    def own_a(r, carry):
        norm_chunk(x, a_all, 0, r * tile, r * tile)
        act_copy(s_a, a_all, 0, r).start()
        return carry

    def got_a(r, carry):
        x_copy(r).wait_recv()
        norm_chunk(x_got, a_all, 0, r * tile, 2 * tokens + r * tile)
        act_copy(s_a, a_all, 2, r).start()
        return carry

    def attention(w_qk, w_v):
        seq = SP * shard_len
        idx = lax.broadcasted_iota(jnp.int32, (1, seq), 1)
        idq = lax.broadcasted_iota(jnp.int32, (seq, 1), 0)

        def position(i):
            piece = (i >= shard_len).astype(jnp.int32) + (i >= 2 * shard_len).astype(jnp.int32) + (i >= 3 * shard_len).astype(jnp.int32)
            chip_of = (chip + (piece >> 1)) & 1
            core_of = (core + piece) & 1
            return SP * (i - shard_len * piece) + 2 * chip_of + core_of

        def attn_body(q_ref, k_ref, v_ref, o_ref):
            keep = position(idx) <= position(idq)

            def head(h, carry):
                here = cols(h * HEAD_DIM, HEAD_DIM)
                q = q_ref[:, 0, :, here].reshape(seq, HEAD_DIM)
                k = k_ref[:, 0, :, here].reshape(seq, HEAD_DIM)
                v = v_ref[:, 0, :, here].reshape(seq, HEAD_DIM)
                s = lax.dot_general(q, k, (((1,), (1,)), ((), ())), preferred_element_type=F32) * HEAD_DIM**-0.5
                s = jnp.where(keep, s, MASK_VALUE)
                p = jnp.exp(s - jnp.max(s, axis=-1, keepdims=True))
                total = jnp.sum(p, axis=-1, keepdims=True)
                o = dot(p.astype(BF16), v) / total
                o_ref[:, 0, :, here] = o.astype(BF16).reshape(SP, shard_len, HEAD_DIM)
                return carry

            lax.fori_loop(0, heads, head, 0)

        def w_loads(j, h, dst, at):
            part = (y + h) % 2
            return [
                load(2 * j, (wq, wk, wv)[j].at[:, cols(part * half + me * eighth, eighth)], dst.at[0:half, at : at + eighth]),
                load(2 * j + 1, qkv_rem.at[2 * j + h], dst.at[half:dim, at : at + eighth]),
            ]

        def heads_half(h, carry):
            @pl.when(h == 0)
            def _():
                got_a(0, 0)

            loads = w_loads(0, h, w_qk, 0) + w_loads(1, h, w_qk, eighth)
            loads[0].start()
            loads[2].start()
            qkv_copy(0, h).wait_recv()
            loads[1].start()
            qkv_copy(1, h).wait_recv()
            loads[3].start()
            for d in loads:
                d.wait()

            def qk_side(side, c2):
                @pl.when((h == 0) & (side == 0))
                def _():
                    for r in range(ROW_CHUNKS):
                        act_copy(s_a, a_all, 0, r).wait_recv()

                @pl.when((h == 0) & (side == 1))
                def _():
                    lax.fori_loop(1, ROW_CHUNKS, got_a, 0)
                    for r in range(ROW_CHUNKS):
                        act_copy(s_a, a_all, 2, r).wait_recv()

                t0 = side * 2 * ROW_CHUNKS

                def body(a_ref, q_ref, k_ref):
                    sp = sp_of((t0 + pl.program_id(0)) // ROW_CHUNKS)
                    c_tab, s_tab = cos_buf[sp], sin_buf[sp]
                    for n in range(2 * eighth // NB):
                        acc = dot(a_ref[...], w_qk[:, n * NB : (n + 1) * NB])
                        for i in range(NB // HEAD_DIM):
                            t = acc[:, i * HEAD_DIM : (i + 1) * HEAD_DIM]
                            turned = pltpu.roll(t, HEAD_DIM // 2, 1)
                            shape = (tile_rows, shard_len, HEAD_DIM)
                            rot = t.reshape(shape) * c_tab + turned.reshape(shape) * s_tab
                            lo = n * NB + i * HEAD_DIM
                            ref = q_ref if lo < eighth else k_ref
                            lo = lo % eighth
                            ref[0, :, :, lo : lo + HEAD_DIM] = rot.astype(BF16)

                def spec(j):
                    return pl.BlockSpec(
                        (1, tile_rows, shard_len, eighth),
                        lambda t: ((2 * j + h) * SP + (t0 + t) // ROW_CHUNKS, (t0 + t) % ROW_CHUNKS, 0, 0),
                    )

                pltpu.emit_pipeline(
                    body,
                    grid=(2 * ROW_CHUNKS,),
                    in_specs=[pl.BlockSpec((tile, dim), lambda t: (t0 + t, 0))],
                    out_specs=[spec(0), spec(1)],
                )(a_all, qkv, qkv)
                return c2

            v_loads = w_loads(2, h, w_v, 0)
            v_loads[0].start()
            lax.fori_loop(0, 2, qk_side, 0)
            qkv_copy(2, h).wait_recv()
            v_loads[1].start()
            for d in v_loads:
                d.wait()

            def rows_chunk(r, c2):
                def v_body(a_ref, v_ref):
                    for lo in range(0, eighth, NB):
                        size = min(NB, eighth - lo)
                        acc = dot(a_ref[...], w_v[:, lo : lo + size])
                        v_ref[0, :, :, lo : lo + size] = acc.astype(BF16).reshape(tile_rows, shard_len, size)

                pltpu.emit_pipeline(
                    v_body,
                    grid=(SP,),
                    in_specs=[pl.BlockSpec((tile, dim), lambda t: (t * ROW_CHUNKS + r, 0))],
                    out_specs=[pl.BlockSpec((1, tile_rows, shard_len, eighth), lambda t: ((4 + h) * SP + t, r, 0, 0))],
                )(a_all, qkv)

                def spec(block):
                    return pl.BlockSpec((SP, 1, shard_len, eighth), lambda t: (block, r * tile_rows + t, 0, 0))

                pltpu.emit_pipeline(
                    attn_body,
                    grid=(tile_rows,),
                    in_specs=[spec(h), spec(2 + h), spec(4 + h)],
                    out_specs=[spec(h)],
                )(qkv, qkv, qkv, o_own)
                for k in (2, 3, 1):
                    for s in range(2):
                        o_copy(h, r, k, s).start()
                return c2

            lax.fori_loop(0, ROW_CHUNKS, rows_chunk, 0)
            return carry

        lax.fori_loop(0, 2, heads_half, 0)

    def out_phase(w_buf, o_buf):
        def fetch(k, slot):
            return [
                load(2 * slot, wo.at[:, cols(sp_of(k) * quarter, quarter)], w_buf.at[slot, 0:half]),
                load(2 * slot + 1, wo_rem.at[k], w_buf.at[slot, half:dim]),
            ]

        def o_load(h, k, s):
            src = o_own.at[4 * h + 2 * s] if k == 0 else o_got.at[6 * h + 2 * (k - 1) + s]
            dst = o_buf.at[s * num_rows : (s + 1) * num_rows, :, cols(h * half + sp_of(k) * eighth, eighth)]
            return load(4 + 8 * h + 2 * k + s, src, dst)

        loads = []

        def o_fetch(h):
            for k in (0, 1, 2, 3):
                for s in range(2):
                    if k:
                        for r in range(ROW_CHUNKS):
                            o_copy(h, r, k, s).wait_recv()
                    d = o_load(h, k, s)
                    d.start()
                    loads.append(d)

        o_fetch(0)
        wo_copy(0).wait_recv()
        wo_copy(2).start()
        wo_copy(1).start()
        for d in fetch(0, 0):
            d.start()
        o_fetch(1)
        for d in loads:
            d.wait()

        def step(k, carry):
            slot = k % 2

            @pl.when(k == 0)
            def _():
                wo_copy(1).wait_recv()
                for d in fetch(1, 1):
                    d.start()

            @pl.when(k == 2)
            def _():
                wo_copy(2).wait_recv()
                wo_copy(3).start()
                for d in fetch(2, 0):
                    d.start()

            for d in fetch(k, slot):
                d.wait()

            def run(x_ref_all, s):
                def body(x_ref, h_ref):
                    mine = pl.ds(s * num_rows + pl.program_id(0) * tile_rows, tile_rows)
                    for n in range(quarter // NB):
                        here = slice(n * NB, (n + 1) * NB)
                        lhs = o_buf[mine].reshape(tile, dim)
                        h_ref[:, here] = (x_ref[:, here].astype(F32) + dot(lhs, w_buf[slot, :, here])).astype(BF16)

                pltpu.emit_pipeline(
                    body,
                    grid=(ROW_CHUNKS,),
                    in_specs=[pl.BlockSpec((tile, quarter), lambda t: (t, sp_of(k)))],
                    out_specs=[pl.BlockSpec((tile, quarter), lambda t: (s * ROW_CHUNKS + t, sp_of(k)))],
                )(x_ref_all, hid)

            run(x, 0)

            @pl.when(k == 2)
            def _():
                wo_copy(3).wait_recv()
                for d in fetch(3, 1):
                    d.start()

            run(x_got, 1)
            return carry

        lax.fori_loop(0, SP, step, 0)

    def b_chunk(n, carry):
        s, r = n // ROW_CHUNKS, n % ROW_CHUNKS
        norm_chunk(hid, b_all, 1, n * tile, 2 * s * tokens + r * tile)
        copy(
            s_b + n,
            b_all.at[rows(2 * s * tokens + r * tile, tile)],
            b_all.at[rows((2 * s + 1) * tokens + r * tile, tile)],
            to[1],
        ).start()
        return carry

    def gate_phase(w_buf):
        def w_load(slot, start, size):
            mine = [
                load(4 * slot + t, (wg, wu)[t].at[:, cols(me * feat + start, size)], w_buf.at[slot, 0:half, t * size : (t + 1) * size])
                for t in range(2)
            ]
            other = [
                load(4 * slot + 2 + t, gu_rem.at[t, :, cols(start, size)], w_buf.at[slot, half:dim, t * size : (t + 1) * size])
                for t in range(2)
            ]
            return mine, other

        def run(c, side, slot, start, size):
            def body(b_ref, o_ref):
                parts = [dot(b_ref[...], w_buf[slot, :, n * NB : (n + 1) * NB]) for n in range(2 * size // NB)]
                both = [p[:, lo : lo + 128] for p in parts for lo in (0, 128)]
                n = size // 128
                for i in range(n):
                    o_ref[:, i * 128 : (i + 1) * 128] = (jax.nn.silu(both[i]) * both[n + i]).astype(BF16)

            n_t = 2 * ROW_CHUNKS
            pltpu.emit_pipeline(
                body,
                grid=(n_t,),
                in_specs=[pl.BlockSpec((tile, dim), lambda t: (side * n_t + t, 0))],
                out_specs=[pl.BlockSpec((tile, size), lambda t: (side * n_t + t, 0))],
            )(b_all, u_own.at[:, cols(start, size)])

            @pl.when(side == 0)
            def _():
                u_copy(c, 1, start, size).start()

            @pl.when(side == 1)
            def _():
                u_copy(c, 2, start, size).start()
                u_copy(c, 3, start, size).start()

        def chunk(c, slot, start, size, prefetch, before, middle, after):
            before()
            mine, other = w_load(slot, start, size)
            for t in range(2):
                gu_copy(c, t, start, size).wait_recv()
            for d in other:
                d.start()
            for d in mine + other:
                d.wait()
            prefetch()

            def sides(t, carry):
                side = 1 - t

                @pl.when(c == 0)
                def _():
                    for r in range(ROW_CHUNKS):
                        n = side * ROW_CHUNKS + r
                        copy(
                            s_b + n,
                            b_all.at[rows(2 * side * tokens + r * tile, tile)],
                            b_all.at[rows((2 * side + 1) * tokens + r * tile, tile)],
                            to[1],
                        ).wait_recv()

                @pl.when(side == 0)
                def _():
                    middle()

                run(c, side, slot, start, size)
                return carry

            lax.fori_loop(0, 2, sides, 0)
            after()

        def at(c, n, work):
            @pl.when(c == n)
            def _():
                work()

        for d in w_load(0, 0, GATE_COLS)[0]:
            d.start()

        def full(c, carry):
            def prefetch():
                @pl.when(c + 1 < FULL_CHUNKS)
                def _():
                    for d in w_load((c + 1) % 2, (c + 1) * GATE_COLS, GATE_COLS)[0]:
                        d.start()

                @pl.when(c + 1 == FULL_CHUNKS)
                def _():
                    for d in w_load((c + 1) % 2, starts[FULL_CHUNKS], 128)[0]:
                        d.start()

            def before():
                at(c, FULL_CHUNKS - 1, lambda: pass_y(0, 1))

            def middle():
                at(c, FULL_CHUNKS - 1, lambda: (pass_y(2, 3, 4), pass_x(0)))

            def after():
                at(c, FULL_CHUNKS - 1, lambda: (pass_y(5, 6, 7), pass_x(1)))

            chunk(c, c % 2, c * GATE_COLS, GATE_COLS, prefetch, before, middle, after)
            return carry

        lax.fori_loop(0, FULL_CHUNKS, full, 0)

        def brief(c, carry):
            def start_of(i):
                return starts[FULL_CHUNKS] + (i - FULL_CHUNKS) * 128

            def prefetch():
                @pl.when(c + 1 < chunks)
                def _():
                    for d in w_load((c + 1) % 2, start_of(c + 1), 128)[0]:
                        d.start()

            def before():
                at(c, FULL_CHUNKS, lambda: pass_y(8))
                at(c, FULL_CHUNKS + 1, lambda: pass_x(4))
                at(c, FULL_CHUNKS + 2, lambda: pass_x(6))

            def middle():
                at(c, FULL_CHUNKS, lambda: pass_x(2, 3))
                at(c, FULL_CHUNKS + 1, lambda: pass_x(5))
                at(c, FULL_CHUNKS + 2, lambda: (pass_y(9), pass_x(7)))

            chunk(c, c % 2, start_of(c), 128, prefetch, before, middle, lambda: None)
            return carry

        lax.fori_loop(FULL_CHUNKS, chunks, brief, 0)

    def down_phase(u_buf, w_mine, w_other, h_buf, acc_buf, o_buf):
        total = SP * down_chunks
        main = total - SP
        pieces = DOWN_PARTS * down_chunks
        last = pieces - DOWN_PARTS
        band = tokens // 2

        def u_load(k):
            sp = sp_of(k)
            at = ((sp // 2 + y) % 2) * half_feat + (sp % 2) * feat
            return load(k, (u_got if k else u_own).at[pl.ds(k * tokens, tokens)], u_buf.at[:, cols(at, feat)])

        def out_cols(n):
            return cols(sp_of(n % SP) * quarter + (n // SP) * DOWN_COLS, DOWN_COLS)

        def fetch(n):
            slot = n % 2
            here = out_cols(n)
            return [load(4 + 2 * slot, wd.at[:, here], w_mine.at[slot]), load(5 + 2 * slot, hid.at[0:tokens, here], h_buf.at[slot])]

        def store(n):
            return load(8 + n % 2, o_buf.at[n % 2], out.at[:, out_cols(n)])

        def mine(n):
            @pl.when(n + 1 < total)
            def _():
                for d in fetch(n + 1):
                    d.start()

            for d in fetch(n):
                d.wait()

            def part(t, carry):
                m = rows(t * band, band)
                acc_buf[n % SP, m] = h_buf[n % 2, m].astype(F32) + dot(u_buf[m, 0:half_feat], w_mine[n % 2])
                return carry

            lax.fori_loop(0, 2, part, 0)

        for d in fetch(0):
            d.start()
        u_load(0).start()
        pass_y(10, 11)
        pass_x(8)
        for k in (1, 2, 3):
            for c in range(chunks):
                u_copy(c, k, starts[c], sizes[c]).wait_recv()
            u_load(k).start()
        for k in range(SP):
            u_load(k).wait()

        def other(n):
            c, k = n // SP, n % SP
            ready = load(12, wd_rem.at[k, :, cols(c * DOWN_COLS, DOWN_COLS)], w_other)
            for side in (1, 3):

                @pl.when(k == side)
                def _():
                    for p in range(DOWN_PARTS):
                        wd_copy(DOWN_PARTS * c + p, side).wait_recv()

            ready.start()

            @pl.when(n >= 2)
            def _():
                store(n - 2).wait()

            ready.wait()

            def part(t, carry):
                m = rows(t * band, band)
                o_buf[k % 2, m] = (acc_buf[k, m] + dot(u_buf[m, half_feat:], w_other[...])).astype(BF16)
                return carry

            lax.fori_loop(0, 2, part, 0)
            store(n).start()

        def first(n, carry):
            @pl.when(n < 5)
            def _():
                pass_y(12 + n)
                pass_x(9 + n)

            @pl.when(n == 6)
            def _():
                pass_y(17)
                pass_x(14)

            mine(n)

            @pl.when(n < SP)
            def _():
                other(n)

            return carry

        def slot(m, carry):
            c, r = (m - 8) // 9, (m - 8) % 9
            pass_y(m + 1)
            pass_x(m - 2)
            two = 2 * (r // 3)

            @pl.when((r == 0) | (r == 3))
            def _():
                def run(k, c2):
                    other(SP * c + two + k)
                    return c2

                lax.fori_loop(0, 2, run, 0)

            @pl.when((r == 1) | (r == 4))
            def _():
                def run(k, c2):
                    mine(SP * (c + 1) + two + k)
                    return c2

                lax.fori_loop(0, 2, run, 0)

            return carry

        lax.fori_loop(0, 2 * SP, first, 0)
        if down_chunks > 2:
            lax.fori_loop(2 * DOWN_PARTS - 1, last + 4, slot, 0)
        next_y, next_x = (5, 2) if down_chunks > 2 else (9, 6)

        def piece_load(k, p):
            at = rows((2 * k + p % 2) * part_rows, part_rows)
            return load(2 * k + p % 2, wd_rem.at[k, rows(p * part_rows, part_rows), cols(quarter - DOWN_COLS, DOWN_COLS)], w_other.at[at])

        def piece_dot(k, p):
            piece_load(k, p).wait()
            at = rows((2 * k + p % 2) * part_rows, part_rows)
            acc_buf[k] = acc_buf[k] + dot(u_buf[:, cols(half_feat + p * part_rows, part_rows)], w_other[at])

        def finish(k):
            store(main + k - 2).wait()
            o_buf[k % 2] = acc_buf[k].astype(BF16)
            store(main + k).start()

        def first_two(p):
            wd_copy(last + p, 1).wait_recv()
            for k in (0, 1):
                piece_load(k, p).start()

        first_two(0)

        def last_step(p, carry):
            @pl.when(p + next_y < DOWN_PARTS)
            def _():
                pass_y(last + next_y + p)

            piece_dot(0, p)
            piece_dot(1, p)

            @pl.when(p == DOWN_PARTS - 1)
            def _():
                finish(0)
                finish(1)

            @pl.when(p >= next_x)
            def _():
                pass_x(last + p)

            piece_load(2, p).start()

            @pl.when(p + 1 < DOWN_PARTS)
            def _():
                first_two(p + 1)

            @pl.when(p > 0)
            def _():
                piece_dot(3, p - 1)

            piece_dot(2, p)

            @pl.when(p == DOWN_PARTS - 1)
            def _():
                finish(2)

            wd_copy(last + p, 3).wait_recv()
            piece_load(3, p).start()
            return carry

        lax.fori_loop(0, DOWN_PARTS, last_step, 0)
        piece_dot(3, DOWN_PARTS - 1)
        finish(3)
        for k in (2, 3):
            store(main + k).wait()

    lax.fori_loop(0, ROW_CHUNKS, own_a, 0)
    pl.run_scoped(attention, pltpu.VMEM((dim, 2 * eighth), BF16), pltpu.VMEM((dim, eighth), BF16))
    pl.run_scoped(out_phase, pltpu.VMEM((2, dim, quarter), BF16), pltpu.VMEM((2 * num_rows, shard_len, dim), BF16))
    lax.fori_loop(0, 2 * ROW_CHUNKS, b_chunk, 0)
    pl.run_scoped(gate_phase, pltpu.VMEM((2, dim, 2 * GATE_COLS), BF16))
    pl.run_scoped(
        down_phase,
        pltpu.VMEM((tokens, 2 * half_feat), BF16),
        pltpu.VMEM((2, half_feat, DOWN_COLS), BF16),
        pltpu.VMEM((half_feat, DOWN_COLS), BF16),
        pltpu.VMEM((2, tokens, DOWN_COLS), BF16),
        pltpu.VMEM((SP, tokens, DOWN_COLS), F32),
        pltpu.VMEM((2, tokens, DOWN_COLS), BF16),
    )

    for d in gain_copies:
        d.wait_send()
    for h in range(2):
        for j in range(3):
            qkv_copy(j, h).wait_send()
    for k in range(SP):
        wo_copy(k).wait_send()
    for c in range(chunks):
        for t in range(2):
            gu_copy(c, t, starts[c], sizes[c]).wait_send()
        for k in (1, 2, 3):
            u_copy(c, k, starts[c], sizes[c]).wait_send()
    for r in range(ROW_CHUNKS):
        x_copy(r).wait_send()
        for piece in (0, 2):
            act_copy(s_a, a_all, piece, r).wait_send()
            act_copy(s_b, b_all, piece, r).wait_send()

        def o_sent(h, carry):
            for k in (1, 2, 3):
                for s in range(2):
                    o_copy(h, r, k, s).wait_send()
            return carry

        lax.fori_loop(0, 2, o_sent, 0)

    def wd_sent(m, carry):
        for k in range(SP):
            wd_copy(m, k).wait_send()
        return carry

    lax.fori_loop(0, DOWN_PARTS * down_chunks, wd_sent, 0)


def hand_over(src, dst, buf, in_sem, out_sem):
    n = src.shape[0]
    reads = [pltpu.make_async_copy(src.at[r], buf.at[r], in_sem.at[r]) for r in range(n)]
    writes = [pltpu.make_async_copy(buf.at[r], dst.at[r], out_sem.at[r]) for r in range(n)]
    for d in reads:
        d.start()
    for r in range(n):
        reads[r].wait()
        writes[r].start()
    for d in writes:
        d.wait()


def tables(shard_len):
    inv_freq = np.exp(np.arange(HEAD_DIM // 2, dtype=np.float32) * np.float32(-2.0 * math.log(ROPE_THETA) / HEAD_DIM))
    pos = np.arange(shard_len)[None, :] * SP + np.arange(SP)[:, None]
    angles = (pos.astype(np.float32)[..., None] * inv_freq.astype(np.float32)).astype(np.float64)
    cos, sin = np.cos(angles), np.sin(angles)
    return (
        np.concatenate([cos, cos], axis=-1).astype(np.float32),
        np.concatenate([-sin, sin], axis=-1).astype(np.float32),
    )


def local_layer(x_loc, norm_attn, w_query, w_key, w_value, w_out, norm_mlp, w_gate, w_up, w_down):
    num_rows, shard_len, dim = x_loc.shape
    tokens = num_rows * shard_len
    half, quarter, eighth = dim // 2, dim // 4, dim // 8
    half_feat = w_down.shape[0]
    feat = half_feat // 2
    cos, sin = tables(shard_len)

    def buf(*shape):
        return jax.ShapeDtypeStruct(shape, BF16)

    shapes = [
        buf(tokens, dim),
        buf(half),
        buf(half),
        buf(tokens, dim),
        buf(SP * tokens, dim),
        buf(6, half, eighth),
        buf(SP, half, quarter),
        buf(2, half, feat),
        buf(SP, half_feat, quarter),
        buf(6 * SP, num_rows, shard_len, eighth),
        buf(2 * SP, num_rows, shard_len, eighth),
        buf(12, num_rows, shard_len, eighth),
        buf(2 * tokens, dim),
        buf(SP * tokens, dim),
        buf(SP * tokens, feat),
        buf(SP * tokens, feat),
    ]
    chunks = FULL_CHUNKS + (feat - FULL_CHUNKS * GATE_COLS) // 128
    copies = 2 + 6 + 4 + 2 * chunks + 4 * DOWN_PARTS * (quarter // DOWN_COLS) + 17 * ROW_CHUNKS + 3 * chunks
    outs = pl.pallas_call(
        layer_kernel,
        out_shape=shapes,
        in_specs=[ANY] * 12,
        out_specs=[ANY] * len(shapes),
        scratch_shapes=[
            *[pltpu.VMEM((half,), BF16)] * 4,
            pltpu.VMEM((SP, shard_len, HEAD_DIM), F32),
            pltpu.VMEM((SP, shard_len, HEAD_DIM), F32),
            pltpu.SemaphoreType.DMA((copies,)),
            pltpu.SemaphoreType.DMA((copies,)),
            pltpu.SemaphoreType.DMA((20,)),
        ],
        compiler_params=pltpu.CompilerParams(collective_id=0, has_side_effects=True, vmem_limit_bytes=67043328),
        name="decoder_layer",
    )(x_loc.reshape(tokens, dim), norm_attn, norm_mlp, w_query, w_key, w_value, w_out, w_gate, w_up, w_down, jnp.asarray(cos), jnp.asarray(sin))
    return pl.pallas_call(
        hand_over,
        out_shape=buf(*x_loc.shape),
        in_specs=[ANY],
        out_specs=ANY,
        scratch_shapes=[
            pltpu.VMEM(x_loc.shape, BF16),
            pltpu.SemaphoreType.DMA((num_rows,)),
            pltpu.SemaphoreType.DMA((num_rows,)),
        ],
        compiler_params=pltpu.CompilerParams(vmem_limit_bytes=67043328),
        name="hand_over",
    )(outs[0].reshape(x_loc.shape))


def solution(mesh):
    row_spec = P(("dp", "fsdp"), "sp", None)
    weight_spec = P("fsdp", None)
    gain_spec = P("fsdp")
    in_specs = (row_spec, gain_spec, weight_spec, weight_spec, weight_spec, weight_spec, gain_spec, weight_spec, weight_spec, weight_spec)
    fn = jax.shard_map(local_layer, mesh=mesh, in_specs=in_specs, out_specs=row_spec, check_vma=False)

    def run(*args):
        with jax.sharding.use_abstract_mesh(mesh.abstract_mesh):
            return fn(*args)

    return run
```

```python
import functools
import math

import jax
import jax.numpy as jnp
import numpy as np
from jax import lax
from jax.experimental import pallas as pl
from jax.experimental.pallas import tpu as pltpu
from jax.sharding import PartitionSpec as P

HEAD_DIM = 128
NORM_EPS = 1e-5
ROPE_THETA = 5e7
MASK_VALUE = -1e30

MESH = pl.DeviceIdType.MESH
ANY = pl.BlockSpec(memory_space=pl.ANY)
VM = pl.BlockSpec(memory_space=pltpu.VMEM)
BF16 = jnp.bfloat16
F32 = jnp.float32

SP = 4
NB = 256
GATE_COLS = 384
FULL_CHUNKS = 8
DOWN_COLS = 256
DOWN_PARTS = 9
LAST_CUTS = 3
ROW_CHUNKS = 3


def dot(a, b):
    return jnp.dot(a, b, preferred_element_type=F32)


def layer_kernel(
    x, gain_attn, gain_mlp, wq, wk, wv, wo, wg, wu, wd, cos, sin,
    out, rem_attn, rem_mlp, x_got, a_all, qkv_rem, wo_rem, gu_rem, wd_rem, qkv, o_own, o_got, hid, b_all, u_own, u_got,
    gain_a, rem_a, gain_m, rem_m, cos_buf, sin_buf, send_sem, recv_sem, load_sem,
):
    tokens, dim = x.shape
    num_rows, shard_len = o_own.shape[1], o_own.shape[2]
    half, quarter, eighth = dim // 2, dim // 4, dim // 8
    feat = u_own.shape[1]
    half_feat = wd.shape[0]
    tile = tokens // ROW_CHUNKS
    tile_rows = num_rows // ROW_CHUNKS
    down_chunks = quarter // DOWN_COLS
    part_rows = half_feat // DOWN_PARTS
    heads = eighth // HEAD_DIM
    short = (feat - FULL_CHUNKS * GATE_COLS) // 128
    sizes = [GATE_COLS] * FULL_CHUNKS + [128] * short
    starts = [sum(sizes[:c]) for c in range(len(sizes))]
    chunks = len(sizes)

    y = lax.axis_index("fsdp")
    me = lax.axis_index("sp")
    core, chip = me % 2, me // 2
    peer = [me, me + 1 - 2 * core, (me + 2) % 4, 3 - me]
    to_y = {"fsdp": 1 - y}
    to = [None] + [{"sp": peer[k]} for k in (1, 2, 3)]

    def sp_of(k):
        return 2 * ((chip + k // 2) % 2) + (core + k) % 2

    def cols(start, size):
        return pl.ds(pl.multiple_of(start, 128), size)

    def rows(start, size):
        return pl.ds(pl.multiple_of(start, 16), size)

    used = [0]

    def slots(n):
        used[0] += n
        return used[0] - n

    s_gain, s_qkv, s_wo, s_gu = slots(2), slots(6), slots(4), slots(2 * chunks)
    s_wd, s_wl = slots(4 * DOWN_PARTS * down_chunks), slots(4 * LAST_CUTS)
    s_x, s_a, s_b = slots(ROW_CHUNKS), slots(2 * ROW_CHUNKS), slots(2 * ROW_CHUNKS)
    s_o, s_u = slots(12 * ROW_CHUNKS), slots(3 * chunks)

    def copy(slot, src, dst, dev):
        return pltpu.make_async_remote_copy(
            src_ref=src, dst_ref=dst, send_sem=send_sem.at[slot], recv_sem=recv_sem.at[slot], device_id=dev, device_id_type=MESH
        )

    def load(slot, src, dst):
        return pltpu.make_async_copy(src, dst, load_sem.at[slot])

    barrier = pltpu.get_barrier_semaphore()
    for dev in (to_y, to[1], to[2], to[3]):
        pl.semaphore_signal(barrier, inc=1, device_id=dev, device_id_type=MESH)
    pl.semaphore_wait(barrier, 4)

    def x_copy(r):
        here = rows(r * tile, tile)
        return copy(s_x + r, x.at[here], x_got.at[here], to[2])

    gain_copies = [copy(s_gain, gain_attn, rem_attn, to_y), copy(s_gain + 1, gain_mlp, rem_mlp, to_y)]

    def qkv_copy(j, h):
        part = (1 - y + h) % 2
        src = (wq, wk, wv)[j].at[:, cols(part * half + me * eighth, eighth)]
        return copy(s_qkv + 2 * j + h, src, qkv_rem.at[2 * j + h], to_y)

    def wo_copy(k):
        if k == 0:
            return copy(s_wo, wo.at[:, cols(me * quarter, quarter)], wo_rem.at[0], to_y)
        return copy(s_wo + k, wo_rem.at[2 if k == 3 else 0], wo_rem.at[k], to[2] if k == 2 else to[1])

    def gu_copy(c, t, start, size):
        src = (wg, wu)[t].at[:, cols(me * feat + start, size)]
        return copy(s_gu + 2 * c + t, src, gu_rem.at[t, :, cols(start, size)], to_y)

    def wd_copy(m, k):
        part, col = rows((m % DOWN_PARTS) * part_rows, part_rows), (m // DOWN_PARTS) * DOWN_COLS
        if k == 0:
            return copy(s_wd + 4 * m, wd.at[part, cols(me * quarter + col, DOWN_COLS)], wd_rem.at[0, part, cols(col, DOWN_COLS)], to_y)
        here = (part, cols(col, DOWN_COLS))
        return copy(s_wd + 4 * m + k, wd_rem.at[(2 if k == 3 else 0, *here)], wd_rem.at[(k, *here)], to[2] if k == 2 else to[1])

    end = DOWN_PARTS * down_chunks - 1

    def last_copy(i, k):
        n = part_rows // LAST_CUTS
        part, col = rows((DOWN_PARTS - 1) * part_rows + i * n, n), quarter - DOWN_COLS
        if k == 0:
            return copy(s_wl + 4 * i, wd.at[part, cols(me * quarter + col, DOWN_COLS)], wd_rem.at[0, part, cols(col, DOWN_COLS)], to_y)
        here = (part, cols(col, DOWN_COLS))
        return copy(s_wl + 4 * i + k, wd_rem.at[(2 if k == 3 else 0, *here)], wd_rem.at[(k, *here)], to[2] if k == 2 else to[1])

    def wd_arrived(m, k):
        if isinstance(m, int) and m == end:
            for i in range(LAST_CUTS):
                last_copy(i, k).wait_recv()
        else:
            wd_copy(m, k).wait_recv()

    def act_copy(base, ref, piece, r):
        return copy(
            base + (piece // 2) * ROW_CHUNKS + r,
            ref.at[rows(piece * tokens + r * tile, tile)],
            ref.at[rows((piece + 1) * tokens + r * tile, tile)],
            to[1],
        )

    def o_copy(h, r, k, s):
        here = pl.ds(r * tile_rows, tile_rows)
        piece = k ^ (2 * s)
        return copy(
            s_o + ((h * ROW_CHUNKS + r) * 3 + k - 1) * 2 + s,
            o_own.at[4 * h + piece, here],
            o_got.at[6 * h + 2 * (k - 1) + s, here],
            to[k],
        )

    def u_copy(c, k, start, size):
        here = (pl.ds(k * tokens, tokens), cols(start, size))
        return copy(s_u + 3 * c + k - 1, u_own.at[here], u_got.at[here], to[k])

    def cuts(m):
        if isinstance(m, int) and m == end:
            return [functools.partial(last_copy, i) for i in range(LAST_CUTS)]
        return [functools.partial(wd_copy, m)]

    def pass_y(*ms):
        for m in ms:
            for piece in cuts(m):
                piece(0).wait_recv()
                piece(2).start()
                piece(1).start()

    def pass_x(*ms):
        for m in ms:
            for piece in cuts(m):
                piece(2).wait_recv()
                piece(3).start()

    for r in range(ROW_CHUNKS):
        x_copy(r).start()
    for d in gain_copies:
        d.start()
    for h in range(2):
        for j in range(3):
            qkv_copy(j, h).start()
    wo_copy(0).start()
    for c in range(chunks):
        if c == FULL_CHUNKS:
            for m in range(DOWN_PARTS):
                wd_copy(m, 0).start()
        for t in range(2):
            gu_copy(c, t, starts[c], sizes[c]).start()
    for m in range(DOWN_PARTS, end):
        wd_copy(m, 0).start()
    for i in range(LAST_CUTS):
        last_copy(i, 0).start()
    tabs = [load(0, cos, cos_buf), load(1, sin, sin_buf), load(2, gain_attn, gain_a), load(3, gain_mlp, gain_m)]
    for d in tabs:
        d.start()
    for d in gain_copies:
        d.wait_recv()
    tabs += [load(4, rem_attn, rem_a), load(5, rem_mlp, rem_m)]
    for d in tabs[4:]:
        d.start()
    for d in tabs:
        d.wait()

    def norm_chunk(src, dst, which, src_row, dst_row):
        n = tile // 3
        gm = (gain_a, gain_m)[which][...].astype(F32).reshape(1, half)
        go = (rem_a, rem_m)[which][...].astype(F32).reshape(1, half)

        def body(in_ref, out_ref):
            def sub(s, carry):
                here = pl.ds(pl.multiple_of(s * 16, 16), 16)
                mine = in_ref[here, cols(y * half, half)].astype(F32)
                other = in_ref[here, cols((1 - y) * half, half)].astype(F32)
                total = jnp.sum(mine * mine, axis=-1, keepdims=True) + jnp.sum(other * other, axis=-1, keepdims=True)
                inv = lax.rsqrt(total / dim + NORM_EPS)
                out_ref[here, 0:half] = (mine * inv * gm).astype(BF16)
                out_ref[here, half:dim] = (other * inv * go).astype(BF16)
                return carry

            lax.fori_loop(0, n // 16, sub, 0)

        pltpu.emit_pipeline(
            body,
            grid=(3,),
            in_specs=[pl.BlockSpec((n, dim), lambda t: (src_row // n + t, 0))],
            out_specs=[pl.BlockSpec((n, dim), lambda t: (dst_row // n + t, 0))],
        )(src, dst)

    def own_a(r, carry):
        norm_chunk(x, a_all, 0, r * tile, r * tile)
        act_copy(s_a, a_all, 0, r).start()
        return carry

    def got_a(r, carry):
        x_copy(r).wait_recv()
        norm_chunk(x_got, a_all, 0, r * tile, 2 * tokens + r * tile)
        act_copy(s_a, a_all, 2, r).start()
        return carry

    def attention(w_qk, w_v):
        seq = SP * shard_len
        idx = lax.broadcasted_iota(jnp.int32, (1, seq), 1)
        idq = lax.broadcasted_iota(jnp.int32, (seq, 1), 0)

        def position(i):
            piece = (i >= shard_len).astype(jnp.int32) + (i >= 2 * shard_len).astype(jnp.int32) + (i >= 3 * shard_len).astype(jnp.int32)
            chip_of = (chip + (piece >> 1)) & 1
            core_of = (core + piece) & 1
            return SP * (i - shard_len * piece) + 2 * chip_of + core_of

        def attn_body(q_ref, k_ref, v_ref, o_ref):
            keep = position(idx) <= position(idq)

            def head(h, carry):
                here = cols(h * HEAD_DIM, HEAD_DIM)
                q = q_ref[:, 0, :, here].reshape(seq, HEAD_DIM)
                k = k_ref[:, 0, :, here].reshape(seq, HEAD_DIM)
                v = v_ref[:, 0, :, here].reshape(seq, HEAD_DIM)
                s = lax.dot_general(q, k, (((1,), (1,)), ((), ())), preferred_element_type=F32) * HEAD_DIM**-0.5
                s = jnp.where(keep, s, MASK_VALUE)
                p = jnp.exp(s - jnp.max(s, axis=-1, keepdims=True))
                total = jnp.sum(p, axis=-1, keepdims=True)
                o = dot(p.astype(BF16), v) / total
                o_ref[:, 0, :, here] = o.astype(BF16).reshape(SP, shard_len, HEAD_DIM)
                return carry

            lax.fori_loop(0, heads, head, 0)

        def w_loads(j, h, dst, at):
            part = (y + h) % 2
            return [
                load(2 * j, (wq, wk, wv)[j].at[:, cols(part * half + me * eighth, eighth)], dst.at[0:half, at : at + eighth]),
                load(2 * j + 1, qkv_rem.at[2 * j + h], dst.at[half:dim, at : at + eighth]),
            ]

        def heads_half(h, carry):
            @pl.when(h == 0)
            def _():
                got_a(0, 0)

            loads = w_loads(0, h, w_qk, 0) + w_loads(1, h, w_qk, eighth)
            loads[0].start()
            loads[2].start()
            qkv_copy(0, h).wait_recv()
            loads[1].start()
            qkv_copy(1, h).wait_recv()
            loads[3].start()
            for d in loads:
                d.wait()

            def qk_side(side, c2):
                @pl.when((h == 0) & (side == 0))
                def _():
                    for r in range(ROW_CHUNKS):
                        act_copy(s_a, a_all, 0, r).wait_recv()

                @pl.when((h == 0) & (side == 1))
                def _():
                    lax.fori_loop(1, ROW_CHUNKS, got_a, 0)
                    for r in range(ROW_CHUNKS):
                        act_copy(s_a, a_all, 2, r).wait_recv()

                t0 = side * 2 * ROW_CHUNKS

                def body(a_ref, q_ref, k_ref):
                    sp = sp_of((t0 + pl.program_id(0)) // ROW_CHUNKS)
                    c_tab, s_tab = cos_buf[sp], sin_buf[sp]
                    for n in range(2 * eighth // NB):
                        acc = dot(a_ref[...], w_qk[:, n * NB : (n + 1) * NB])
                        for i in range(NB // HEAD_DIM):
                            t = acc[:, i * HEAD_DIM : (i + 1) * HEAD_DIM]
                            turned = pltpu.roll(t, HEAD_DIM // 2, 1)
                            shape = (tile_rows, shard_len, HEAD_DIM)
                            rot = t.reshape(shape) * c_tab + turned.reshape(shape) * s_tab
                            lo = n * NB + i * HEAD_DIM
                            ref = q_ref if lo < eighth else k_ref
                            lo = lo % eighth
                            ref[0, :, :, lo : lo + HEAD_DIM] = rot.astype(BF16)

                def spec(j):
                    return pl.BlockSpec(
                        (1, tile_rows, shard_len, eighth),
                        lambda t: ((2 * j + h) * SP + (t0 + t) // ROW_CHUNKS, (t0 + t) % ROW_CHUNKS, 0, 0),
                    )

                pltpu.emit_pipeline(
                    body,
                    grid=(2 * ROW_CHUNKS,),
                    in_specs=[pl.BlockSpec((tile, dim), lambda t: (t0 + t, 0))],
                    out_specs=[spec(0), spec(1)],
                )(a_all, qkv, qkv)
                return c2

            v_loads = w_loads(2, h, w_v, 0)
            v_loads[0].start()
            lax.fori_loop(0, 2, qk_side, 0)
            qkv_copy(2, h).wait_recv()
            v_loads[1].start()
            for d in v_loads:
                d.wait()

            def rows_chunk(r, c2):
                def v_body(a_ref, v_ref):
                    for lo in range(0, eighth, NB):
                        size = min(NB, eighth - lo)
                        acc = dot(a_ref[...], w_v[:, lo : lo + size])
                        v_ref[0, :, :, lo : lo + size] = acc.astype(BF16).reshape(tile_rows, shard_len, size)

                pltpu.emit_pipeline(
                    v_body,
                    grid=(SP,),
                    in_specs=[pl.BlockSpec((tile, dim), lambda t: (t * ROW_CHUNKS + r, 0))],
                    out_specs=[pl.BlockSpec((1, tile_rows, shard_len, eighth), lambda t: ((4 + h) * SP + t, r, 0, 0))],
                )(a_all, qkv)

                def spec(block):
                    return pl.BlockSpec((SP, 1, shard_len, eighth), lambda t: (block, r * tile_rows + t, 0, 0))

                pltpu.emit_pipeline(
                    attn_body,
                    grid=(tile_rows,),
                    in_specs=[spec(h), spec(2 + h), spec(4 + h)],
                    out_specs=[spec(h)],
                )(qkv, qkv, qkv, o_own)
                for k in (2, 3, 1):
                    for s in range(2):
                        o_copy(h, r, k, s).start()
                return c2

            lax.fori_loop(0, ROW_CHUNKS, rows_chunk, 0)
            return carry

        lax.fori_loop(0, 2, heads_half, 0)

    def out_phase(w_buf, o_buf):
        def fetch(k, slot):
            return [
                load(2 * slot, wo.at[:, cols(sp_of(k) * quarter, quarter)], w_buf.at[slot, 0:half]),
                load(2 * slot + 1, wo_rem.at[k], w_buf.at[slot, half:dim]),
            ]

        def o_load(h, k, s):
            src = o_own.at[4 * h + 2 * s] if k == 0 else o_got.at[6 * h + 2 * (k - 1) + s]
            dst = o_buf.at[s * num_rows : (s + 1) * num_rows, :, cols(h * half + sp_of(k) * eighth, eighth)]
            return load(4 + 8 * h + 2 * k + s, src, dst)

        loads = []

        def o_fetch(h):
            for k in (0, 1, 2, 3):
                for s in range(2):
                    if k:
                        for r in range(ROW_CHUNKS):
                            o_copy(h, r, k, s).wait_recv()
                    d = o_load(h, k, s)
                    d.start()
                    loads.append(d)

        o_fetch(0)
        wo_copy(0).wait_recv()
        wo_copy(2).start()
        wo_copy(1).start()
        for d in fetch(0, 0):
            d.start()
        o_fetch(1)
        for d in loads:
            d.wait()

        def step(k, carry):
            slot = k % 2

            @pl.when(k == 0)
            def _():
                wo_copy(1).wait_recv()
                for d in fetch(1, 1):
                    d.start()

            @pl.when(k == 2)
            def _():
                wo_copy(2).wait_recv()
                wo_copy(3).start()
                for d in fetch(2, 0):
                    d.start()

            for d in fetch(k, slot):
                d.wait()

            def run(x_ref_all, s):
                def body(x_ref, h_ref):
                    mine = pl.ds(s * num_rows + pl.program_id(0) * tile_rows, tile_rows)
                    for n in range(quarter // NB):
                        here = slice(n * NB, (n + 1) * NB)
                        lhs = o_buf[mine].reshape(tile, dim)
                        h_ref[:, here] = (x_ref[:, here].astype(F32) + dot(lhs, w_buf[slot, :, here])).astype(BF16)

                pltpu.emit_pipeline(
                    body,
                    grid=(ROW_CHUNKS,),
                    in_specs=[pl.BlockSpec((tile, quarter), lambda t: (t, sp_of(k)))],
                    out_specs=[pl.BlockSpec((tile, quarter), lambda t: (s * ROW_CHUNKS + t, sp_of(k)))],
                )(x_ref_all, hid)

            run(x, 0)

            @pl.when(k == 2)
            def _():
                wo_copy(3).wait_recv()
                for d in fetch(3, 1):
                    d.start()

            run(x_got, 1)
            return carry

        lax.fori_loop(0, SP, step, 0)

    def b_chunk(n, carry):
        s, r = n // ROW_CHUNKS, n % ROW_CHUNKS
        norm_chunk(hid, b_all, 1, n * tile, 2 * s * tokens + r * tile)
        copy(
            s_b + n,
            b_all.at[rows(2 * s * tokens + r * tile, tile)],
            b_all.at[rows((2 * s + 1) * tokens + r * tile, tile)],
            to[1],
        ).start()
        return carry

    def gate_phase(w_buf):
        def w_load(slot, start, size):
            mine = [
                load(4 * slot + t, (wg, wu)[t].at[:, cols(me * feat + start, size)], w_buf.at[slot, 0:half, t * size : (t + 1) * size])
                for t in range(2)
            ]
            other = [
                load(4 * slot + 2 + t, gu_rem.at[t, :, cols(start, size)], w_buf.at[slot, half:dim, t * size : (t + 1) * size])
                for t in range(2)
            ]
            return mine, other

        def run(c, side, slot, start, size):
            def body(b_ref, o_ref):
                parts = [dot(b_ref[...], w_buf[slot, :, n * NB : (n + 1) * NB]) for n in range(2 * size // NB)]
                both = [p[:, lo : lo + 128] for p in parts for lo in (0, 128)]
                n = size // 128
                for i in range(n):
                    o_ref[:, i * 128 : (i + 1) * 128] = (jax.nn.silu(both[i]) * both[n + i]).astype(BF16)

            n_t = 2 * ROW_CHUNKS
            pltpu.emit_pipeline(
                body,
                grid=(n_t,),
                in_specs=[pl.BlockSpec((tile, dim), lambda t: (side * n_t + t, 0))],
                out_specs=[pl.BlockSpec((tile, size), lambda t: (side * n_t + t, 0))],
            )(b_all, u_own.at[:, cols(start, size)])

            @pl.when(side == 0)
            def _():
                u_copy(c, 1, start, size).start()

            @pl.when(side == 1)
            def _():
                u_copy(c, 2, start, size).start()
                u_copy(c, 3, start, size).start()

        def chunk(c, slot, start, size, prefetch, before, middle, after):
            before()
            mine, other = w_load(slot, start, size)
            for t in range(2):
                gu_copy(c, t, start, size).wait_recv()
            for d in other:
                d.start()
            for d in mine + other:
                d.wait()
            prefetch()

            def sides(t, carry):
                side = 1 - t

                @pl.when(c == 0)
                def _():
                    for r in range(ROW_CHUNKS):
                        n = side * ROW_CHUNKS + r
                        copy(
                            s_b + n,
                            b_all.at[rows(2 * side * tokens + r * tile, tile)],
                            b_all.at[rows((2 * side + 1) * tokens + r * tile, tile)],
                            to[1],
                        ).wait_recv()

                @pl.when(side == 0)
                def _():
                    middle()

                run(c, side, slot, start, size)
                return carry

            lax.fori_loop(0, 2, sides, 0)
            after()

        def at(c, n, work):
            @pl.when(c == n)
            def _():
                work()

        for d in w_load(0, 0, GATE_COLS)[0]:
            d.start()

        def full(c, carry):
            def prefetch():
                @pl.when(c + 1 < FULL_CHUNKS)
                def _():
                    for d in w_load((c + 1) % 2, (c + 1) * GATE_COLS, GATE_COLS)[0]:
                        d.start()

                @pl.when(c + 1 == FULL_CHUNKS)
                def _():
                    for d in w_load((c + 1) % 2, starts[FULL_CHUNKS], 128)[0]:
                        d.start()

            def before():
                at(c, FULL_CHUNKS - 1, lambda: pass_y(0, 1))

            def middle():
                at(c, FULL_CHUNKS - 1, lambda: (pass_y(2, 3, 4), pass_x(0)))

            def after():
                at(c, FULL_CHUNKS - 1, lambda: (pass_y(5, 6, 7), pass_x(1)))

            chunk(c, c % 2, c * GATE_COLS, GATE_COLS, prefetch, before, middle, after)
            return carry

        lax.fori_loop(0, FULL_CHUNKS, full, 0)

        def brief(c, carry):
            def start_of(i):
                return starts[FULL_CHUNKS] + (i - FULL_CHUNKS) * 128

            def prefetch():
                @pl.when(c + 1 < chunks)
                def _():
                    for d in w_load((c + 1) % 2, start_of(c + 1), 128)[0]:
                        d.start()

            def before():
                at(c, FULL_CHUNKS, lambda: pass_y(8))
                at(c, FULL_CHUNKS + 1, lambda: pass_x(4))
                at(c, FULL_CHUNKS + 2, lambda: pass_x(6))

            def middle():
                at(c, FULL_CHUNKS, lambda: pass_x(2, 3))
                at(c, FULL_CHUNKS + 1, lambda: pass_x(5))
                at(c, FULL_CHUNKS + 2, lambda: (pass_y(9), pass_x(7)))

            chunk(c, c % 2, start_of(c), 128, prefetch, before, middle, lambda: None)
            return carry

        lax.fori_loop(FULL_CHUNKS, chunks, brief, 0)

    def down_phase(u_buf, w_mine, w_other, h_buf, acc_buf, o_buf):
        total = SP * down_chunks
        main = total - SP
        last = end + 1 - DOWN_PARTS
        band = tokens // 2

        def u_load(k):
            sp = sp_of(k)
            at = ((sp // 2 + y) % 2) * half_feat + (sp % 2) * feat
            return load(k, (u_got if k else u_own).at[pl.ds(k * tokens, tokens)], u_buf.at[:, cols(at, feat)])

        def out_cols(n):
            return cols(sp_of(n % SP) * quarter + (n // SP) * DOWN_COLS, DOWN_COLS)

        def fetch(n):
            slot = n % 2
            here = out_cols(n)
            return [load(4 + 2 * slot, wd.at[:, here], w_mine.at[slot]), load(5 + 2 * slot, hid.at[0:tokens, here], h_buf.at[slot])]

        def store(n):
            return load(8 + n % 2, o_buf.at[n % 2], out.at[:, out_cols(n)])

        def mine(n):
            @pl.when(n + 1 < total)
            def _():
                for d in fetch(n + 1):
                    d.start()

            for d in fetch(n):
                d.wait()

            def part(t, carry):
                m = rows(t * band, band)
                acc_buf[n % SP, m] = h_buf[n % 2, m].astype(F32) + dot(u_buf[m, 0:half_feat], w_mine[n % 2])
                return carry

            lax.fori_loop(0, 2, part, 0)

        for d in fetch(0):
            d.start()
        u_load(0).start()
        pass_y(10, 11)
        pass_x(8)
        for k in (1, 2, 3):
            for c in range(chunks):
                u_copy(c, k, starts[c], sizes[c]).wait_recv()
            u_load(k).start()
        for k in range(SP):
            u_load(k).wait()

        def other(n):
            c, k = n // SP, n % SP
            ready = load(12, wd_rem.at[k, :, cols(c * DOWN_COLS, DOWN_COLS)], w_other)
            for side in (1, 3):

                @pl.when(k == side)
                def _():
                    for p in range(DOWN_PARTS):
                        wd_copy(DOWN_PARTS * c + p, side).wait_recv()

            ready.start()

            @pl.when(n >= 2)
            def _():
                store(n - 2).wait()

            ready.wait()

            def part(t, carry):
                m = rows(t * band, band)
                o_buf[k % 2, m] = (acc_buf[k, m] + dot(u_buf[m, half_feat:], w_other[...])).astype(BF16)
                return carry

            lax.fori_loop(0, 2, part, 0)
            store(n).start()

        pieces = DOWN_PARTS * down_chunks

        def passes(n, table):
            for when, (m_y, m_x) in table.items():

                @pl.when(n == when)
                def _():
                    if m_y < pieces:
                        pass_y(m_y)
                    if m_x is not None:
                        pass_x(m_x)

        def first(n, carry):
            passes(n, {0: (12, None), 2: (15, 11), 3: (16, 12), 5: (18, 14), 7: (19, 15)})
            mine(n)
            passes(n, {0: (13, 9), 1: (14, 10), 3: (17, 13)})

            @pl.when(n < SP)
            def _():
                other(n)

            return carry

        def slot(i, carry):
            m = 17 + i + 2 * ((i + 14) // 21)
            c, r = (m - 8) // 9, (m - 8) % 9
            pass_y(20 + i)
            pass_x(16 + i)
            two = 2 * (r // 3)

            @pl.when((r == 0) | (r == 3))
            def _():
                def run(k, c2):
                    other(SP * c + two + k)
                    return c2

                lax.fori_loop(0, 2, run, 0)

            @pl.when((r == 1) | (r == 4))
            def _():
                def run(k, c2):
                    mine(SP * (c + 1) + two + k)
                    return c2

                lax.fori_loop(0, 2, run, 0)

            return carry

        lax.fori_loop(0, 2 * SP, first, 0)
        if down_chunks > 2:
            lax.fori_loop(0, last + 4 - 19, slot, 0)
        next_y, next_x = (5, 1) if down_chunks > 2 else (9, 7)

        def piece_load(k, p):
            at = rows((2 * k + p % 2) * part_rows, part_rows)
            return load(2 * k + p % 2, wd_rem.at[k, rows(p * part_rows, part_rows), cols(quarter - DOWN_COLS, DOWN_COLS)], w_other.at[at])

        def piece_dot(k, p):
            piece_load(k, p).wait()
            at = rows((2 * k + p % 2) * part_rows, part_rows)
            acc_buf[k] = acc_buf[k] + dot(u_buf[:, cols(half_feat + p * part_rows, part_rows)], w_other[at])

        def finish(k):
            store(main + k - 2).wait()
            o_buf[k % 2] = acc_buf[k].astype(BF16)
            store(main + k).start()

        def first_two(p):
            if isinstance(p, int):
                wd_arrived(last + p, 1)
            else:

                @pl.when(p < DOWN_PARTS - 1)
                def _():
                    wd_arrived(last + p, 1)

                @pl.when(p == DOWN_PARTS - 1)
                def _():
                    wd_arrived(end, 1)

            for k in (0, 1):
                piece_load(k, p).start()

        first_two(0)

        def last_step(p, carry):
            @pl.when(p + next_y < DOWN_PARTS - 1)
            def _():
                pass_y(last + next_y + p)

            @pl.when(p + next_y == DOWN_PARTS - 1)
            def _():
                pass_y(end)

            piece_dot(0, p)
            piece_dot(1, p)

            @pl.when(p == DOWN_PARTS - 1)
            def _():
                finish(0)
                finish(1)

            @pl.when((p >= next_x) & (p < DOWN_PARTS - 1))
            def _():
                pass_x(last + p)

            @pl.when(p == DOWN_PARTS - 1)
            def _():
                pass_x(end)

            piece_load(2, p).start()

            @pl.when(p + 1 < DOWN_PARTS)
            def _():
                first_two(p + 1)

            @pl.when(p > 0)
            def _():
                piece_dot(3, p - 1)

            piece_dot(2, p)

            @pl.when(p == DOWN_PARTS - 1)
            def _():
                finish(2)

            @pl.when(p < DOWN_PARTS - 1)
            def _():
                wd_arrived(last + p, 3)

            @pl.when(p == DOWN_PARTS - 1)
            def _():
                wd_arrived(end, 3)

            piece_load(3, p).start()
            return carry

        lax.fori_loop(0, DOWN_PARTS, last_step, 0)
        piece_dot(3, DOWN_PARTS - 1)
        finish(3)
        for k in (2, 3):
            store(main + k).wait()

    lax.fori_loop(0, ROW_CHUNKS, own_a, 0)
    pl.run_scoped(attention, pltpu.VMEM((dim, 2 * eighth), BF16), pltpu.VMEM((dim, eighth), BF16))
    pl.run_scoped(out_phase, pltpu.VMEM((2, dim, quarter), BF16), pltpu.VMEM((2 * num_rows, shard_len, dim), BF16))
    lax.fori_loop(0, 2 * ROW_CHUNKS, b_chunk, 0)
    pl.run_scoped(gate_phase, pltpu.VMEM((2, dim, 2 * GATE_COLS), BF16))
    pl.run_scoped(
        down_phase,
        pltpu.VMEM((tokens, 2 * half_feat), BF16),
        pltpu.VMEM((2, half_feat, DOWN_COLS), BF16),
        pltpu.VMEM((half_feat, DOWN_COLS), BF16),
        pltpu.VMEM((2, tokens, DOWN_COLS), BF16),
        pltpu.VMEM((SP, tokens, DOWN_COLS), F32),
        pltpu.VMEM((2, tokens, DOWN_COLS), BF16),
    )

    for d in gain_copies:
        d.wait_send()
    for h in range(2):
        for j in range(3):
            qkv_copy(j, h).wait_send()
    for k in range(SP):
        wo_copy(k).wait_send()
    for c in range(chunks):
        for t in range(2):
            gu_copy(c, t, starts[c], sizes[c]).wait_send()
        for k in (1, 2, 3):
            u_copy(c, k, starts[c], sizes[c]).wait_send()
    for r in range(ROW_CHUNKS):
        x_copy(r).wait_send()
        for piece in (0, 2):
            act_copy(s_a, a_all, piece, r).wait_send()
            act_copy(s_b, b_all, piece, r).wait_send()

        def o_sent(h, carry):
            for k in (1, 2, 3):
                for s in range(2):
                    o_copy(h, r, k, s).wait_send()
            return carry

        lax.fori_loop(0, 2, o_sent, 0)

    def wd_sent(m, carry):
        for k in range(SP):
            wd_copy(m, k).wait_send()
        return carry

    lax.fori_loop(0, end, wd_sent, 0)
    for i in range(LAST_CUTS):
        for k in range(SP):
            last_copy(i, k).wait_send()


def hand_over(src, dst, buf, in_sem, out_sem):
    n = src.shape[0]
    reads = [pltpu.make_async_copy(src.at[r], buf.at[r], in_sem.at[r]) for r in range(n)]
    writes = [pltpu.make_async_copy(buf.at[r], dst.at[r], out_sem.at[r]) for r in range(n)]
    for d in reads:
        d.start()
    for r in range(n):
        reads[r].wait()
        writes[r].start()
    for d in writes:
        d.wait()


def tables(shard_len):
    inv_freq = np.exp(np.arange(HEAD_DIM // 2, dtype=np.float32) * np.float32(-2.0 * math.log(ROPE_THETA) / HEAD_DIM))
    pos = np.arange(shard_len)[None, :] * SP + np.arange(SP)[:, None]
    angles = (pos.astype(np.float32)[..., None] * inv_freq.astype(np.float32)).astype(np.float64)
    cos, sin = np.cos(angles), np.sin(angles)
    return (
        np.concatenate([cos, cos], axis=-1).astype(np.float32),
        np.concatenate([-sin, sin], axis=-1).astype(np.float32),
    )


def local_layer(x_loc, norm_attn, w_query, w_key, w_value, w_out, norm_mlp, w_gate, w_up, w_down):
    num_rows, shard_len, dim = x_loc.shape
    tokens = num_rows * shard_len
    half, quarter, eighth = dim // 2, dim // 4, dim // 8
    half_feat = w_down.shape[0]
    feat = half_feat // 2
    cos, sin = tables(shard_len)

    def buf(*shape):
        return jax.ShapeDtypeStruct(shape, BF16)

    shapes = [
        buf(tokens, dim),
        buf(half),
        buf(half),
        buf(tokens, dim),
        buf(SP * tokens, dim),
        buf(6, half, eighth),
        buf(SP, half, quarter),
        buf(2, half, feat),
        buf(SP, half_feat, quarter),
        buf(6 * SP, num_rows, shard_len, eighth),
        buf(2 * SP, num_rows, shard_len, eighth),
        buf(12, num_rows, shard_len, eighth),
        buf(2 * tokens, dim),
        buf(SP * tokens, dim),
        buf(SP * tokens, feat),
        buf(SP * tokens, feat),
    ]
    chunks = FULL_CHUNKS + (feat - FULL_CHUNKS * GATE_COLS) // 128
    copies = 2 + 6 + 4 + 2 * chunks + 4 * DOWN_PARTS * (quarter // DOWN_COLS) + 4 * LAST_CUTS + 17 * ROW_CHUNKS + 3 * chunks
    outs = pl.pallas_call(
        layer_kernel,
        out_shape=shapes,
        in_specs=[ANY] * 12,
        out_specs=[ANY] * len(shapes),
        scratch_shapes=[
            *[pltpu.VMEM((half,), BF16)] * 4,
            pltpu.VMEM((SP, shard_len, HEAD_DIM), F32),
            pltpu.VMEM((SP, shard_len, HEAD_DIM), F32),
            pltpu.SemaphoreType.DMA((copies,)),
            pltpu.SemaphoreType.DMA((copies,)),
            pltpu.SemaphoreType.DMA((20,)),
        ],
        compiler_params=pltpu.CompilerParams(collective_id=0, has_side_effects=True, vmem_limit_bytes=67043328),
        name="decoder_layer",
    )(x_loc.reshape(tokens, dim), norm_attn, norm_mlp, w_query, w_key, w_value, w_out, w_gate, w_up, w_down, jnp.asarray(cos), jnp.asarray(sin))
    return pl.pallas_call(
        hand_over,
        out_shape=buf(*x_loc.shape),
        in_specs=[ANY],
        out_specs=ANY,
        scratch_shapes=[
            pltpu.VMEM(x_loc.shape, BF16),
            pltpu.SemaphoreType.DMA((num_rows,)),
            pltpu.SemaphoreType.DMA((num_rows,)),
        ],
        compiler_params=pltpu.CompilerParams(vmem_limit_bytes=67043328),
        name="hand_over",
    )(outs[0].reshape(x_loc.shape))


def solution(mesh):
    row_spec = P(("dp", "fsdp"), "sp", None)
    weight_spec = P("fsdp", None)
    gain_spec = P("fsdp")
    in_specs = (row_spec, gain_spec, weight_spec, weight_spec, weight_spec, weight_spec, gain_spec, weight_spec, weight_spec, weight_spec)
    fn = jax.shard_map(local_layer, mesh=mesh, in_specs=in_specs, out_specs=row_spec, check_vma=False)

    def run(*args):
        with jax.sharding.use_abstract_mesh(mesh.abstract_mesh):
            return fn(*args)

    return run
```

```python
import functools
import math

import jax
import jax.numpy as jnp
import numpy as np
from jax import lax
from jax.experimental import pallas as pl
from jax.experimental.pallas import tpu as pltpu
from jax.sharding import PartitionSpec as P

HEAD_DIM = 128
NORM_EPS = 1e-5
ROPE_THETA = 5e7
MASK_VALUE = -1e30

MESH = pl.DeviceIdType.MESH
ANY = pl.BlockSpec(memory_space=pl.ANY)
VM = pl.BlockSpec(memory_space=pltpu.VMEM)
BF16 = jnp.bfloat16
F32 = jnp.float32

SP = 4
NB = 256
GATE_COLS = 384
FULL_CHUNKS = 8
DOWN_COLS = 256
DOWN_PARTS = 9
LAST_CUTS = 1
ROW_CHUNKS = 3


def dot(a, b):
    return jnp.dot(a, b, preferred_element_type=F32)


def layer_kernel(
    x, gain_attn, gain_mlp, wq, wk, wv, wo, wg, wu, wd, cos, sin,
    out, rem_attn, rem_mlp, x_got, a_all, qkv_rem, wo_rem, gu_rem, wd_rem, qkv, o_own, o_got, hid, b_all, u_own, u_got,
    gain_a, rem_a, gain_m, rem_m, cos_buf, sin_buf, send_sem, recv_sem, load_sem,
):
    tokens, dim = x.shape
    num_rows, shard_len = o_own.shape[1], o_own.shape[2]
    half, quarter, eighth = dim // 2, dim // 4, dim // 8
    feat = u_own.shape[1]
    half_feat = wd.shape[0]
    tile = tokens // ROW_CHUNKS
    tile_rows = num_rows // ROW_CHUNKS
    down_chunks = quarter // DOWN_COLS
    part_rows = half_feat // DOWN_PARTS
    heads = eighth // HEAD_DIM
    short = (feat - FULL_CHUNKS * GATE_COLS) // 128
    sizes = [GATE_COLS] * FULL_CHUNKS + [128] * short
    starts = [sum(sizes[:c]) for c in range(len(sizes))]
    chunks = len(sizes)

    y = lax.axis_index("fsdp")
    me = lax.axis_index("sp")
    core, chip = me % 2, me // 2
    peer = [me, me + 1 - 2 * core, (me + 2) % 4, 3 - me]
    to_y = {"fsdp": 1 - y}
    to = [None] + [{"sp": peer[k]} for k in (1, 2, 3)]

    def sp_of(k):
        return 2 * ((chip + k // 2) % 2) + (core + k) % 2

    def cols(start, size):
        return pl.ds(pl.multiple_of(start, 128), size)

    def rows(start, size):
        return pl.ds(pl.multiple_of(start, 16), size)

    used = [0]

    def slots(n):
        used[0] += n
        return used[0] - n

    s_gain, s_qkv, s_wo, s_gu = slots(2), slots(6), slots(4), slots(2 * chunks)
    s_wd, s_wl = slots(4 * DOWN_PARTS * down_chunks), slots(4 * LAST_CUTS)
    s_x, s_a, s_b = slots(ROW_CHUNKS), slots(2 * ROW_CHUNKS), slots(2 * ROW_CHUNKS)
    s_o, s_u = slots(12 * ROW_CHUNKS), slots(3 * chunks)

    def copy(slot, src, dst, dev):
        return pltpu.make_async_remote_copy(
            src_ref=src, dst_ref=dst, send_sem=send_sem.at[slot], recv_sem=recv_sem.at[slot], device_id=dev, device_id_type=MESH
        )

    def load(slot, src, dst):
        return pltpu.make_async_copy(src, dst, load_sem.at[slot])

    barrier = pltpu.get_barrier_semaphore()
    for dev in (to_y, to[1], to[2], to[3]):
        pl.semaphore_signal(barrier, inc=1, device_id=dev, device_id_type=MESH)
    pl.semaphore_wait(barrier, 4)

    def x_copy(r):
        here = rows(r * tile, tile)
        return copy(s_x + r, x.at[here], x_got.at[here], to[2])

    gain_copies = [copy(s_gain, gain_attn, rem_attn, to_y), copy(s_gain + 1, gain_mlp, rem_mlp, to_y)]

    def qkv_copy(j, h):
        part = (1 - y + h) % 2
        src = (wq, wk, wv)[j].at[:, cols(part * half + me * eighth, eighth)]
        return copy(s_qkv + 2 * j + h, src, qkv_rem.at[2 * j + h], to_y)

    def wo_copy(k):
        if k == 0:
            return copy(s_wo, wo.at[:, cols(me * quarter, quarter)], wo_rem.at[0], to_y)
        return copy(s_wo + k, wo_rem.at[2 if k == 3 else 0], wo_rem.at[k], to[2] if k == 2 else to[1])

    def gu_copy(c, t, start, size):
        src = (wg, wu)[t].at[:, cols(me * feat + start, size)]
        return copy(s_gu + 2 * c + t, src, gu_rem.at[t, :, cols(start, size)], to_y)

    def wd_copy(m, k):
        part, col = rows((m % DOWN_PARTS) * part_rows, part_rows), (m // DOWN_PARTS) * DOWN_COLS
        if k == 0:
            return copy(s_wd + 4 * m, wd.at[part, cols(me * quarter + col, DOWN_COLS)], wd_rem.at[0, part, cols(col, DOWN_COLS)], to_y)
        here = (part, cols(col, DOWN_COLS))
        return copy(s_wd + 4 * m + k, wd_rem.at[(2 if k == 3 else 0, *here)], wd_rem.at[(k, *here)], to[2] if k == 2 else to[1])

    end = DOWN_PARTS * down_chunks - 1

    def last_copy(i, k):
        n = part_rows // LAST_CUTS
        part, col = rows((DOWN_PARTS - 1) * part_rows + i * n, n), quarter - DOWN_COLS
        if k == 0:
            return copy(s_wl + 4 * i, wd.at[part, cols(me * quarter + col, DOWN_COLS)], wd_rem.at[0, part, cols(col, DOWN_COLS)], to_y)
        if k == 2:
            return copy(s_wl + 4 * i + 2, wd.at[part, cols(sp_of(2) * quarter + col, DOWN_COLS)], wd_rem.at[2, part, cols(col, DOWN_COLS)], to_y)
        here = (part, cols(col, DOWN_COLS))
        return copy(s_wl + 4 * i + k, wd_rem.at[(k - 1, *here)], wd_rem.at[(k, *here)], to[1])

    def wd_arrived(m, k):
        if isinstance(m, int) and m == end:
            for i in range(LAST_CUTS):
                last_copy(i, k).wait_recv()
        else:
            wd_copy(m, k).wait_recv()

    def act_copy(base, ref, piece, r):
        return copy(
            base + (piece // 2) * ROW_CHUNKS + r,
            ref.at[rows(piece * tokens + r * tile, tile)],
            ref.at[rows((piece + 1) * tokens + r * tile, tile)],
            to[1],
        )

    def o_copy(h, r, k, s):
        here = pl.ds(r * tile_rows, tile_rows)
        piece = k ^ (2 * s)
        return copy(
            s_o + ((h * ROW_CHUNKS + r) * 3 + k - 1) * 2 + s,
            o_own.at[4 * h + piece, here],
            o_got.at[6 * h + 2 * (k - 1) + s, here],
            to[k],
        )

    def u_copy(c, k, start, size):
        here = (pl.ds(k * tokens, tokens), cols(start, size))
        return copy(s_u + 3 * c + k - 1, u_own.at[here], u_got.at[here], to[k])

    def cuts(m):
        if isinstance(m, int) and m == end:
            return [functools.partial(last_copy, i) for i in range(LAST_CUTS)]
        return [functools.partial(wd_copy, m)]

    def pass_y(*ms):
        for m in ms:
            for piece in cuts(m):
                piece(0).wait_recv()
                if not (isinstance(m, int) and m == end):
                    piece(2).start()
                piece(1).start()

    def pass_x(*ms):
        for m in ms:
            for piece in cuts(m):
                piece(2).wait_recv()
                piece(3).start()

    for r in range(ROW_CHUNKS):
        x_copy(r).start()
    for d in gain_copies:
        d.start()
    for h in range(2):
        for j in range(3):
            qkv_copy(j, h).start()
    wo_copy(0).start()
    for c in range(chunks):
        if c == FULL_CHUNKS:
            for m in range(DOWN_PARTS):
                wd_copy(m, 0).start()
        for t in range(2):
            gu_copy(c, t, starts[c], sizes[c]).start()
    for m in range(DOWN_PARTS, end):
        wd_copy(m, 0).start()
    for k in (0, 2):
        for i in range(LAST_CUTS):
            last_copy(i, k).start()
    tabs = [load(0, cos, cos_buf), load(1, sin, sin_buf), load(2, gain_attn, gain_a), load(3, gain_mlp, gain_m)]
    for d in tabs:
        d.start()
    for d in gain_copies:
        d.wait_recv()
    tabs += [load(4, rem_attn, rem_a), load(5, rem_mlp, rem_m)]
    for d in tabs[4:]:
        d.start()
    for d in tabs:
        d.wait()

    def norm_chunk(src, dst, which, src_row, dst_row):
        n = tile // 3
        gm = (gain_a, gain_m)[which][...].astype(F32).reshape(1, half)
        go = (rem_a, rem_m)[which][...].astype(F32).reshape(1, half)

        def body(in_ref, out_ref):
            def sub(s, carry):
                here = pl.ds(pl.multiple_of(s * 16, 16), 16)
                mine = in_ref[here, cols(y * half, half)].astype(F32)
                other = in_ref[here, cols((1 - y) * half, half)].astype(F32)
                total = jnp.sum(mine * mine, axis=-1, keepdims=True) + jnp.sum(other * other, axis=-1, keepdims=True)
                inv = lax.rsqrt(total / dim + NORM_EPS)
                out_ref[here, 0:half] = (mine * inv * gm).astype(BF16)
                out_ref[here, half:dim] = (other * inv * go).astype(BF16)
                return carry

            lax.fori_loop(0, n // 16, sub, 0)

        pltpu.emit_pipeline(
            body,
            grid=(3,),
            in_specs=[pl.BlockSpec((n, dim), lambda t: (src_row // n + t, 0))],
            out_specs=[pl.BlockSpec((n, dim), lambda t: (dst_row // n + t, 0))],
        )(src, dst)

    def own_a(r, carry):
        norm_chunk(x, a_all, 0, r * tile, r * tile)
        act_copy(s_a, a_all, 0, r).start()
        return carry

    def got_a(r, carry):
        x_copy(r).wait_recv()
        norm_chunk(x_got, a_all, 0, r * tile, 2 * tokens + r * tile)
        act_copy(s_a, a_all, 2, r).start()
        return carry

    def attention(w_qk, w_v):
        seq = SP * shard_len
        idx = lax.broadcasted_iota(jnp.int32, (1, seq), 1)
        idq = lax.broadcasted_iota(jnp.int32, (seq, 1), 0)

        def position(i):
            piece = (i >= shard_len).astype(jnp.int32) + (i >= 2 * shard_len).astype(jnp.int32) + (i >= 3 * shard_len).astype(jnp.int32)
            chip_of = (chip + (piece >> 1)) & 1
            core_of = (core + piece) & 1
            return SP * (i - shard_len * piece) + 2 * chip_of + core_of

        def attn_body(q_ref, k_ref, v_ref, o_ref):
            keep = position(idx) <= position(idq)

            def head(h, carry):
                here = cols(h * HEAD_DIM, HEAD_DIM)
                q = q_ref[:, 0, :, here].reshape(seq, HEAD_DIM)
                k = k_ref[:, 0, :, here].reshape(seq, HEAD_DIM)
                v = v_ref[:, 0, :, here].reshape(seq, HEAD_DIM)
                s = lax.dot_general(q, k, (((1,), (1,)), ((), ())), preferred_element_type=F32) * HEAD_DIM**-0.5
                s = jnp.where(keep, s, MASK_VALUE)
                p = jnp.exp(s - jnp.max(s, axis=-1, keepdims=True))
                total = jnp.sum(p, axis=-1, keepdims=True)
                o = dot(p.astype(BF16), v) / total
                o_ref[:, 0, :, here] = o.astype(BF16).reshape(SP, shard_len, HEAD_DIM)
                return carry

            lax.fori_loop(0, heads, head, 0)

        def w_loads(j, h, dst, at):
            part = (y + h) % 2
            return [
                load(2 * j, (wq, wk, wv)[j].at[:, cols(part * half + me * eighth, eighth)], dst.at[0:half, at : at + eighth]),
                load(2 * j + 1, qkv_rem.at[2 * j + h], dst.at[half:dim, at : at + eighth]),
            ]

        def heads_half(h, carry):
            @pl.when(h == 0)
            def _():
                got_a(0, 0)

            loads = w_loads(0, h, w_qk, 0) + w_loads(1, h, w_qk, eighth)
            loads[0].start()
            loads[2].start()
            qkv_copy(0, h).wait_recv()
            loads[1].start()
            qkv_copy(1, h).wait_recv()
            loads[3].start()
            for d in loads:
                d.wait()

            def qk_side(side, c2):
                @pl.when((h == 0) & (side == 0))
                def _():
                    for r in range(ROW_CHUNKS):
                        act_copy(s_a, a_all, 0, r).wait_recv()

                @pl.when((h == 0) & (side == 1))
                def _():
                    lax.fori_loop(1, ROW_CHUNKS, got_a, 0)
                    for r in range(ROW_CHUNKS):
                        act_copy(s_a, a_all, 2, r).wait_recv()

                t0 = side * 2 * ROW_CHUNKS

                def body(a_ref, q_ref, k_ref):
                    sp = sp_of((t0 + pl.program_id(0)) // ROW_CHUNKS)
                    c_tab, s_tab = cos_buf[sp], sin_buf[sp]
                    for n in range(2 * eighth // NB):
                        acc = dot(a_ref[...], w_qk[:, n * NB : (n + 1) * NB])
                        for i in range(NB // HEAD_DIM):
                            t = acc[:, i * HEAD_DIM : (i + 1) * HEAD_DIM]
                            turned = pltpu.roll(t, HEAD_DIM // 2, 1)
                            shape = (tile_rows, shard_len, HEAD_DIM)
                            rot = t.reshape(shape) * c_tab + turned.reshape(shape) * s_tab
                            lo = n * NB + i * HEAD_DIM
                            ref = q_ref if lo < eighth else k_ref
                            lo = lo % eighth
                            ref[0, :, :, lo : lo + HEAD_DIM] = rot.astype(BF16)

                def spec(j):
                    return pl.BlockSpec(
                        (1, tile_rows, shard_len, eighth),
                        lambda t: ((2 * j + h) * SP + (t0 + t) // ROW_CHUNKS, (t0 + t) % ROW_CHUNKS, 0, 0),
                    )

                pltpu.emit_pipeline(
                    body,
                    grid=(2 * ROW_CHUNKS,),
                    in_specs=[pl.BlockSpec((tile, dim), lambda t: (t0 + t, 0))],
                    out_specs=[spec(0), spec(1)],
                )(a_all, qkv, qkv)
                return c2

            v_loads = w_loads(2, h, w_v, 0)
            v_loads[0].start()
            lax.fori_loop(0, 2, qk_side, 0)
            qkv_copy(2, h).wait_recv()
            v_loads[1].start()
            for d in v_loads:
                d.wait()

            def rows_chunk(r, c2):
                def v_body(a_ref, v_ref):
                    for lo in range(0, eighth, NB):
                        size = min(NB, eighth - lo)
                        acc = dot(a_ref[...], w_v[:, lo : lo + size])
                        v_ref[0, :, :, lo : lo + size] = acc.astype(BF16).reshape(tile_rows, shard_len, size)

                pltpu.emit_pipeline(
                    v_body,
                    grid=(SP,),
                    in_specs=[pl.BlockSpec((tile, dim), lambda t: (t * ROW_CHUNKS + r, 0))],
                    out_specs=[pl.BlockSpec((1, tile_rows, shard_len, eighth), lambda t: ((4 + h) * SP + t, r, 0, 0))],
                )(a_all, qkv)

                def spec(block):
                    return pl.BlockSpec((SP, 1, shard_len, eighth), lambda t: (block, r * tile_rows + t, 0, 0))

                pltpu.emit_pipeline(
                    attn_body,
                    grid=(tile_rows,),
                    in_specs=[spec(h), spec(2 + h), spec(4 + h)],
                    out_specs=[spec(h)],
                )(qkv, qkv, qkv, o_own)
                for k in (2, 3, 1):
                    for s in range(2):
                        o_copy(h, r, k, s).start()
                return c2

            lax.fori_loop(0, ROW_CHUNKS, rows_chunk, 0)
            return carry

        lax.fori_loop(0, 2, heads_half, 0)

    def out_phase(w_buf, o_buf):
        def fetch(k, slot):
            return [
                load(2 * slot, wo.at[:, cols(sp_of(k) * quarter, quarter)], w_buf.at[slot, 0:half]),
                load(2 * slot + 1, wo_rem.at[k], w_buf.at[slot, half:dim]),
            ]

        def o_load(h, k, s):
            src = o_own.at[4 * h + 2 * s] if k == 0 else o_got.at[6 * h + 2 * (k - 1) + s]
            dst = o_buf.at[s * num_rows : (s + 1) * num_rows, :, cols(h * half + sp_of(k) * eighth, eighth)]
            return load(4 + 8 * h + 2 * k + s, src, dst)

        loads = []

        def o_fetch(h):
            for k in (0, 1, 2, 3):
                for s in range(2):
                    if k:
                        for r in range(ROW_CHUNKS):
                            o_copy(h, r, k, s).wait_recv()
                    d = o_load(h, k, s)
                    d.start()
                    loads.append(d)

        o_fetch(0)
        wo_copy(0).wait_recv()
        wo_copy(2).start()
        wo_copy(1).start()
        for d in fetch(0, 0):
            d.start()
        o_fetch(1)
        for d in loads:
            d.wait()

        def step(k, carry):
            slot = k % 2

            @pl.when(k == 0)
            def _():
                wo_copy(1).wait_recv()
                for d in fetch(1, 1):
                    d.start()

            @pl.when(k == 2)
            def _():
                wo_copy(2).wait_recv()
                wo_copy(3).start()
                for d in fetch(2, 0):
                    d.start()

            for d in fetch(k, slot):
                d.wait()

            def run(x_ref_all, s):
                def body(x_ref, h_ref):
                    mine = pl.ds(s * num_rows + pl.program_id(0) * tile_rows, tile_rows)
                    for n in range(quarter // NB):
                        here = slice(n * NB, (n + 1) * NB)
                        lhs = o_buf[mine].reshape(tile, dim)
                        h_ref[:, here] = (x_ref[:, here].astype(F32) + dot(lhs, w_buf[slot, :, here])).astype(BF16)

                pltpu.emit_pipeline(
                    body,
                    grid=(ROW_CHUNKS,),
                    in_specs=[pl.BlockSpec((tile, quarter), lambda t: (t, sp_of(k)))],
                    out_specs=[pl.BlockSpec((tile, quarter), lambda t: (s * ROW_CHUNKS + t, sp_of(k)))],
                )(x_ref_all, hid)

            run(x, 0)

            @pl.when(k == 2)
            def _():
                wo_copy(3).wait_recv()
                for d in fetch(3, 1):
                    d.start()

            run(x_got, 1)
            return carry

        lax.fori_loop(0, SP, step, 0)

    def b_chunk(n, carry):
        s, r = n // ROW_CHUNKS, n % ROW_CHUNKS
        norm_chunk(hid, b_all, 1, n * tile, 2 * s * tokens + r * tile)
        copy(
            s_b + n,
            b_all.at[rows(2 * s * tokens + r * tile, tile)],
            b_all.at[rows((2 * s + 1) * tokens + r * tile, tile)],
            to[1],
        ).start()
        return carry

    def gate_phase(w_buf):
        def w_load(slot, start, size):
            mine = [
                load(4 * slot + t, (wg, wu)[t].at[:, cols(me * feat + start, size)], w_buf.at[slot, 0:half, t * size : (t + 1) * size])
                for t in range(2)
            ]
            other = [
                load(4 * slot + 2 + t, gu_rem.at[t, :, cols(start, size)], w_buf.at[slot, half:dim, t * size : (t + 1) * size])
                for t in range(2)
            ]
            return mine, other

        def run(c, side, slot, start, size):
            def body(b_ref, o_ref):
                parts = [dot(b_ref[...], w_buf[slot, :, n * NB : (n + 1) * NB]) for n in range(2 * size // NB)]
                both = [p[:, lo : lo + 128] for p in parts for lo in (0, 128)]
                n = size // 128
                for i in range(n):
                    o_ref[:, i * 128 : (i + 1) * 128] = (jax.nn.silu(both[i]) * both[n + i]).astype(BF16)

            n_t = 2 * ROW_CHUNKS
            pltpu.emit_pipeline(
                body,
                grid=(n_t,),
                in_specs=[pl.BlockSpec((tile, dim), lambda t: (side * n_t + t, 0))],
                out_specs=[pl.BlockSpec((tile, size), lambda t: (side * n_t + t, 0))],
            )(b_all, u_own.at[:, cols(start, size)])

            @pl.when(side == 0)
            def _():
                u_copy(c, 1, start, size).start()

            @pl.when(side == 1)
            def _():
                u_copy(c, 2, start, size).start()
                u_copy(c, 3, start, size).start()

        def chunk(c, slot, start, size, prefetch, before, middle, after):
            before()
            mine, other = w_load(slot, start, size)
            for t in range(2):
                gu_copy(c, t, start, size).wait_recv()
            for d in other:
                d.start()
            for d in mine + other:
                d.wait()
            prefetch()

            def sides(t, carry):
                side = 1 - t

                @pl.when(c == 0)
                def _():
                    for r in range(ROW_CHUNKS):
                        n = side * ROW_CHUNKS + r
                        copy(
                            s_b + n,
                            b_all.at[rows(2 * side * tokens + r * tile, tile)],
                            b_all.at[rows((2 * side + 1) * tokens + r * tile, tile)],
                            to[1],
                        ).wait_recv()

                @pl.when(side == 0)
                def _():
                    middle()

                run(c, side, slot, start, size)
                return carry

            lax.fori_loop(0, 2, sides, 0)
            after()

        def at(c, n, work):
            @pl.when(c == n)
            def _():
                work()

        for d in w_load(0, 0, GATE_COLS)[0]:
            d.start()

        def full(c, carry):
            def prefetch():
                @pl.when(c + 1 < FULL_CHUNKS)
                def _():
                    for d in w_load((c + 1) % 2, (c + 1) * GATE_COLS, GATE_COLS)[0]:
                        d.start()

                @pl.when(c + 1 == FULL_CHUNKS)
                def _():
                    for d in w_load((c + 1) % 2, starts[FULL_CHUNKS], 128)[0]:
                        d.start()

            def before():
                at(c, FULL_CHUNKS - 1, lambda: pass_y(0, 1))

            def middle():
                at(c, FULL_CHUNKS - 1, lambda: (pass_y(2, 3, 4), pass_x(0)))

            def after():
                at(c, FULL_CHUNKS - 1, lambda: (pass_y(5, 6, 7), pass_x(1)))

            chunk(c, c % 2, c * GATE_COLS, GATE_COLS, prefetch, before, middle, after)
            return carry

        lax.fori_loop(0, FULL_CHUNKS, full, 0)

        def brief(c, carry):
            def start_of(i):
                return starts[FULL_CHUNKS] + (i - FULL_CHUNKS) * 128

            def prefetch():
                @pl.when(c + 1 < chunks)
                def _():
                    for d in w_load((c + 1) % 2, start_of(c + 1), 128)[0]:
                        d.start()

            def before():
                at(c, FULL_CHUNKS, lambda: pass_y(8))
                at(c, FULL_CHUNKS + 1, lambda: pass_x(4))
                at(c, FULL_CHUNKS + 2, lambda: pass_x(6))

            def middle():
                at(c, FULL_CHUNKS, lambda: pass_x(2, 3))
                at(c, FULL_CHUNKS + 1, lambda: pass_x(5))
                at(c, FULL_CHUNKS + 2, lambda: (pass_y(9), pass_x(7)))

            chunk(c, c % 2, start_of(c), 128, prefetch, before, middle, lambda: None)
            return carry

        lax.fori_loop(FULL_CHUNKS, chunks, brief, 0)

    def down_phase(u_buf, w_mine, w_other, h_buf, acc_buf, o_buf):
        total = SP * down_chunks
        main = total - SP
        last = end + 1 - DOWN_PARTS
        band = tokens // 2

        def u_load(k):
            sp = sp_of(k)
            at = ((sp // 2 + y) % 2) * half_feat + (sp % 2) * feat
            return load(k, (u_got if k else u_own).at[pl.ds(k * tokens, tokens)], u_buf.at[:, cols(at, feat)])

        def out_cols(n):
            return cols(sp_of(n % SP) * quarter + (n // SP) * DOWN_COLS, DOWN_COLS)

        def fetch(n):
            slot = n % 2
            here = out_cols(n)
            return [load(4 + 2 * slot, wd.at[:, here], w_mine.at[slot]), load(5 + 2 * slot, hid.at[0:tokens, here], h_buf.at[slot])]

        def store(n):
            return load(8 + n % 2, o_buf.at[n % 2], out.at[:, out_cols(n)])

        def mine(n):
            @pl.when(n + 1 < total)
            def _():
                for d in fetch(n + 1):
                    d.start()

            for d in fetch(n):
                d.wait()

            def part(t, carry):
                m = rows(t * band, band)
                acc_buf[n % (2 * SP), m] = h_buf[n % 2, m].astype(F32) + dot(u_buf[m, 0:half_feat], w_mine[n % 2])
                return carry

            lax.fori_loop(0, 2, part, 0)

        for d in fetch(0):
            d.start()
        u_load(0).start()
        pass_y(10, 11)
        pass_x(8)
        for k in (1, 2, 3):
            for c in range(chunks):
                u_copy(c, k, starts[c], sizes[c]).wait_recv()
            u_load(k).start()
        for k in range(SP):
            u_load(k).wait()

        def other(n):
            c, k = n // SP, n % SP
            ready = load(12, wd_rem.at[k, :, cols(c * DOWN_COLS, DOWN_COLS)], w_other)
            for side in (1, 3):

                @pl.when(k == side)
                def _():
                    for p in range(DOWN_PARTS):
                        wd_copy(DOWN_PARTS * c + p, side).wait_recv()

            ready.start()

            @pl.when(n >= 2)
            def _():
                store(n - 2).wait()

            ready.wait()

            def part(t, carry):
                m = rows(t * band, band)
                o_buf[k % 2, m] = (acc_buf[n % (2 * SP), m] + dot(u_buf[m, half_feat:], w_other[...])).astype(BF16)
                return carry

            lax.fori_loop(0, 2, part, 0)
            store(n).start()

        pieces = DOWN_PARTS * down_chunks

        def passes(n, table):
            for when, (m_y, m_x) in table.items():

                @pl.when(n == when)
                def _():
                    if m_y < pieces:
                        pass_y(m_y)
                    if m_x is not None:
                        pass_x(m_x)

        def first(n, carry):
            passes(n, {0: (12, None), 2: (15, 11), 3: (16, 12), 5: (18, 14), 7: (19, 15)})
            mine(n)
            passes(n, {0: (13, 9), 1: (14, 10), 3: (17, 13)})

            @pl.when(n < SP)
            def _():
                other(n)

            return carry

        def slot(i, carry):
            m = 17 + i + 2 * ((i + 14) // 21)
            c, r = (m - 8) // 9, (m - 8) % 9
            pass_y(20 + i)
            pass_x(16 + i)
            two = 2 * (r // 3)

            @pl.when((r == 0) | (r == 3))
            def _():
                def run(k, c2):
                    other(SP * c + two + k)
                    return c2

                lax.fori_loop(0, 2, run, 0)

            @pl.when((((r == 1) | (r == 4)) & (c < 3)) | (((r == 5) | (r == 6)) & (c == 1)))
            def _():
                def run(k, c2):
                    mine(2 * SP * c + two + 2 * (r // 5) + k)
                    return c2

                lax.fori_loop(0, 2, run, 0)

            return carry

        lax.fori_loop(0, 2 * SP, first, 0)
        if down_chunks > 2:
            lax.fori_loop(0, last + 4 - 19, slot, 0)
        next_y, next_x = (4, 1) if down_chunks > 2 else (9, 7)

        base = main % (2 * SP)

        def piece_load(k, p):
            at = rows((2 * k + p % 2) * part_rows, part_rows)
            return load(2 * k + p % 2, wd_rem.at[k, rows(p * part_rows, part_rows), cols(quarter - DOWN_COLS, DOWN_COLS)], w_other.at[at])

        def piece_dot(k, p):
            piece_load(k, p).wait()
            at = rows((2 * k + p % 2) * part_rows, part_rows)
            acc_buf[base + k] = acc_buf[base + k] + dot(u_buf[:, cols(half_feat + p * part_rows, part_rows)], w_other[at])

        def finish(k):
            store(main + k - 2).wait()
            o_buf[k % 2] = acc_buf[base + k].astype(BF16)
            store(main + k).start()

        def first_two(p):
            if isinstance(p, int):
                wd_arrived(last + p, 1)
            else:

                @pl.when(p < DOWN_PARTS - 1)
                def _():
                    wd_arrived(last + p, 1)

                @pl.when(p == DOWN_PARTS - 1)
                def _():
                    wd_arrived(end, 1)

            for k in (0, 1):
                piece_load(k, p).start()

        first_two(0)

        def last_step(p, carry):
            @pl.when((p > 0) & (p + next_y < DOWN_PARTS - 1))
            def _():
                pass_y(last + next_y + p)

            @pl.when(p + next_y == DOWN_PARTS - 1)
            def _():
                pass_y(end)

            piece_dot(0, p)
            piece_dot(1, p)

            @pl.when(p == DOWN_PARTS - 1)
            def _():
                finish(0)
                finish(1)

            @pl.when((p >= next_x) & (p < DOWN_PARTS - 1))
            def _():
                pass_x(last + p)

            @pl.when(p == DOWN_PARTS - 1)
            def _():
                pass_x(end)

            piece_load(2, p).start()

            @pl.when(p + 1 < DOWN_PARTS)
            def _():
                first_two(p + 1)

            @pl.when(p > 0)
            def _():
                piece_dot(3, p - 1)

            piece_dot(2, p)

            @pl.when(p == DOWN_PARTS - 1)
            def _():
                finish(2)

            @pl.when(p < DOWN_PARTS - 1)
            def _():
                wd_arrived(last + p, 3)

            @pl.when(p == DOWN_PARTS - 1)
            def _():
                wd_arrived(end, 3)

            piece_load(3, p).start()
            return carry

        lax.fori_loop(0, DOWN_PARTS, last_step, 0)
        piece_dot(3, DOWN_PARTS - 1)
        finish(3)
        for k in (2, 3):
            store(main + k).wait()

    lax.fori_loop(0, ROW_CHUNKS, own_a, 0)
    pl.run_scoped(attention, pltpu.VMEM((dim, 2 * eighth), BF16), pltpu.VMEM((dim, eighth), BF16))
    pl.run_scoped(out_phase, pltpu.VMEM((2, dim, quarter), BF16), pltpu.VMEM((2 * num_rows, shard_len, dim), BF16))
    lax.fori_loop(0, 2 * ROW_CHUNKS, b_chunk, 0)
    pl.run_scoped(gate_phase, pltpu.VMEM((2, dim, 2 * GATE_COLS), BF16))
    pl.run_scoped(
        down_phase,
        pltpu.VMEM((tokens, 2 * half_feat), BF16),
        pltpu.VMEM((2, half_feat, DOWN_COLS), BF16),
        pltpu.VMEM((half_feat, DOWN_COLS), BF16),
        pltpu.VMEM((2, tokens, DOWN_COLS), BF16),
        pltpu.VMEM((2 * SP, tokens, DOWN_COLS), F32),
        pltpu.VMEM((2, tokens, DOWN_COLS), BF16),
    )

    for d in gain_copies:
        d.wait_send()
    for h in range(2):
        for j in range(3):
            qkv_copy(j, h).wait_send()
    for k in range(SP):
        wo_copy(k).wait_send()
    for c in range(chunks):
        for t in range(2):
            gu_copy(c, t, starts[c], sizes[c]).wait_send()
        for k in (1, 2, 3):
            u_copy(c, k, starts[c], sizes[c]).wait_send()
    for r in range(ROW_CHUNKS):
        x_copy(r).wait_send()
        for piece in (0, 2):
            act_copy(s_a, a_all, piece, r).wait_send()
            act_copy(s_b, b_all, piece, r).wait_send()

        def o_sent(h, carry):
            for k in (1, 2, 3):
                for s in range(2):
                    o_copy(h, r, k, s).wait_send()
            return carry

        lax.fori_loop(0, 2, o_sent, 0)

    def wd_sent(m, carry):
        for k in range(SP):
            wd_copy(m, k).wait_send()
        return carry

    lax.fori_loop(0, end, wd_sent, 0)
    for i in range(LAST_CUTS):
        for k in range(SP):
            last_copy(i, k).wait_send()


def hand_over(src, dst, buf, in_sem, out_sem):
    n = src.shape[0]
    reads = [pltpu.make_async_copy(src.at[r], buf.at[r], in_sem.at[r]) for r in range(n)]
    writes = [pltpu.make_async_copy(buf.at[r], dst.at[r], out_sem.at[r]) for r in range(n)]
    for d in reads:
        d.start()
    for r in range(n):
        reads[r].wait()
        writes[r].start()
    for d in writes:
        d.wait()


def tables(shard_len):
    inv_freq = np.exp(np.arange(HEAD_DIM // 2, dtype=np.float32) * np.float32(-2.0 * math.log(ROPE_THETA) / HEAD_DIM))
    pos = np.arange(shard_len)[None, :] * SP + np.arange(SP)[:, None]
    angles = (pos.astype(np.float32)[..., None] * inv_freq.astype(np.float32)).astype(np.float64)
    cos, sin = np.cos(angles), np.sin(angles)
    return (
        np.concatenate([cos, cos], axis=-1).astype(np.float32),
        np.concatenate([-sin, sin], axis=-1).astype(np.float32),
    )


def local_layer(x_loc, norm_attn, w_query, w_key, w_value, w_out, norm_mlp, w_gate, w_up, w_down):
    num_rows, shard_len, dim = x_loc.shape
    tokens = num_rows * shard_len
    half, quarter, eighth = dim // 2, dim // 4, dim // 8
    half_feat = w_down.shape[0]
    feat = half_feat // 2
    cos, sin = tables(shard_len)

    def buf(*shape):
        return jax.ShapeDtypeStruct(shape, BF16)

    shapes = [
        buf(tokens, dim),
        buf(half),
        buf(half),
        buf(tokens, dim),
        buf(SP * tokens, dim),
        buf(6, half, eighth),
        buf(SP, half, quarter),
        buf(2, half, feat),
        buf(SP, half_feat, quarter),
        buf(6 * SP, num_rows, shard_len, eighth),
        buf(2 * SP, num_rows, shard_len, eighth),
        buf(12, num_rows, shard_len, eighth),
        buf(2 * tokens, dim),
        buf(SP * tokens, dim),
        buf(SP * tokens, feat),
        buf(SP * tokens, feat),
    ]
    chunks = FULL_CHUNKS + (feat - FULL_CHUNKS * GATE_COLS) // 128
    copies = 2 + 6 + 4 + 2 * chunks + 4 * DOWN_PARTS * (quarter // DOWN_COLS) + 4 * LAST_CUTS + 17 * ROW_CHUNKS + 3 * chunks
    outs = pl.pallas_call(
        layer_kernel,
        out_shape=shapes,
        in_specs=[ANY] * 12,
        out_specs=[ANY] * len(shapes),
        scratch_shapes=[
            *[pltpu.VMEM((half,), BF16)] * 4,
            pltpu.VMEM((SP, shard_len, HEAD_DIM), F32),
            pltpu.VMEM((SP, shard_len, HEAD_DIM), F32),
            pltpu.SemaphoreType.DMA((copies,)),
            pltpu.SemaphoreType.DMA((copies,)),
            pltpu.SemaphoreType.DMA((20,)),
        ],
        compiler_params=pltpu.CompilerParams(collective_id=0, has_side_effects=True, vmem_limit_bytes=67043328),
        name="decoder_layer",
    )(x_loc.reshape(tokens, dim), norm_attn, norm_mlp, w_query, w_key, w_value, w_out, w_gate, w_up, w_down, jnp.asarray(cos), jnp.asarray(sin))
    return pl.pallas_call(
        hand_over,
        out_shape=buf(*x_loc.shape),
        in_specs=[ANY],
        out_specs=ANY,
        scratch_shapes=[
            pltpu.VMEM(x_loc.shape, BF16),
            pltpu.SemaphoreType.DMA((num_rows,)),
            pltpu.SemaphoreType.DMA((num_rows,)),
        ],
        compiler_params=pltpu.CompilerParams(vmem_limit_bytes=67043328),
        name="hand_over",
    )(outs[0].reshape(x_loc.shape))


def solution(mesh):
    row_spec = P(("dp", "fsdp"), "sp", None)
    weight_spec = P("fsdp", None)
    gain_spec = P("fsdp")
    in_specs = (row_spec, gain_spec, weight_spec, weight_spec, weight_spec, weight_spec, gain_spec, weight_spec, weight_spec, weight_spec)
    fn = jax.shard_map(local_layer, mesh=mesh, in_specs=in_specs, out_specs=row_spec, check_vma=False)

    def run(*args):
        with jax.sharding.use_abstract_mesh(mesh.abstract_mesh):
            return fn(*args)

    return run
```
